256 devices in a mesh: gx: 32 (over y, x, core), gy: 8 (over z).
Axes of the slice: x: 4, y: 4, z: 8, core: 2. Of those that a mesh axis runs over, the one named last changes fastest.
Arguments:
- displacement: float32 [3, 512, 256, 128], P(None, 'gx', 'gy'), may hold values from -4 to 4
- force: float32 [3, 512, 256, 128], P(None, 'gx', 'gy'), may hold values from -12 to 12
- damage: float32 [512, 256, 128], P('gx', 'gy'), may hold values from 0 to 0.8
- history: float32 [512, 256, 128], P('gx', 'gy'), may hold values from 0.05 to 3
- crack_flags: int32 [512, 256, 128], P('gx', 'gy'), may hold values 0 or 1
Outputs:
- displacement_out: float32 [3, 512, 256, 128], P(None, 'gx', 'gy')
- damage_out: float32 [512, 256, 128], P('gx', 'gy')
- history_out: float32 [512, 256, 128], P('gx', 'gy')
The draws below stay inside these ranges and needn't reach their ends.
All inputs are finite; a program needn't handle non-finite values. No bound on the sum of `crack_flags` on one device may be relied on, other than what follows from the above.
Results may differ from the reference program's by a relative error of at most 0.0003.
Values sent between devices are 32-bit elements; how exact they have to be, the bound alone decides.
No kernel may reach another device: no remote copies, remote signals or barrier semaphores. Data moves between devices by JAX's collectives and lax.ppermute only.
A program may use at most 64 MiB of HBM per device.

```python
import math
import jax
import jax.numpy as jnp

NZ = 128
ITERS = 3
NX = 512
NY = 256


def draw_force(key, part):
    key_rows = jax.random.fold_in(key, 11)
    key_values = jax.random.fold_in(key, 23)
    rising = 10.0 ** (0.5 * jnp.arange(NX, dtype=jnp.float32) / max(NX - 1, 1))
    across = 3.0 ** jax.random.uniform(key_rows, (NY,), jnp.float32, 0.0, 1.0)
    scales = 0.3 * rising[:, None, None] * across[None, :, None]
    values = jnp.clip(jax.random.normal(key_values, (3, NX, NY, NZ), jnp.float32), -4.0, 4.0)
    return values * scales[None]


def place_ends(values, stream_key, smallest, high):
    spot = [jax.random.randint(jax.random.fold_in(stream_key, axis), (), 0, length) for axis, length in enumerate(values.shape)]
    widest = values.shape.index(max(values.shape))
    beside = spot[:widest] + [(spot[widest] + 1) % values.shape[widest]] + spot[widest + 1:]
    return values.at[tuple(spot)].set(smallest).at[tuple(beside)].set(high)


def shard_levels(own_key, shape, pieces, low, largest):
    level, own = 1.0, jax.random.fold_in(own_key, 6)
    for dim, shards_of in pieces:
        steps = jnp.exp(jax.random.uniform(jax.random.fold_in(own, dim), (shards_of,), jnp.float32, low / len(pieces), largest / len(pieces)))
        level = level * jnp.repeat(steps, shape[dim] // shards_of).reshape([-1 if axis == dim else 1 for axis in range(len(shape))])
    return level


def noise(rng, dims, scale, limit, split=(), kind=jnp.bfloat16):
    values = scale * jax.random.normal(rng, dims, jnp.float32)
    if split:
        values = values * shard_levels(rng, dims, split, -0.22, 0.18)
    return jnp.clip(values, -limit, limit).astype(kind)


def setup_inputs(seed: int = 0) -> dict:
    arg_keys = jax.random.split(jax.random.key(seed), 6)
    return {
        "displacement": noise(arg_keys[0], (3, NX, NY, NZ), 0.3, 4.0, ((1, 32), (2, 8)), jnp.float32),
        "force": draw_force(jax.random.fold_in(arg_keys[5], 71), 0),
        "damage": jnp.clip(0.8 * jax.random.uniform(arg_keys[2], (NX, NY, NZ), jnp.float32) ** shard_levels(arg_keys[2], (NX, NY, NZ), ((0, 32), (1, 8)), -0.2, 0.2), 0.0, 0.8),
        "history": jnp.clip(jnp.exp(math.log(3.0) - 4.0943445 * jax.random.uniform(arg_keys[3], (NX, NY, NZ), jnp.float32) ** shard_levels(arg_keys[3], (NX, NY, NZ), ((0, 32), (1, 8)), -0.2, 0.2)), 0.05, 3.0),
        "crack_flags": place_ends((jax.random.randint(arg_keys[4], (NX, NY, NZ), 0, 16) < 1).astype(jnp.int32), jax.random.fold_in(arg_keys[4], 1), 0, 1),
    }


shear_modulus = 1.0
lame_first = 1.5
spring_term = 0.5
stiff_floor = 1e-3
crack_load = 4.0
tough_ratio = 0.5
length_term = 2.0
stress_index = ((0, 3, 4), (3, 1, 5), (4, 5, 2))


def strains(padded):
    base = padded[:, :-1, :-1, :-1]
    grads = []
    for component in range(3):
        grads.append((padded[component, 1:, :-1, :-1] - base[component],
                      padded[component, :-1, 1:, :-1] - base[component],
                      padded[component, :-1, :-1, 1:] - base[component]))
    return (grads[0][0], grads[1][1], grads[2][2],
            0.5 * (grads[0][1] + grads[1][0]),
            0.5 * (grads[0][2] + grads[2][0]),
            0.5 * (grads[1][2] + grads[2][1]))


def lowered(values, direction):
    if direction == 0:
        return values[:-1, 1:, 1:]
    if direction == 1:
        return values[1:, :-1, 1:]
    return values[1:, 1:, :-1]


def elastic(padded, padded_gain):
    strain = strains(padded)
    weight = padded_gain[:-1, :-1, :-1]
    trace = strain[0] + strain[1] + strain[2]
    stress = [weight * (2.0 * shear_modulus * strain[index] + lame_first * trace) for index in range(3)]
    stress = stress + [weight * (2.0 * shear_modulus * strain[index]) for index in range(3, 6)]
    images = []
    for component in range(3):
        summed = spring_term * padded[component, 1:-1, 1:-1, 1:-1]
        for direction in range(3):
            values = stress[stress_index[component][direction]]
            summed = summed + lowered(values, direction) - values[1:, 1:, 1:]
        images.append(summed)
    return jnp.stack(images), strain


def energy(strain):
    owned = [item[1:, 1:, 1:] for item in strain]
    trace = owned[0] + owned[1] + owned[2]
    squares = owned[0] ** 2 + owned[1] ** 2 + owned[2] ** 2 + 2.0 * (owned[3] ** 2 + owned[4] ** 2 + owned[5] ** 2)
    bulk_half = 0.5 * (lame_first + 2.0 * shear_modulus / 3.0)
    return bulk_half * jnp.maximum(trace, 0.0) ** 2 + shear_modulus * (squares - trace * trace / 3.0)


def damage_apply(padded, driving):
    center = padded[1:-1, 1:-1, 1:-1]
    beside_all = (padded[2:, 1:-1, 1:-1] + padded[:-2, 1:-1, 1:-1] + padded[1:-1, 2:, 1:-1]
              + padded[1:-1, :-2, 1:-1] + padded[1:-1, 1:-1, 2:] + padded[1:-1, 1:-1, :-2])
    return (tough_ratio + 2.0 * driving) * center + length_term * (6.0 * center - beside_all)


def pad_vector(values):
    return jnp.pad(values, ((0, 0), (1, 1), (1, 1), (1, 1)))


def conjugate(operate, start, target):
    current = start
    resid = target - operate(start)
    direction = resid
    norm_now = jnp.sum(resid * resid)
    for number in range(ITERS):
        image = operate(direction)
        alpha = norm_now / jnp.sum(direction * image)
        current = current + alpha * direction
        resid = resid - alpha * image
        norm_next = jnp.sum(resid * resid)
        direction = resid + (norm_next / norm_now) * direction
        norm_now = norm_next
    return current


def reference(displacement, force, damage, history, crack_flags):
    gain = (1.0 - damage) ** 2 + stiff_floor
    padded_gain = jnp.pad(gain, 1)

    def elastic_only(values):
        return elastic(pad_vector(values), padded_gain)[0]

    moved = conjugate(elastic_only, displacement, force)
    psi = energy(elastic(pad_vector(moved), padded_gain)[1])
    history_out = jnp.maximum(jnp.maximum(history, psi), crack_load * crack_flags.astype(jnp.float32))

    def damage_only(values):
        return damage_apply(jnp.pad(values, 1), history_out)

    damage_out = conjugate(damage_only, damage, 2.0 * history_out)
    return moved, damage_out, history_out
```

```python
import jax
import jax.numpy as jnp
from jax import lax
from jax.experimental import pallas as pl
from jax.experimental.pallas import tpu as pltpu
from jax.sharding import PartitionSpec as P

INTERPRET = False
f32 = jnp.float32

spring_term = 0.5
stiff_floor = 0.001
crack_load = 4.0
tough_ratio = 0.5
length_term = 2.0
bulk_half = 0.5 * (1.5 + 2.0 / 3.0)

LX, LY, LZ = 16, 32, 128
ROWS, DEPTH, OFF = 40, 23, 3

SHIFT_U = 14.0
SHIFT_D = 18.0


def call(kernel, outs, scratch=(), limit=8 << 20, name=None):
    vmem = pl.BlockSpec(memory_space=pltpu.VMEM)
    smem = pl.BlockSpec(memory_space=pltpu.SMEM)

    def run(*args, flags=None):
        specs = [vmem] * len(args)
        if flags is not None:
            args, specs = (*args, flags), specs + [smem]
        return pl.pallas_call(
            kernel,
            out_shape=[jax.ShapeDtypeStruct(s, f32) for s in outs],
            in_specs=specs,
            out_specs=[vmem] * len(outs),
            scratch_shapes=[pltpu.VMEM(s, f32) for s in scratch],
            compiler_params=pltpu.CompilerParams(vmem_limit_bytes=limit),
            interpret=INTERPRET,
            name=name,
        )(*args)

    return run


def roll(x, shift, axis):
    return pltpu.roll(x, shift % x.shape[axis], axis)


def next_row(x):
    return roll(x, -1, 0)


def last_row(x):
    return roll(x, 1, 0)


def lanes(shape):
    return lax.broadcasted_iota(jnp.int32, shape, 1)


def next_lane(x):
    return jnp.where(lanes(x.shape) == LZ - 1, 0.0, roll(x, -1, 1))


def last_lane(x):
    return jnp.where(lanes(x.shape) == 0, 0.0, roll(x, 1, 1))


def low_half():
    return lax.broadcasted_iota(jnp.int32, (8, LZ), 0) < 4


def pack_first(one, two):
    return jnp.where(low_half(), one, roll(two, 4, 0))


def pack_last(one, two):
    return jnp.where(low_half(), roll(two, 4, 0), one)


def unpack(high, low, second):
    if second:
        return roll(jnp.where(low_half(), low, high), 4, 0)
    return jnp.where(low_half(), high, low)


def row_mask(flags):
    row = lax.broadcasted_iota(jnp.int32, (ROWS, LZ), 0)
    return jnp.where(row < LY, 1.0, jnp.where(row < LY + 4, flags[3], flags[2]))


def layer_flag(flags, i):
    return jnp.where(i < OFF, flags[0], jnp.where(i >= OFF + LX, flags[1], 1.0))


def pack_rows_kernel(disp, force, damage, first, last):
    def pack(field, k, at):
        first[at, k] = pack_first(field(k, 0), field(k + 8, 0))
        last[at, k] = pack_last(field(k, 24), field(k + 8, 24))

    def step(k, carry):
        for j in range(3):
            pack(lambda i, r: disp[j, i, r : r + 8], k, j)
            pack(lambda i, r: force[j, i, r : r + 8], k, 3 + j)
        pack(lambda i, r: damage[i, r : r + 8], k, 6)
        return carry

    lax.fori_loop(0, 8, step, 0, unroll=2)


def pack_layers_kernel(disp, force, damage, high, low, first, last):
    def put(ref, at, own, field, c):
        ref[at, 0:LY] = own[c]
        ref[at, LY:ROWS] = unpack(high[field, c % 8], low[field, c % 8], c >= 8)

    at = bt = 0
    for field in range(7):
        own = disp.at[field] if field < 3 else force.at[field - 3] if field < 6 else damage
        ahead, behind = (3, 2) if 3 <= field < 6 else (4, 3)
        for c in range(ahead):
            put(first, at, own, field, c)
            at += 1
        for c in range(LX - behind, LX):
            put(last, bt, own, field, c)
            bt += 1


def stress(u, n, gain):
    dx = [n[j] - u[j] for j in range(3)]
    dy = [next_row(u[j]) - u[j] for j in range(3)]
    dz = [next_lane(u[j]) - u[j] for j in range(3)]
    twice = gain + gain
    part = 0.75 * (dx[0] + dy[1] + dz[2])
    return (
        twice * (dx[0] + part),
        twice * (dy[1] + part),
        twice * (dz[2] + part),
        gain * (dx[1] + dy[0]),
        gain * (dx[2] + dz[0]),
        gain * (dy[2] + dz[1]),
    )


def divergence(u, s, before, diag):
    s00, s11, s22, s01, s02, s12 = s
    return (
        diag * u[0] + before[0] + last_row(s01) + last_lane(s02) - (s00 + s01 + s02),
        diag * u[1] + before[1] + last_row(s11) + last_lane(s12) - (s01 + s11 + s12),
        diag * u[2] + before[2] + last_row(s12) + last_lane(s22) - (s02 + s12 + s22),
    )


def fold(x):
    return x[0:8] + x[8:16] + x[16:24] + x[24:32]


def moments_out(out, sums):
    lane = lanes((1, LZ))
    row = jnp.zeros((1, LZ), f32)
    for k, value in enumerate(sums):
        total = jnp.sum(jnp.sum(value, axis=0, keepdims=True), axis=1, keepdims=True)
        row = jnp.where(lane == k, total, row)
    out[...] = jnp.broadcast_to(row, out.shape)


def elastic_kernel(
    disp, force, damage, high, low, layers_high, layers_low, flags,
    wide, v0, v1, v2, wide_damage, sums, load, gain,
):
    for field in range(7):
        if field < 3:
            own, into, ahead, behind = disp.at[field], wide.at[field], 4, 3
        elif field < 6:
            own, into, ahead, behind = force.at[field - 3], load.at[field - 3], 3, 2
        else:
            own, into, ahead, behind = damage, wide_damage, 4, 3
        start = 4 * field if field < 3 else 12 + 3 * (field - 3) if field < 6 else 21
        into[OFF + LX : OFF + LX + ahead] = layers_high[start : start + ahead]
        start = 3 * field if field < 3 else 9 + 2 * (field - 3) if field < 6 else 15
        into[OFF - behind : OFF] = layers_low[start : start + behind]
        if 3 <= field < 6:
            into[0] = jnp.zeros((ROWS, LZ), f32)

        def assemble(k, carry):
            into[OFF + k, 0:LY] = own[k]
            into[OFF + k + 8, 0:LY] = own[k + 8]
            into[OFF + k, LY:ROWS] = unpack(high[field, k], low[field, k], False)
            into[OFF + k + 8, LY:ROWS] = unpack(high[field, k], low[field, k], True)
            return carry

        lax.fori_loop(0, 8, assemble, 0, unroll=2)

    rows = row_mask(flags)

    def fill_gain(i, carry):
        left = 1.0 - wide_damage[i]
        gain[i] = (left * left + stiff_floor) * (rows * layer_flag(flags, i))
        return carry

    lax.fori_loop(0, DEPTH - 1, fill_gain, 0)

    none = jnp.zeros((ROWS, LZ), f32)

    def sweep(source, begin, end, diag, store):
        def step(i, carry):
            before, u = carry
            n = tuple(source[j, i + 1] for j in range(3))
            s = stress(u, n, gain[i])
            store(i, divergence(u, s, before, diag))
            return (s[0], s[3], s[4]), n

        first = tuple(source[j, OFF + begin] for j in range(3))
        lax.fori_loop(OFF + begin, OFF + end, step, ((none,) * 3, first))

    def store0(i, image):
        mask = rows * layer_flag(flags, i)
        for j in range(3):
            v0[j, i] = (load[j, i] - image[j]) * mask

    def store_to(ref):
        def store(i, image):
            mask = rows * layer_flag(flags, i)
            for j in range(3):
                ref[j, i] = image[j] * mask

        return store

    sweep(wide, -3, LX + 3, spring_term, store0)
    sweep(v0, -2, LX + 2, spring_term - SHIFT_U, store_to(v1))
    sweep(v1, -1, LX + 1, spring_term - SHIFT_U, store_to(v2))

    def add(c, acc):
        u = [v2[j, OFF + c] for j in range(3)]
        n = [v2[j, OFF + c + 1, 0:LY] for j in range(3)]
        up = [next_row(u[j])[0:LY] for j in range(3)]
        u = [u[j][0:LY] for j in range(3)]
        dx = [n[j] - u[j] for j in range(3)]
        dy = [up[j] - u[j] for j in range(3)]
        dz = [next_lane(u[j]) - u[j] for j in range(3)]
        trace = dx[0] + dy[1] + dz[2]
        e01, e02, e12 = dx[1] + dy[0], dx[2] + dz[0], dy[2] + dz[1]
        work = 2.0 * (dx[0] * dx[0] + dy[1] * dy[1] + dz[2] * dz[2])
        work = work + 1.5 * (trace * trace) + (e01 * e01 + e02 * e02 + e12 * e12)
        work = gain[OFF + c, 0:LY] * work
        a = [v0[j, OFF + c, 0:LY] for j in range(3)]
        b = [v1[j, OFF + c, 0:LY] for j in range(3)]

        def dot(x, y):
            return x[0] * y[0] + x[1] * y[1] + x[2] * y[2]

        square = dot(u, u)
        new = (
            dot(a, a), dot(a, b), dot(b, b), dot(b, u), square,
            work + (spring_term - SHIFT_U) * square,
        )
        return tuple(x + fold(y) for x, y in zip(acc, new))

    zero = jnp.zeros((8, LZ), f32)
    moments_out(sums, lax.fori_loop(0, LX, add, (zero,) * 6))


def coefficients(gathered, shift):
    row = jnp.sum(gathered[...], axis=0, keepdims=True)
    lane = lanes((1, LZ))
    mu = [
        jnp.broadcast_to(
            jnp.sum(jnp.where(lane == k, row, 0.0), axis=1, keepdims=True), (1, LZ)
        )
        for k in range(6)
    ]

    def inner(a, b, up=0):
        total = None
        for i, x in enumerate(a):
            for j, y in enumerate(b):
                term = x * y * mu[i + j + up]
                total = term if total is None else total + term
        return total

    one = jnp.ones((1, LZ), f32)
    resid, direction = [one], [one]
    found = []
    norm = mu[0]
    for number in range(3):
        work = inner(direction, direction, 1) + shift * inner(direction, direction)
        alpha = norm / work
        for i, x in enumerate(direction):
            if i < len(found):
                found[i] = found[i] + alpha * x
            else:
                found.append(alpha * x)
        if number < 2:
            image = [shift * x for x in direction] + [jnp.zeros((1, LZ), f32)]
            for i, x in enumerate(direction):
                image[i + 1] = image[i + 1] + x
            resid = [
                (resid[i] if i < len(resid) else 0.0) - alpha * x for i, x in enumerate(image)
            ]
            new = inner(resid, resid)
            ratio = new / norm
            direction = [
                x + ratio * direction[i] if i < len(direction) else x
                for i, x in enumerate(resid)
            ]
            norm = new
    return found


def history_kernel(
    gathered, wide, v0, v1, v2, history, crack, moved, found, first, last
):
    a0, a1, a2 = coefficients(gathered, SHIFT_U)

    def current(c):
        return tuple(
            wide[j, OFF + c] + a0 * v0[j, OFF + c] + a1 * v1[j, OFF + c] + a2 * v2[j, OFF + c]
            for j in range(3)
        )

    def step(c, u):
        n = current(c + 1)
        for j in range(3):
            moved[j, c] = u[j][0:LY]
        up = [next_row(u[j])[0:LY] for j in range(3)]
        here = [u[j][0:LY] for j in range(3)]
        dx = [n[j][0:LY] - here[j] for j in range(3)]
        dy = [up[j] - here[j] for j in range(3)]
        dz = [next_lane(here[j]) - here[j] for j in range(3)]
        trace = dx[0] + dy[1] + dz[2]
        e01, e02, e12 = dx[1] + dy[0], dx[2] + dz[0], dy[2] + dz[1]
        squares = dx[0] * dx[0] + dy[1] * dy[1] + dz[2] * dz[2]
        squares = squares + 0.5 * (e01 * e01 + e02 * e02 + e12 * e12)
        positive = jnp.maximum(trace, 0.0)
        psi = bulk_half * (positive * positive) + (squares - trace * trace / 3.0)
        flagged = crack_load * crack[c].astype(f32)
        found[c] = jnp.maximum(jnp.maximum(history[c], psi), flagged)
        return n

    lax.fori_loop(0, LX, step, current(0))

    def pack(k, carry):
        first[k] = pack_first(found[k, 0:8], found[k + 8, 0:8])
        last[k] = pack_last(found[k, 24:32], found[k + 8, 24:32])
        return carry

    lax.fori_loop(0, 8, pack, 0, unroll=2)


def pack_history_kernel(found, high, low, first, last):
    for at in range(3):
        first[at, 0:LY] = found[at]
        first[at, LY:ROWS] = unpack(high[at], low[at], False)
    for at, c in enumerate((LX - 2, LX - 1)):
        last[at, 0:LY] = found[c]
        last[at, LY:ROWS] = unpack(high[c - 8], low[c - 8], True)


def damage_kernel(
    found, high, low, layers_high, layers_low, wide_damage, flags, w0, w1, w2, sums, drive
):
    drive[OFF + LX : OFF + LX + 3] = layers_high[...]
    drive[OFF - 2 : OFF] = layers_low[...]

    def assemble(k, carry):
        drive[OFF + k, 0:LY] = found[k]
        drive[OFF + k + 8, 0:LY] = found[k + 8]
        drive[OFF + k, LY:ROWS] = unpack(high[k], low[k], False)
        drive[OFF + k + 8, LY:ROWS] = unpack(high[k], low[k], True)
        return carry

    lax.fori_loop(0, 8, assemble, 0, unroll=2)
    rows = row_mask(flags)

    def sweep(source, begin, end, store):
        def step(i, carry):
            before, now = carry
            n = source[i + 1]
            beside = before + n + next_row(now) + last_row(now)
            beside = beside + next_lane(now) + last_lane(now)
            store(i, now, beside)
            return now, n

        start = OFF + begin
        lax.fori_loop(start, OFF + end, step, (source[start - 1], source[start]))

    full = tough_ratio + 6.0 * length_term

    def store0(i, now, beside):
        twice = 2.0 * drive[i]
        image = (full + twice) * now - length_term * beside
        w0[i] = (twice - image) * (rows * layer_flag(flags, i))

    def store_to(ref):
        def store(i, now, beside):
            diag = (full - SHIFT_D) + 2.0 * drive[i]
            ref[i] = (diag * now - length_term * beside) * (rows * layer_flag(flags, i))

        return store

    sweep(wide_damage, -2, LX + 3, store0)
    sweep(w0, -1, LX + 2, store_to(w1))
    sweep(w1, 0, LX + 1, store_to(w2))

    lane = lanes((LY, LZ))
    row = lax.broadcasted_iota(jnp.int32, (LY, LZ), 0)
    edge = jnp.where(lane == 0, length_term, 0.0)
    edge = edge + jnp.where(row == 0, length_term * (1.0 - flags[2]), 0.0)
    edge = edge + (tough_ratio - SHIFT_D)

    def add(c, acc):
        wide_now = w2[OFF + c]
        u = wide_now[0:LY]
        dx = w2[OFF + c + 1, 0:LY] - u
        dy = next_row(wide_now)[0:LY] - u
        dz = next_lane(u) - u
        side = jnp.where(c == 0, length_term * (1.0 - flags[0]), 0.0)
        square = u * u
        work = (edge + side + 2.0 * drive[OFF + c, 0:LY]) * square
        work = work + length_term * (dx * dx + dy * dy + dz * dz)
        a, b = w0[OFF + c, 0:LY], w1[OFF + c, 0:LY]
        new = (a * a, a * b, b * b, b * u, square, work)
        return tuple(x + fold(y) for x, y in zip(acc, new))

    zero = jnp.zeros((8, LZ), f32)
    moments_out(sums, lax.fori_loop(0, LX, add, (zero,) * 6))


def update_kernel(gathered, damage, w0, w1, w2, out):
    b0, b1, b2 = coefficients(gathered, SHIFT_D)

    def step(c, carry):
        image = b0 * w0[OFF + c, 0:LY] + b1 * w1[OFF + c, 0:LY] + b2 * w2[OFF + c, 0:LY]
        out[c] = damage[c] + image
        return carry

    lax.fori_loop(0, LX, step, 0, unroll=2)


def exchange(first, last, axis):
    size = lax.axis_size(axis)
    up = [(i, i + 1) for i in range(size - 1)]
    down = [(b, a) for a, b in up]
    return lax.ppermute(first, axis, down), lax.ppermute(last, axis, up)


def body(displacement, force, damage, history, crack_flags):
    both = ("gx", "gy")
    count = lax.axis_size(both)
    ix, iy = lax.axis_index("gx"), lax.axis_index("gy")
    flags = jnp.stack(
        [ix > 0, ix < lax.axis_size("gx") - 1, iy > 0, iy < lax.axis_size("gy") - 1]
    ).astype(f32)
    wide_shape = (3, DEPTH, ROWS, LZ)
    field_shape = (DEPTH, ROWS, LZ)

    def gather(sums):
        return lax.all_to_all(sums, both, 0, 0, tiled=True)

    rows = call(pack_rows_kernel, [(7, 8, 8, LZ)] * 2, name="pack_rows")(
        displacement, force, damage
    )
    high, low = exchange(*rows, "gy")
    layers = call(pack_layers_kernel, [(25, ROWS, LZ), (18, ROWS, LZ)], name="pack_layers")(
        displacement, force, damage, high, low
    )
    layers_high, layers_low = exchange(*layers, "gx")
    wide, v0, v1, v2, wide_damage, sums = call(
        elastic_kernel,
        [wide_shape] * 4 + [field_shape, (count, LZ)],
        [wide_shape, field_shape],
        name="elastic",
        limit=16 << 20,
    )(displacement, force, damage, high, low, layers_high, layers_low, flags=flags)
    moved, found, first, last = call(
        history_kernel,
        [(3, LX, LY, LZ), (LX, LY, LZ), (8, 8, LZ), (8, 8, LZ)],
        name="history",
    )(gather(sums), wide, v0, v1, v2, history, crack_flags)
    high, low = exchange(first, last, "gy")
    layers = call(pack_history_kernel, [(3, ROWS, LZ), (2, ROWS, LZ)], name="pack_history")(
        found, high, low
    )
    layers_high, layers_low = exchange(*layers, "gx")
    w0, w1, w2, sums = call(
        damage_kernel, [field_shape] * 3 + [(count, LZ)], [field_shape], name="damage"
    )(found, high, low, layers_high, layers_low, wide_damage, flags=flags)
    (damage_out,) = call(update_kernel, [(LX, LY, LZ)], name="update")(
        gather(sums), damage, w0, w1, w2
    )
    return moved, damage_out, found


def solution(mesh):
    return jax.shard_map(
        body,
        mesh=mesh,
        in_specs=(
            P(None, "gx", "gy", None),
            P(None, "gx", "gy", None),
            P("gx", "gy", None),
            P("gx", "gy", None),
            P("gx", "gy", None),
        ),
        out_specs=(P(None, "gx", "gy", None), P("gx", "gy", None), P("gx", "gy", None)),
        check_vma=False,
    )
```

```python
import jax
import jax.numpy as jnp
from jax import lax
from jax.experimental import pallas as pl
from jax.experimental.pallas import tpu as pltpu
from jax.sharding import PartitionSpec as P


INTERPRET = False
f32 = jnp.float32

spring_term = 0.5
stiff_floor = 0.001
crack_load = 4.0
tough_ratio = 0.5
length_term = 2.0
bulk_half = 0.5 * (1.5 + 2.0 / 3.0)

LX, LY, LZ = 16, 32, 128
ROWS, SHORT, DEPTH, OFF = 48, 40, 23, 3

SHIFT_U = 14.0
SHIFT_D = 18.0

VECTOR = (3, DEPTH, ROWS, LZ)
SCALAR = (DEPTH, ROWS, LZ)
BRIEF = (DEPTH, SHORT, LZ)


def call(kernel, outs, scratch=(), limit=8 << 20, aliases=None, hbm=False):
    vmem = pl.BlockSpec(memory_space=pltpu.VMEM)
    smem = pl.BlockSpec(memory_space=pltpu.SMEM)

    def run(*args, flags=None):
        specs = [pl.BlockSpec(memory_space=pl.ANY) if hbm else vmem] * len(args)
        if flags is not None:
            args, specs = (*args, flags), specs + [smem]
        return pl.pallas_call(
            kernel,
            out_shape=[jax.ShapeDtypeStruct(s, f32) for s in outs],
            in_specs=specs,
            out_specs=[vmem] * len(outs),
            scratch_shapes=[pltpu.VMEM(s, f32) if isinstance(s, tuple) else s for s in scratch],
            input_output_aliases=aliases or {},
            compiler_params=pltpu.CompilerParams(vmem_limit_bytes=limit),
            interpret=INTERPRET,
        )(*args)

    return run


def roll(x, shift, axis):
    return pltpu.roll(x, shift % x.shape[axis], axis)


def next_row(x):
    return roll(x, -1, 0)


def last_row(x):
    return roll(x, 1, 0)


def lanes(shape):
    return lax.broadcasted_iota(jnp.int32, shape, 1)


def next_lane(x):
    return jnp.where(lanes(x.shape) == LZ - 1, 0.0, roll(x, -1, 1))


def last_lane(x):
    return jnp.where(lanes(x.shape) == 0, 0.0, roll(x, 1, 1))


def tile_row():
    return lax.broadcasted_iota(jnp.int32, (8, LZ), 0)


def pack_first(u, load, damage, past):
    row = tile_row()
    tiles = [jnp.where(row == 7, roll(past, 7 - j, 0), u[j]) for j in range(3)]
    return tiles + [jnp.where(row < 6, load[j], roll(damage, 6 - 2 * j, 0)) for j in range(3)]


def pack_last(u, load, damage, past):
    row = tile_row()
    return list(u) + [
        jnp.where(row < 4, roll(damage, 4, 0), load[0]),
        jnp.where(row < 4, damage, load[1]),
        jnp.where(row < 4, roll(past, 4, 0), load[2]),
    ]


def damage_tiles(high, low, k):
    row = tile_row()
    above = jnp.where(row < 2, roll(high[3, k], 2, 0), roll(high[4, k], 4, 0))
    above = jnp.where(row < 4, above, roll(high[5, k], 6, 0))
    below = jnp.where(row < 4, low[4, k], roll(low[3, k], 4, 0))
    return above, below


def past_tile(high, low, k):
    row = tile_row()
    above = jnp.where(row < 1, roll(high[0, k], 1, 0), roll(high[1, k], 2, 0))
    above = jnp.where(row < 2, above, roll(high[2, k], 3, 0))
    return jnp.where(row < 4, above, roll(low[5, k], 4, 0))


def brief(above, below):
    return jnp.where(tile_row() < 4, above, below)


def row_mask(flags):
    row = lax.broadcasted_iota(jnp.int32, (ROWS - LY, LZ), 0)
    return jnp.where(row < 8, flags[3], flags[2])


def pack_rows_kernel(
    disp, force, damage, history, crack, first, last, top, bottom, top_crack, bottom_crack, sem
):
    copies = []
    for rows, into, into_crack in ((0, top, top_crack), (24, bottom, bottom_crack)):
        for source, target in (
            (disp.at[:, :, rows : rows + 8], into.at[0:3]),
            (force.at[:, :, rows : rows + 8], into.at[3:6]),
            (damage.at[:, rows : rows + 8], into.at[6]),
            (history.at[:, rows : rows + 8], into.at[7]),
            (crack.at[:, rows : rows + 8], into_crack),
        ):
            copies.append(pltpu.make_async_copy(source, target, sem.at[len(copies)]))
    for copy in copies:
        copy.start()
    for copy in copies:
        copy.wait()

    def step(k, carry):
        for into, flag, out, pack in (
            (top, top_crack, first, pack_first),
            (bottom, bottom_crack, last, pack_last),
        ):
            past = jnp.maximum(into[7, k], crack_load * flag[k].astype(f32))
            tiles = pack(
                [into[j, k] for j in range(3)], [into[3 + j, k] for j in range(3)],
                into[6, k], past,
            )
            for at, tile in enumerate(tiles):
                out[at, k] = tile
        return carry

    lax.fori_loop(0, LX, step, 0, unroll=2)


def pack_layers_kernel(disp, force, damage, high, low, first, last):
    at = {True: 0, False: 0}
    for field in range(7):
        own = disp.at[field] if field < 3 else force.at[field - 3] if field < 6 else damage
        ahead, behind = (3, 2) if 3 <= field < 6 else (4, 3)
        for c in (*range(ahead), *range(LX - behind, LX)):
            out, front = (first, True) if c < ahead else (last, False)
            if field < 6:
                above, below = high[field, c], low[field, c]
            else:
                above, below = damage_tiles(high, low, c)
            out[at[front], 0:LY] = own[c]
            out[at[front], LY : LY + 8] = above
            out[at[front], LY + 8 : ROWS] = below
            at[front] += 1


def stress(u, n, gain):
    dx = [n[j] - u[j] for j in range(3)]
    dy = [next_row(u[j]) - u[j] for j in range(3)]
    dz = [next_lane(u[j]) - u[j] for j in range(3)]
    twice = gain + gain
    part = 0.75 * (dx[0] + dy[1] + dz[2])
    return (
        twice * (dx[0] + part),
        twice * (dy[1] + part),
        twice * (dz[2] + part),
        gain * (dx[1] + dy[0]),
        gain * (dx[2] + dz[0]),
        gain * (dy[2] + dz[1]),
    )


def divergence(u, s, before, diag):
    s00, s11, s22, s01, s02, s12 = s
    return (
        diag * u[0] + before[0] + last_row(s01) + last_lane(s02) - (s00 + s01 + s02),
        diag * u[1] + before[1] + last_row(s11) + last_lane(s12) - (s01 + s11 + s12),
        diag * u[2] + before[2] + last_row(s12) + last_lane(s22) - (s02 + s12 + s22),
    )


def vector(ref, i):
    return tuple(ref[j, i] for j in range(3))


def sweep(source, gain, begin, end, diag, store, unroll=None):
    u, n = vector(source, begin), vector(source, begin + 1)
    s = stress(u, n, gain[begin])

    def step(i, carry):
        before, u = carry
        n = vector(source, i + 1)
        s = stress(u, n, gain[i])
        store(i, divergence(u, s, before, diag))
        return (s[0], s[3], s[4]), n

    carry = ((s[0], s[3], s[4]), n)
    if unroll is None:
        for i in range(begin + 1, end):
            carry = step(i, carry)
    else:
        lax.fori_loop(begin + 1, end, step, carry, unroll=unroll)


def store_to(ref, mask, flag=None, load=None):
    def store(i, image):
        for j in range(3):
            value = image[j] if load is None else load(j, i) - image[j]
            own, rest = value[0:LY], value[LY:ROWS] * mask
            if flag is not None:
                own, rest = own * flag, rest * flag
            ref[j, i, 0:LY] = own
            ref[j, i, LY:ROWS] = rest

    return store


def fold(x):
    return x[0:8] + x[8:16] + x[16:24] + x[24:32]


def moments_out(out, sums):
    lane = lanes((1, LZ))
    row = jnp.zeros((1, LZ), f32)
    for k, value in enumerate(sums):
        total = jnp.sum(jnp.sum(value, axis=0, keepdims=True), axis=1, keepdims=True)
        row = jnp.where(lane == k, total, row)
    out[...] = jnp.broadcast_to(row, out.shape)


def elastic_moments(v0, v1, v2, gain):
    def add(i, acc):
        u = vector(v2, i)
        up = [next_row(x)[0:LY] for x in u]
        u = [x[0:LY] for x in u]
        dx = [v2[j, i + 1, 0:LY] - u[j] for j in range(3)]
        dy = [up[j] - u[j] for j in range(3)]
        dz = [next_lane(u[j]) - u[j] for j in range(3)]
        trace = dx[0] + dy[1] + dz[2]
        e01, e02, e12 = dx[1] + dy[0], dx[2] + dz[0], dy[2] + dz[1]
        work = 2.0 * (dx[0] * dx[0] + dy[1] * dy[1] + dz[2] * dz[2])
        work = work + 1.5 * (trace * trace) + (e01 * e01 + e02 * e02 + e12 * e12)
        work = gain[i, 0:LY] * work
        a = [v0[j, i, 0:LY] for j in range(3)]
        b = [v1[j, i, 0:LY] for j in range(3)]

        def dot(x, y):
            return x[0] * y[0] + x[1] * y[1] + x[2] * y[2]

        square = dot(u, u)
        new = (
            dot(a, a), dot(a, b), dot(b, b), dot(b, u), square,
            work + (spring_term - SHIFT_U) * square,
        )
        return tuple(x + fold(y) for x, y in zip(acc, new))

    return add


def inner_kernel(
    disp, force, damage, history, crack, high, low, flags,
    wide, load, gain, v0, v1, v2, short_damage, past, partial,
):
    mask = row_mask(flags)

    def assemble(k, carry):
        i = OFF + k
        for j in range(3):
            wide[j, i, 0:LY] = disp[j, k]
            wide[j, i, LY : LY + 8] = high[j, k]
            wide[j, i, LY + 8 : ROWS] = low[j, k]
            load[j, k, 0:LY] = force[j, k]
            load[j, k, LY : LY + 8] = high[3 + j, k]
            load[j, k, LY + 8 : ROWS] = low[3 + j, k]
        own = damage[k]
        above, below = damage_tiles(high, low, k)
        short_damage[i, 0:LY] = own
        short_damage[i, LY:SHORT] = brief(above, below)
        left = 1.0 - own
        gain[i, 0:LY] = left * left + stiff_floor
        left = 1.0 - above
        gain[i, LY : LY + 8] = (left * left + stiff_floor) * mask[0:8]
        left = 1.0 - below
        gain[i, LY + 8 : ROWS] = (left * left + stiff_floor) * mask[8:16]
        past[k, 0:LY] = jnp.maximum(history[k], crack_load * crack[k].astype(f32))
        past[k, LY:SHORT] = past_tile(high, low, k)
        return carry

    lax.fori_loop(0, LX, assemble, 0, unroll=2)
    diag = spring_term - SHIFT_U
    first = store_to(v0, mask, load=lambda j, i: load[j, i - OFF])
    sweep(wide, gain, OFF, OFF + 15, spring_term, first, unroll=UNROLL)
    sweep(v0, gain, OFF + 1, OFF + 14, diag, store_to(v1, mask), unroll=UNROLL)
    sweep(v1, gain, OFF + 2, OFF + 13, diag, store_to(v2, mask), unroll=UNROLL)
    zero = jnp.zeros((8, LZ), f32)
    add = elastic_moments(v0, v1, v2, gain)
    for k, value in enumerate(
        lax.fori_loop(OFF + 3, OFF + 12, add, (zero,) * 6, unroll=3)
    ):
        partial[k] = value


UNROLL = 4


def outer_kernel(
    wide_in, load, gain_in, v0_in, v1_in, v2_in, short_in, past, partial,
    layers_high, layers_low, flags,
    wide, gain, v0, v1, v2, short_damage, sums, first, last,
):
    mask = row_mask(flags)
    for j in range(3):
        wide[j, OFF + LX : DEPTH] = layers_high[4 * j : 4 * j + 4]
        wide[j, 0:OFF] = layers_low[3 * j : 3 * j + 3]
    for side, count, at, base, flag in (
        (layers_high, 4, OFF + LX, 21, flags[1]), (layers_low, 3, 0, 15, flags[0])
    ):
        for c in range(count):
            value = side[base + c]
            short_damage[at + c, 0:LY] = value[0:LY]
            short_damage[at + c, LY:SHORT] = brief(value[LY : LY + 8], value[LY + 8 : ROWS])
            left = 1.0 - value
            value = (left * left + stiff_floor) * flag
            gain[at + c, 0:LY] = value[0:LY]
            gain[at + c, LY:ROWS] = value[LY:ROWS] * mask

    def force_at(j, i):
        if i < OFF:
            return layers_low[9 + 2 * j + i - 1]
        if i >= OFF + LX:
            return layers_high[12 + 3 * j + i - OFF - LX]
        return load[j, i - OFF]

    def both(source, target, low_end, high_begin, diag, load=None):
        def store(i, image):
            flag = flags[0] if i < OFF else flags[1] if i >= OFF + LX else None
            store_to(target, mask, flag, load)(i, image)

        begin = low_end - 4
        sweep(source, gain, begin, low_end, diag, store)
        sweep(source, gain, high_begin, high_begin + 5, diag, store)

    diag = spring_term - SHIFT_U
    both(wide, v0, OFF + 1, OFF + 14, spring_term, force_at)
    both(v0, v1, OFF + 2, OFF + 13, diag)
    both(v1, v2, OFF + 3, OFF + 12, diag)

    add = elastic_moments(v0, v1, v2, gain)
    acc = tuple(partial[k] for k in range(6))
    for i in (*range(OFF, OFF + 3), *range(OFF + 12, OFF + 16)):
        acc = add(i, acc)
    moments_out(sums, acc)

    def put(out, at, ref, j, c):
        out[at, 0:LY] = ref[j, OFF + c, 0:LY]
        out[at, LY:SHORT] = brief(ref[j, OFF + c, LY : LY + 8], ref[j, OFF + c, LY + 8 : ROWS])

    for j in range(3):
        put(first, j, v0, j, 3)
        for c in range(2):
            put(first, 3 + 2 * j + c, v1, j, 2 + c)
            put(last, 3 + 2 * j + c, v2, j, 14 + c)
        for c in range(3):
            put(first, 9 + 3 * j + c, v2, j, 1 + c)
        put(last, j, v1, j, 14)
    first[18:21] = past[0:3]
    last[9:11] = past[14:16]


def coefficients(gathered, shift):
    row = jnp.sum(gathered[...], axis=0, keepdims=True)
    lane = lanes((1, LZ))
    mu = [
        jnp.broadcast_to(
            jnp.sum(jnp.where(lane == k, row, 0.0), axis=1, keepdims=True), (1, LZ)
        )
        for k in range(6)
    ]

    def inner(a, b, up=0):
        total = None
        for i, x in enumerate(a):
            for j, y in enumerate(b):
                term = x * y * mu[i + j + up]
                total = term if total is None else total + term
        return total

    one = jnp.ones((1, LZ), f32)
    resid, direction = [one], [one]
    found = []
    norm = mu[0]
    for number in range(3):
        work = inner(direction, direction, 1) + shift * inner(direction, direction)
        alpha = norm / work
        for i, x in enumerate(direction):
            if i < len(found):
                found[i] = found[i] + alpha * x
            else:
                found.append(alpha * x)
        if number < 2:
            image = [shift * x for x in direction] + [jnp.zeros((1, LZ), f32)]
            for i, x in enumerate(direction):
                image[i + 1] = image[i + 1] + x
            resid = [
                (resid[i] if i < len(resid) else 0.0) - alpha * x for i, x in enumerate(image)
            ]
            new = inner(resid, resid)
            ratio = new / norm
            direction = [
                x + ratio * direction[i] if i < len(direction) else x
                for i, x in enumerate(resid)
            ]
            norm = new
    return found


def damage_kernel(
    gathered, wide, v0, v1, v2, short_damage, past, high, low, flags,
    moved, found, w0, w1, w2, sums, now, drive,
):
    a0, a1, a2 = coefficients(gathered, SHIFT_U)

    def cut(value):
        return value[0:LY], brief(value[LY : LY + 8], value[LY + 8 : ROWS])

    def put(j, i, base, far):
        body, rest = cut(base)
        now[j, i, 0:LY] = body
        now[j, i, LY:SHORT] = rest
        if far is not None:
            now[j, i] = now[j, i] + far

    def middle(i, carry):
        for j in range(3):
            value = wide[j, i] + a0 * v0[j, i] + a1 * v1[j, i] + a2 * v2[j, i]
            put(j, i, value, None)
            moved[j, i - OFF] = value[0:LY]
        return carry

    lax.fori_loop(OFF, OFF + LX, middle, 0, unroll=2)
    for j in range(3):
        i = OFF + LX
        put(j, i, wide[j, i] + a0 * v0[j, i] + a1 * v1[j, i] + a2 * v2[j, i], None)
        i = OFF - 2
        put(j, i, wide[j, i] + a0 * v0[j, i], a1 * low[j] + a2 * low[3 + 2 * j])
        i = OFF - 1
        put(j, i, wide[j, i] + a0 * v0[j, i] + a1 * v1[j, i], a2 * low[4 + 2 * j])
        i = OFF + LX + 1
        put(j, i, wide[j, i] + a0 * v0[j, i] + a1 * v1[j, i], a2 * high[9 + 3 * j])
        i = OFF + LX + 2
        put(j, i, wide[j, i] + a0 * v0[j, i], a1 * high[3 + 2 * j] + a2 * high[10 + 3 * j])
        i = OFF + LX + 3
        far = a0 * high[j] + a1 * high[4 + 2 * j] + a2 * high[11 + 3 * j]
        put(j, i, wide[j, i], far)

    row = lax.broadcasted_iota(jnp.int32, (8, LZ), 0)
    mask = jnp.where(row < 4, flags[3], flags[2])

    def energy(i):
        u, n = vector(now, i), vector(now, i + 1)
        dx = [n[j] - u[j] for j in range(3)]
        dy = [next_row(u[j]) - u[j] for j in range(3)]
        dz = [next_lane(u[j]) - u[j] for j in range(3)]
        trace = dx[0] + dy[1] + dz[2]
        e01, e02, e12 = dx[1] + dy[0], dx[2] + dz[0], dy[2] + dz[1]
        squares = dx[0] * dx[0] + dy[1] * dy[1] + dz[2] * dz[2]
        squares = squares + 0.5 * (e01 * e01 + e02 * e02 + e12 * e12)
        positive = jnp.maximum(trace, 0.0)
        return bulk_half * (positive * positive) + (squares - trace * trace * (1.0 / 3.0))

    def step(i, carry):
        value = jnp.maximum(past[i - OFF], energy(i))
        drive[i] = value
        found[i - OFF] = value[0:LY]
        return carry

    lax.fori_loop(OFF, OFF + LX, step, 0, unroll=4)
    for c in range(3):
        i = OFF + LX + c
        drive[i] = jnp.maximum(high[18 + c], energy(i))
    for c in range(2):
        i = OFF - 2 + c
        drive[i] = jnp.maximum(low[9 + c], energy(i))

    def flag_of(i):
        return jnp.where(i < OFF, flags[0], jnp.where(i >= OFF + LX, flags[1], 1.0))

    def apply(source, begin, end, make, target):
        def step(i, carry):
            before, here = carry
            n = source[i + 1]
            beside = before + n + next_row(here) + last_row(here)
            beside = beside + next_lane(here) + last_lane(here)
            value = make(i, here, beside) * flag_of(i)
            target[i, 0:LY] = value[0:LY]
            target[i, LY:SHORT] = value[LY:SHORT] * mask
            return here, n

        lax.fori_loop(begin, end, step, (source[begin - 1], source[begin]), unroll=4)

    full = tough_ratio + 6.0 * length_term

    def start(i, here, beside):
        twice = 2.0 * drive[i]
        return twice - ((full + twice) * here - length_term * beside)

    def image(i, here, beside):
        return ((full - SHIFT_D) + 2.0 * drive[i]) * here - length_term * beside

    apply(short_damage, OFF - 2, OFF + LX + 3, start, w0)
    apply(w0, OFF - 1, OFF + LX + 2, image, w1)
    apply(w1, OFF, OFF + LX + 1, image, w2)

    lane = lanes((LY, LZ))
    row = lax.broadcasted_iota(jnp.int32, (LY, LZ), 0)
    edge = jnp.where(lane == 0, length_term, 0.0)
    edge = edge + jnp.where(row == 0, length_term * (1.0 - flags[2]), 0.0)
    edge = edge + (tough_ratio - SHIFT_D)

    def add(i, acc):
        wide_now = w2[i]
        u = wide_now[0:LY]
        dx = w2[i + 1, 0:LY] - u
        dy = next_row(wide_now)[0:LY] - u
        dz = next_lane(u) - u
        side = jnp.where(i == OFF, length_term * (1.0 - flags[0]), 0.0)
        square = u * u
        work = (edge + side + 2.0 * drive[i, 0:LY]) * square
        work = work + length_term * (dx * dx + dy * dy + dz * dz)
        a, b = w0[i, 0:LY], w1[i, 0:LY]
        new = (a * a, a * b, b * b, b * u, square, work)
        return tuple(x + fold(y) for x, y in zip(acc, new))

    zero = jnp.zeros((8, LZ), f32)
    moments_out(sums, lax.fori_loop(OFF, OFF + LX, add, (zero,) * 6, unroll=4))


def update_kernel(gathered, damage, w0, w1, w2, out):
    b0, b1, b2 = coefficients(gathered, SHIFT_D)

    def step(c, carry):
        i = OFF + c
        image = b0 * w0[i, 0:LY] + b1 * w1[i, 0:LY] + b2 * w2[i, 0:LY]
        out[c] = damage[c] + image
        return carry

    lax.fori_loop(0, LX, step, 0, unroll=2)


def exchange(first, last, axis):
    size = lax.axis_size(axis)
    up = [(i, i + 1) for i in range(size - 1)]
    down = [(b, a) for a, b in up]
    high = lax.ppermute(first, axis, down)
    low = lax.ppermute(last, axis, up)
    return high, low


def step(displacement, force, damage, history, crack_flags):
    axes = ("gx", "gy")
    count = lax.axis_size(axes)
    ix, iy = lax.axis_index("gx"), lax.axis_index("gy")
    flags = jnp.stack(
        [ix > 0, ix < lax.axis_size("gx") - 1, iy > 0, iy < lax.axis_size("gy") - 1]
    ).astype(f32)

    def gather(sums):
        return lax.all_to_all(sums, axes, 0, 0, tiled=True)

    edge_rows = (8, LX, 8, LZ)
    rows = call(
        pack_rows_kernel,
        [(6, LX, 8, LZ)] * 2,
        [
            edge_rows, edge_rows,
            pltpu.VMEM((LX, 8, LZ), jnp.int32), pltpu.VMEM((LX, 8, LZ), jnp.int32),
            pltpu.SemaphoreType.DMA((10,)),
        ],
        hbm=True,
    )(displacement, force, damage, history, crack_flags)
    high, low = exchange(*rows, "gy")
    layers = call(pack_layers_kernel, [(25, ROWS, LZ), (18, ROWS, LZ)])(
        displacement, force, damage, high, low
    )
    layers_high, layers_low = exchange(*layers, "gx")
    wide, load, gain, v0, v1, v2, short_damage, past, partial = call(
        inner_kernel,
        [VECTOR, (3, LX, ROWS, LZ), SCALAR, VECTOR, VECTOR, VECTOR, BRIEF]
        + [(LX, SHORT, LZ), (6, 8, LZ)],
    )(displacement, force, damage, history, crack_flags, high, low, flags=flags)
    wide, gain, v0, v1, v2, short_damage, sums, first, last = call(
        outer_kernel,
        [VECTOR, SCALAR, VECTOR, VECTOR, VECTOR, BRIEF]
        + [(count, LZ), (21, SHORT, LZ), (11, SHORT, LZ)],
        aliases={0: 0, 2: 1, 3: 2, 4: 3, 5: 4, 6: 5},
    )(
        wide, load, gain, v0, v1, v2, short_damage, past, partial,
        layers_high, layers_low, flags=flags,
    )
    high, low = exchange(first, last, "gx")
    gathered = gather(sums)
    moved, found, w0, w1, w2, sums = call(
        damage_kernel,
        [(3, LX, LY, LZ), (LX, LY, LZ), BRIEF, BRIEF, BRIEF, (count, LZ)],
        [(3, DEPTH, SHORT, LZ), BRIEF],
    )(gathered, wide, v0, v1, v2, short_damage, past, high, low, flags=flags)
    (damage_out,) = call(update_kernel, [(LX, LY, LZ)])(
        gather(sums), damage, w0, w1, w2
    )
    return moved, damage_out, found


def solution(mesh):
    return jax.shard_map(
        step,
        mesh=mesh,
        in_specs=(
            P(None, "gx", "gy", None),
            P(None, "gx", "gy", None),
            P("gx", "gy", None),
            P("gx", "gy", None),
            P("gx", "gy", None),
        ),
        out_specs=(P(None, "gx", "gy", None), P("gx", "gy", None), P("gx", "gy", None)),
        check_vma=False,
    )
```

```python
import jax
import jax.numpy as jnp
from jax import lax
from jax.experimental import pallas as pl
from jax.experimental.pallas import tpu as pltpu
from jax.sharding import PartitionSpec as P


INTERPRET = False
f32 = jnp.float32

spring_term = 0.5
stiff_floor = 0.001
crack_load = 4.0
tough_ratio = 0.5
length_term = 2.0
bulk_half = 0.5 * (1.5 + 2.0 / 3.0)

LX, LY, LZ = 16, 32, 128
ROWS, SHORT, DEPTH, OFF = 48, 40, 23, 3

SHIFT_U = 14.0
SHIFT_D = 18.0

VECTOR = (3, DEPTH, ROWS, LZ)
SCALAR = (DEPTH, ROWS, LZ)
BRIEF = (DEPTH, SHORT, LZ)


def fast(shape):
    if INTERPRET:
        return jax.ShapeDtypeStruct(shape, f32)
    return pltpu.VMEM(shape, f32)


def whole(*shape):
    return jax.ShapeDtypeStruct(shape, f32)


def call(kernel, outs, scratch=(), limit=8 << 20, aliases=None, hbm=False):
    vmem = pl.BlockSpec(memory_space=pltpu.VMEM)
    smem = pl.BlockSpec(memory_space=pltpu.SMEM)

    def run(*args, flags=None):
        specs = [pl.BlockSpec(memory_space=pltpu.HBM) if hbm else vmem] * len(args)
        if hbm and not INTERPRET:
            args = [pltpu.with_memory_space_constraint(x, pltpu.HBM) for x in args]
        if flags is not None:
            args, specs = (*args, flags), specs + [smem]
        return pl.pallas_call(
            kernel,
            out_shape=[s if isinstance(s, jax.ShapeDtypeStruct) else fast(s) for s in outs],
            in_specs=specs,
            out_specs=[vmem] * len(outs),
            scratch_shapes=[pltpu.VMEM(s, f32) if isinstance(s, tuple) else s for s in scratch],
            input_output_aliases=aliases or {},
            compiler_params=pltpu.CompilerParams(vmem_limit_bytes=limit),
            interpret=INTERPRET,
        )(*args)

    return run


def roll(x, shift, axis):
    return pltpu.roll(x, shift % x.shape[axis], axis)


def next_row(x):
    return roll(x, -1, 0)


def last_row(x):
    return roll(x, 1, 0)


def lanes(shape):
    return lax.broadcasted_iota(jnp.int32, shape, 1)


def next_lane(x):
    return jnp.where(lanes(x.shape) == LZ - 1, 0.0, roll(x, -1, 1))


def last_lane(x):
    return jnp.where(lanes(x.shape) == 0, 0.0, roll(x, 1, 1))


def tile_row():
    return lax.broadcasted_iota(jnp.int32, (8, LZ), 0)


def pack_first(u, load, damage, past):
    row = tile_row()
    tiles = [jnp.where(row == 7, roll(past, 7 - j, 0), u[j]) for j in range(3)]
    return tiles + [jnp.where(row < 6, load[j], roll(damage, 6 - 2 * j, 0)) for j in range(3)]


def pack_last(u, load, damage, past):
    row = tile_row()
    return list(u) + [
        jnp.where(row < 4, roll(damage, 4, 0), load[0]),
        jnp.where(row < 4, damage, load[1]),
        jnp.where(row < 4, roll(past, 4, 0), load[2]),
    ]


def damage_tiles(high, low, k):
    row = tile_row()
    above = jnp.where(row < 2, roll(high[3, k], 2, 0), roll(high[4, k], 4, 0))
    above = jnp.where(row < 4, above, roll(high[5, k], 6, 0))
    below = jnp.where(row < 4, low[4, k], roll(low[3, k], 4, 0))
    return above, below


def past_tile(high, low, k):
    row = tile_row()
    above = jnp.where(row < 1, roll(high[0, k], 1, 0), roll(high[1, k], 2, 0))
    above = jnp.where(row < 2, above, roll(high[2, k], 3, 0))
    return jnp.where(row < 4, above, roll(low[5, k], 4, 0))


def brief(above, below):
    return jnp.where(tile_row() < 4, above, below)


def row_mask(flags):
    row = lax.broadcasted_iota(jnp.int32, (ROWS - LY, LZ), 0)
    return jnp.where(row < 8, flags[3], flags[2])


AHEAD = (4, 4, 4, 3, 3, 3, 4)
BEHIND = (3, 3, 3, 2, 2, 2, 3)
AHEAD_AT = tuple(sum(AHEAD[:k]) for k in range(7))
BEHIND_AT = tuple(sum(BEHIND[:k]) for k in range(7))


def pack_kernel(
    disp, force, damage, history, crack,
    first, last, front, back, front_first, front_last, back_first, back_last,
    top, bottom, top_crack, bottom_crack, sem,
):
    fields = [disp.at[j] for j in range(3)] + [force.at[j] for j in range(3)] + [damage]
    near, far = [], []
    for rows, into, into_crack in ((0, top, top_crack), (24, bottom, bottom_crack)):
        near += [
            (disp.at[:, :, rows : rows + 8], into.at[0:3]),
            (force.at[:, :, rows : rows + 8], into.at[3:6]),
            (damage.at[:, rows : rows + 8], into.at[6]),
            (history.at[:, rows : rows + 8], into.at[7]),
            (crack.at[:, rows : rows + 8], into_crack),
        ]
    for k, field in enumerate(fields):
        at = AHEAD_AT[k]
        far.append((field.at[0 : AHEAD[k]], front.at[at : at + AHEAD[k]]))
        at = BEHIND_AT[k]
        far.append((field.at[LX - BEHIND[k] : LX], back.at[at : at + BEHIND[k]]))
    copies = [
        pltpu.make_async_copy(source, target, sem.at[n])
        for n, (source, target) in enumerate(near + far)
    ]
    for copy in copies:
        copy.start()
    for copy in copies[: len(near)]:
        copy.wait()

    def step(k, carry):
        for into, flag, out, pack in (
            (top, top_crack, first, pack_first),
            (bottom, bottom_crack, last, pack_last),
        ):
            past = jnp.maximum(into[7, k], crack_load * flag[k].astype(f32))
            tiles = pack(
                [into[j, k] for j in range(3)], [into[3 + j, k] for j in range(3)],
                into[6, k], past,
            )
            for at, tile in enumerate(tiles):
                out[at, k] = tile
        return carry

    lax.fori_loop(0, LX, step, 0, unroll=2)
    for k in range(7):
        at = AHEAD_AT[k]
        front_first[at : at + AHEAD[k]] = top[k, 0 : AHEAD[k]]
        front_last[at : at + AHEAD[k]] = bottom[k, 0 : AHEAD[k]]
        at = BEHIND_AT[k]
        back_first[at : at + BEHIND[k]] = top[k, LX - BEHIND[k] : LX]
        back_last[at : at + BEHIND[k]] = bottom[k, LX - BEHIND[k] : LX]
    for copy in copies[len(near) :]:
        copy.wait()


def stress(u, n, gain):
    dx = [n[j] - u[j] for j in range(3)]
    dy = [next_row(u[j]) - u[j] for j in range(3)]
    dz = [next_lane(u[j]) - u[j] for j in range(3)]
    twice = gain + gain
    part = 0.75 * (dx[0] + dy[1] + dz[2])
    return (
        twice * (dx[0] + part),
        twice * (dy[1] + part),
        twice * (dz[2] + part),
        gain * (dx[1] + dy[0]),
        gain * (dx[2] + dz[0]),
        gain * (dy[2] + dz[1]),
    )


def divergence(u, s, before, diag):
    s00, s11, s22, s01, s02, s12 = s
    return (
        diag * u[0] + before[0] + last_row(s01) + last_lane(s02) - (s00 + s01 + s02),
        diag * u[1] + before[1] + last_row(s11) + last_lane(s12) - (s01 + s11 + s12),
        diag * u[2] + before[2] + last_row(s12) + last_lane(s22) - (s02 + s12 + s22),
    )


def vector(ref, i):
    return tuple(ref[j, i] for j in range(3))


def sweep(source, gain, begin, end, diag, store, unroll=None):
    u, n = vector(source, begin), vector(source, begin + 1)
    s = stress(u, n, gain[begin])

    def step(i, carry):
        before, u = carry
        n = vector(source, i + 1)
        s = stress(u, n, gain[i])
        store(i, divergence(u, s, before, diag))
        return (s[0], s[3], s[4]), n

    carry = ((s[0], s[3], s[4]), n)
    if unroll is None:
        for i in range(begin + 1, end):
            carry = step(i, carry)
    else:
        lax.fori_loop(begin + 1, end, step, carry, unroll=unroll)


def store_to(ref, mask, flag=None, load=None):
    def store(i, image):
        for j in range(3):
            value = image[j] if load is None else load(j, i) - image[j]
            own, rest = value[0:LY], value[LY:ROWS] * mask
            if flag is not None:
                own, rest = own * flag, rest * flag
            ref[j, i, 0:LY] = own
            ref[j, i, LY:ROWS] = rest

    return store


def fold(x):
    return x[0:8] + x[8:16] + x[16:24] + x[24:32]


def moments_out(out, sums):
    lane = lanes((1, LZ))
    row = jnp.zeros((1, LZ), f32)
    for k, value in enumerate(sums):
        total = jnp.sum(jnp.sum(value, axis=0, keepdims=True), axis=1, keepdims=True)
        row = jnp.where(lane == k, total, row)
    out[...] = jnp.broadcast_to(row, out.shape)


def elastic_moments(v0, v1, v2, gain):
    def add(i, acc):
        u = vector(v2, i)
        up = [next_row(x)[0:LY] for x in u]
        u = [x[0:LY] for x in u]
        dx = [v2[j, i + 1, 0:LY] - u[j] for j in range(3)]
        dy = [up[j] - u[j] for j in range(3)]
        dz = [next_lane(u[j]) - u[j] for j in range(3)]
        trace = dx[0] + dy[1] + dz[2]
        e01, e02, e12 = dx[1] + dy[0], dx[2] + dz[0], dy[2] + dz[1]
        work = 2.0 * (dx[0] * dx[0] + dy[1] * dy[1] + dz[2] * dz[2])
        work = work + 1.5 * (trace * trace) + (e01 * e01 + e02 * e02 + e12 * e12)
        work = gain[i, 0:LY] * work
        a = [v0[j, i, 0:LY] for j in range(3)]
        b = [v1[j, i, 0:LY] for j in range(3)]

        def dot(x, y):
            return x[0] * y[0] + x[1] * y[1] + x[2] * y[2]

        square = dot(u, u)
        new = (
            dot(a, a), dot(a, b), dot(b, b), dot(b, u), square,
            work + (spring_term - SHIFT_U) * square,
        )
        return tuple(x + fold(y) for x, y in zip(acc, new))

    return add


def inner_kernel(
    disp, force, damage, history, crack, high, low, flags,
    wide, load, gain, v0, v1, v2, short_damage, past, partial,
):
    mask = row_mask(flags)

    def assemble(k, carry):
        i = OFF + k
        for j in range(3):
            wide[j, i, 0:LY] = disp[j, k]
            wide[j, i, LY : LY + 8] = high[j, k] * flags[3]
            wide[j, i, LY + 8 : ROWS] = low[j, k] * flags[2]
            load[j, k, 0:LY] = force[j, k]
            load[j, k, LY : LY + 8] = high[3 + j, k]
            load[j, k, LY + 8 : ROWS] = low[3 + j, k]
        own = damage[k]
        above, below = damage_tiles(high, low, k)
        short_damage[i, 0:LY] = own
        short_damage[i, LY:SHORT] = brief(above * flags[3], below * flags[2])
        left = 1.0 - own
        gain[i, 0:LY] = left * left + stiff_floor
        left = 1.0 - above
        gain[i, LY : LY + 8] = (left * left + stiff_floor) * mask[0:8]
        left = 1.0 - below
        gain[i, LY + 8 : ROWS] = (left * left + stiff_floor) * mask[8:16]
        past[k, 0:LY] = jnp.maximum(history[k], crack_load * crack[k].astype(f32))
        past[k, LY:SHORT] = past_tile(high, low, k)
        return carry

    lax.fori_loop(0, LX, assemble, 0, unroll=2)
    diag = spring_term - SHIFT_U
    first = store_to(v0, mask, load=lambda j, i: load[j, i - OFF])
    sweep(wide, gain, OFF, OFF + 15, spring_term, first, unroll=UNROLL)
    sweep(v0, gain, OFF + 1, OFF + 14, diag, store_to(v1, mask), unroll=UNROLL)
    sweep(v1, gain, OFF + 2, OFF + 13, diag, store_to(v2, mask), unroll=UNROLL)
    zero = jnp.zeros((8, LZ), f32)
    add = elastic_moments(v0, v1, v2, gain)
    for k, value in enumerate(
        lax.fori_loop(OFF + 3, OFF + 12, add, (zero,) * 6, unroll=3)
    ):
        partial[k] = value


UNROLL = 4


def outer_kernel(
    wide_in, load, gain_in, v0_in, v1_in, v2_in, short_in, past, partial,
    ahead, ahead_high, ahead_low, behind, behind_high, behind_low, flags,
    wide, gain, v0, v1, v2, short_damage, sums, first, last, edge_load,
):
    mask = row_mask(flags)
    for counts, starts, at, middle, above, below, flag in (
        (AHEAD, AHEAD_AT, OFF + LX, ahead, ahead_high, ahead_low, flags[1]),
        (BEHIND, BEHIND_AT, OFF, behind, behind_high, behind_low, flags[0]),
    ):
        for k in range(7):
            begin = at if at > OFF else OFF - counts[k]
            for c in range(counts[k]):
                own = middle[starts[k] + c] * flag
                high = above[starts[k] + c] * (flag * flags[3])
                low = below[starts[k] + c] * (flag * flags[2])
                i = begin + c
                if k < 3:
                    into = wide.at[k, i]
                elif k < 6:
                    into = edge_load.at[k - 3, i - 1 if i < OFF else i - OFF - LX + 2]
                else:
                    into = gain.at[i]
                    short_damage[i, 0:LY] = own
                    short_damage[i, LY:SHORT] = brief(high, low)
                    own, high, low = ((1.0 - x) * (1.0 - x) + stiff_floor for x in (own, high, low))
                    own = own * flag
                    high = high * (mask[0:8] * flag)
                    low = low * (mask[8:16] * flag)
                into[0:LY] = own
                into[LY : LY + 8] = high
                into[LY + 8 : ROWS] = low

    def force_at(j, i):
        if i < OFF:
            return edge_load[j, i - 1]
        if i >= OFF + LX:
            return edge_load[j, i - OFF - LX + 2]
        return load[j, i - OFF]

    def both(source, target, low_end, high_begin, diag, load=None):
        def store(i, image):
            flag = flags[0] if i < OFF else flags[1] if i >= OFF + LX else None
            store_to(target, mask, flag, load)(i, image)

        begin = low_end - 4
        sweep(source, gain, begin, low_end, diag, store)
        sweep(source, gain, high_begin, high_begin + 5, diag, store)

    diag = spring_term - SHIFT_U
    both(wide, v0, OFF + 1, OFF + 14, spring_term, force_at)
    both(v0, v1, OFF + 2, OFF + 13, diag)
    both(v1, v2, OFF + 3, OFF + 12, diag)

    add = elastic_moments(v0, v1, v2, gain)
    acc = tuple(partial[k] for k in range(6))
    for i in (*range(OFF, OFF + 3), *range(OFF + 12, OFF + 16)):
        acc = add(i, acc)
    moments_out(sums, acc)

    def put(out, at, ref, j, c):
        out[at, 0:LY] = ref[j, OFF + c, 0:LY]
        out[at, LY:SHORT] = brief(ref[j, OFF + c, LY : LY + 8], ref[j, OFF + c, LY + 8 : ROWS])

    for j in range(3):
        put(first, j, v0, j, 3)
        for c in range(2):
            put(first, 3 + 2 * j + c, v1, j, 2 + c)
            put(last, 3 + 2 * j + c, v2, j, 14 + c)
        for c in range(3):
            put(first, 9 + 3 * j + c, v2, j, 1 + c)
        put(last, j, v1, j, 14)
    first[18:21] = past[0:3]
    last[9:11] = past[14:16]


def coefficients(gathered, shift):
    row = jnp.sum(gathered[...], axis=0, keepdims=True)
    lane = lanes((1, LZ))
    mu = [
        jnp.broadcast_to(
            jnp.sum(jnp.where(lane == k, row, 0.0), axis=1, keepdims=True), (1, LZ)
        )
        for k in range(6)
    ]

    def inner(a, b, up=0):
        total = None
        for i, x in enumerate(a):
            for j, y in enumerate(b):
                term = x * y * mu[i + j + up]
                total = term if total is None else total + term
        return total

    one = jnp.ones((1, LZ), f32)
    resid, direction = [one], [one]
    found = []
    norm = mu[0]
    for number in range(3):
        work = inner(direction, direction, 1) + shift * inner(direction, direction)
        alpha = norm / work
        for i, x in enumerate(direction):
            if i < len(found):
                found[i] = found[i] + alpha * x
            else:
                found.append(alpha * x)
        if number < 2:
            image = [shift * x for x in direction] + [jnp.zeros((1, LZ), f32)]
            for i, x in enumerate(direction):
                image[i + 1] = image[i + 1] + x
            resid = [
                (resid[i] if i < len(resid) else 0.0) - alpha * x for i, x in enumerate(image)
            ]
            new = inner(resid, resid)
            ratio = new / norm
            direction = [
                x + ratio * direction[i] if i < len(direction) else x
                for i, x in enumerate(resid)
            ]
            norm = new
    return found


def damage_kernel(
    gathered, wide, v0, v1, v2, short_damage, past, high, low, flags,
    moved, found, w0, w1, w2, sums, now, drive,
):
    a0, a1, a2 = coefficients(gathered, SHIFT_U)

    def cut(value):
        return value[0:LY], brief(value[LY : LY + 8], value[LY + 8 : ROWS])

    def put(j, i, base, far):
        body, rest = cut(base)
        now[j, i, 0:LY] = body
        now[j, i, LY:SHORT] = rest
        if far is not None:
            now[j, i] = now[j, i] + far

    def middle(i, carry):
        for j in range(3):
            value = wide[j, i] + a0 * v0[j, i] + a1 * v1[j, i] + a2 * v2[j, i]
            put(j, i, value, None)
            moved[j, i - OFF] = value[0:LY]
        return carry

    lax.fori_loop(OFF, OFF + LX, middle, 0, unroll=2)
    for j in range(3):
        i = OFF + LX
        put(j, i, wide[j, i] + a0 * v0[j, i] + a1 * v1[j, i] + a2 * v2[j, i], None)
        i = OFF - 2
        far = (a1 * low[j] + a2 * low[3 + 2 * j]) * flags[0]
        put(j, i, wide[j, i] + a0 * v0[j, i], far)
        i = OFF - 1
        far = (a2 * low[4 + 2 * j]) * flags[0]
        put(j, i, wide[j, i] + a0 * v0[j, i] + a1 * v1[j, i], far)
        i = OFF + LX + 1
        far = (a2 * high[9 + 3 * j]) * flags[1]
        put(j, i, wide[j, i] + a0 * v0[j, i] + a1 * v1[j, i], far)
        i = OFF + LX + 2
        far = (a1 * high[3 + 2 * j] + a2 * high[10 + 3 * j]) * flags[1]
        put(j, i, wide[j, i] + a0 * v0[j, i], far)
        i = OFF + LX + 3
        far = (a0 * high[j] + a1 * high[4 + 2 * j] + a2 * high[11 + 3 * j]) * flags[1]
        put(j, i, wide[j, i], far)

    row = lax.broadcasted_iota(jnp.int32, (8, LZ), 0)
    mask = jnp.where(row < 4, flags[3], flags[2])

    def energy(i):
        u, n = vector(now, i), vector(now, i + 1)
        dx = [n[j] - u[j] for j in range(3)]
        dy = [next_row(u[j]) - u[j] for j in range(3)]
        dz = [next_lane(u[j]) - u[j] for j in range(3)]
        trace = dx[0] + dy[1] + dz[2]
        e01, e02, e12 = dx[1] + dy[0], dx[2] + dz[0], dy[2] + dz[1]
        squares = dx[0] * dx[0] + dy[1] * dy[1] + dz[2] * dz[2]
        squares = squares + 0.5 * (e01 * e01 + e02 * e02 + e12 * e12)
        positive = jnp.maximum(trace, 0.0)
        return bulk_half * (positive * positive) + (squares - trace * trace * (1.0 / 3.0))

    def step(i, carry):
        value = jnp.maximum(past[i - OFF], energy(i))
        drive[i] = value
        found[i - OFF] = value[0:LY]
        return carry

    lax.fori_loop(OFF, OFF + LX, step, 0, unroll=4)
    for c in range(3):
        i = OFF + LX + c
        drive[i] = jnp.maximum(high[18 + c], energy(i))
    for c in range(2):
        i = OFF - 2 + c
        drive[i] = jnp.maximum(low[9 + c], energy(i))

    def flag_of(i):
        return jnp.where(i < OFF, flags[0], jnp.where(i >= OFF + LX, flags[1], 1.0))

    def apply(source, begin, end, make, target):
        def step(i, carry):
            before, here = carry
            n = source[i + 1]
            beside = before + n + next_row(here) + last_row(here)
            beside = beside + next_lane(here) + last_lane(here)
            value = make(i, here, beside) * flag_of(i)
            target[i, 0:LY] = value[0:LY]
            target[i, LY:SHORT] = value[LY:SHORT] * mask
            return here, n

        lax.fori_loop(begin, end, step, (source[begin - 1], source[begin]), unroll=4)

    full = tough_ratio + 6.0 * length_term

    def start(i, here, beside):
        twice = 2.0 * drive[i]
        return twice - ((full + twice) * here - length_term * beside)

    def image(i, here, beside):
        return ((full - SHIFT_D) + 2.0 * drive[i]) * here - length_term * beside

    apply(short_damage, OFF - 2, OFF + LX + 3, start, w0)
    apply(w0, OFF - 1, OFF + LX + 2, image, w1)
    apply(w1, OFF, OFF + LX + 1, image, w2)

    lane = lanes((LY, LZ))
    row = lax.broadcasted_iota(jnp.int32, (LY, LZ), 0)
    edge = jnp.where(lane == 0, length_term, 0.0)
    edge = edge + jnp.where(row == 0, length_term * (1.0 - flags[2]), 0.0)
    edge = edge + (tough_ratio - SHIFT_D)

    def add(i, acc):
        wide_now = w2[i]
        u = wide_now[0:LY]
        dx = w2[i + 1, 0:LY] - u
        dy = next_row(wide_now)[0:LY] - u
        dz = next_lane(u) - u
        side = jnp.where(i == OFF, length_term * (1.0 - flags[0]), 0.0)
        square = u * u
        work = (edge + side + 2.0 * drive[i, 0:LY]) * square
        work = work + length_term * (dx * dx + dy * dy + dz * dz)
        a, b = w0[i, 0:LY], w1[i, 0:LY]
        new = (a * a, a * b, b * b, b * u, square, work)
        return tuple(x + fold(y) for x, y in zip(acc, new))

    zero = jnp.zeros((8, LZ), f32)
    moments_out(sums, lax.fori_loop(OFF, OFF + LX, add, (zero,) * 6, unroll=4))


def update_kernel(gathered, damage, w0, w1, w2, out):
    b0, b1, b2 = coefficients(gathered, SHIFT_D)

    def step(c, carry):
        i = OFF + c
        image = b0 * w0[i, 0:LY] + b1 * w1[i, 0:LY] + b2 * w2[i, 0:LY]
        out[c] = damage[c] + image
        return carry

    lax.fori_loop(0, LX, step, 0, unroll=2)


def send(values, dx, dy):
    nx, ny = lax.axis_size("gx"), lax.axis_size("gy")
    if not dy:
        return lax.ppermute(values, "gx", [(i, (i + dx) % nx) for i in range(nx)])
    if not dx:
        return lax.ppermute(values, "gy", [(k, (k + dy) % ny) for k in range(ny)])
    pairs = [
        (i * ny + k, (i + dx) % nx * ny + (k + dy) % ny) for i in range(nx) for k in range(ny)
    ]
    return lax.ppermute(values, ("gx", "gy"), pairs)


def step(displacement, force, damage, history, crack_flags):
    axes = ("gx", "gy")
    count = lax.axis_size(axes)
    ix, iy = lax.axis_index("gx"), lax.axis_index("gy")
    flags = jnp.stack(
        [ix > 0, ix < lax.axis_size("gx") - 1, iy > 0, iy < lax.axis_size("gy") - 1]
    ).astype(f32)

    def gather(sums):
        return lax.all_to_all(sums, axes, 0, 0, tiled=True)

    edge_rows = (8, LX, 8, LZ)
    front, back = sum(AHEAD), sum(BEHIND)
    first, last, front_own, back_own, ff, fl, bf, bl = call(
        pack_kernel,
        [(6, LX, 8, LZ)] * 2
        + [(front, LY, LZ), (back, LY, LZ)]
        + [(front, 8, LZ)] * 2
        + [(back, 8, LZ)] * 2,
        [
            edge_rows, edge_rows,
            pltpu.VMEM((LX, 8, LZ), jnp.int32), pltpu.VMEM((LX, 8, LZ), jnp.int32),
            pltpu.SemaphoreType.DMA((24,)),
        ],
        hbm=True,
    )(displacement, force, damage, history, crack_flags)
    high = send(first, 0, -1)
    low = send(last, 0, 1)
    ahead, behind = send(front_own, -1, 0), send(back_own, 1, 0)
    ahead_high, ahead_low = send(ff, -1, -1), send(fl, -1, 1)
    behind_high, behind_low = send(bf, 1, -1), send(bl, 1, 1)
    wide, load, gain, v0, v1, v2, short_damage, past, partial = call(
        inner_kernel,
        [VECTOR, (3, LX, ROWS, LZ), SCALAR, VECTOR, VECTOR, VECTOR, BRIEF]
        + [(LX, SHORT, LZ), (6, 8, LZ)],
    )(displacement, force, damage, history, crack_flags, high, low, flags=flags)
    wide, gain, v0, v1, v2, short_damage, sums, first, last = call(
        outer_kernel,
        [VECTOR, SCALAR, VECTOR, VECTOR, VECTOR, BRIEF]
        + [(count, LZ), (21, SHORT, LZ), (11, SHORT, LZ)],
        scratch=[(3, 5, ROWS, LZ)],
        aliases={0: 0, 2: 1, 3: 2, 4: 3, 5: 4, 6: 5},
    )(
        wide, load, gain, v0, v1, v2, short_damage, past, partial,
        ahead, ahead_high, ahead_low, behind, behind_high, behind_low, flags=flags,
    )
    high = send(first, -1, 0)
    low = send(last, 1, 0)
    gathered = gather(sums)
    moved, found, w0, w1, w2, sums = call(
        damage_kernel,
        [whole(3, LX, LY, LZ), whole(LX, LY, LZ), BRIEF, BRIEF, BRIEF, (count, LZ)],
        [(3, DEPTH, SHORT, LZ), BRIEF],
    )(gathered, wide, v0, v1, v2, short_damage, past, high, low, flags=flags)
    (damage_out,) = call(update_kernel, [whole(LX, LY, LZ)])(
        gather(sums), damage, w0, w1, w2
    )
    return moved, damage_out, found


def solution(mesh):
    return jax.shard_map(
        step,
        mesh=mesh,
        in_specs=(
            P(None, "gx", "gy", None),
            P(None, "gx", "gy", None),
            P("gx", "gy", None),
            P("gx", "gy", None),
            P("gx", "gy", None),
        ),
        out_specs=(P(None, "gx", "gy", None), P("gx", "gy", None), P("gx", "gy", None)),
        check_vma=False,
    )
```

```python
import jax
import jax.numpy as jnp
from jax import lax
from jax.experimental import pallas as pl
from jax.experimental.pallas import tpu as pltpu
from jax.sharding import PartitionSpec as P


INTERPRET = False
f32 = jnp.float32

spring_term = 0.5
stiff_floor = 0.001
crack_load = 4.0
tough_ratio = 0.5
length_term = 2.0
bulk_half = 0.5 * (1.5 + 2.0 / 3.0)

LX, LY, LZ = 16, 32, 128
ROWS, SHORT, DEPTH, OFF = 48, 40, 28, 5

SHIFT_U = 14.0
SHIFT_D = 18.0

VECTOR = (3, DEPTH, ROWS, LZ)
SCALAR = (DEPTH, ROWS, LZ)
BRIEF = (DEPTH, SHORT, LZ)


def fast(shape):
    if INTERPRET:
        return jax.ShapeDtypeStruct(shape, f32)
    return pltpu.VMEM(shape, f32)


def whole(*shape):
    return jax.ShapeDtypeStruct(shape, f32)


def call(kernel, outs, scratch=(), limit=8 << 20, aliases=None, hbm=False):
    vmem = pl.BlockSpec(memory_space=pltpu.VMEM)
    smem = pl.BlockSpec(memory_space=pltpu.SMEM)

    def run(*args, flags=None):
        specs = [pl.BlockSpec(memory_space=pltpu.HBM) if hbm else vmem] * len(args)
        if hbm and not INTERPRET:
            args = [pltpu.with_memory_space_constraint(x, pltpu.HBM) for x in args]
        if flags is not None:
            args, specs = (*args, flags), specs + [smem]
        return pl.pallas_call(
            kernel,
            out_shape=[s if isinstance(s, jax.ShapeDtypeStruct) else fast(s) for s in outs],
            in_specs=specs,
            out_specs=[vmem] * len(outs),
            scratch_shapes=[pltpu.VMEM(s, f32) if isinstance(s, tuple) else s for s in scratch],
            input_output_aliases=aliases or {},
            compiler_params=pltpu.CompilerParams(vmem_limit_bytes=limit),
            interpret=INTERPRET,
        )(*args)

    return run


def roll(x, shift, axis):
    return pltpu.roll(x, shift % x.shape[axis], axis)


def next_row(x):
    return roll(x, -1, 0)


def last_row(x):
    return roll(x, 1, 0)


def lanes(shape):
    return lax.broadcasted_iota(jnp.int32, shape, 1)


def next_lane(x):
    return jnp.where(lanes(x.shape) == LZ - 1, 0.0, roll(x, -1, 1))


def last_lane(x):
    return jnp.where(lanes(x.shape) == 0, 0.0, roll(x, 1, 1))


def tile_row():
    return lax.broadcasted_iota(jnp.int32, (8, LZ), 0)


def pack_first(u, load, damage, past):
    row = tile_row()
    tiles = [jnp.where(row == 7, roll(past, 7 - j, 0), u[j]) for j in range(3)]
    return tiles + [jnp.where(row < 6, load[j], roll(damage, 6 - 2 * j, 0)) for j in range(3)]


def pack_last(u, load, damage, past):
    row = tile_row()
    return [
        jnp.where(row < 3, roll(damage, -1, 0), u[0]),
        jnp.where(row < 3, roll(past, 2, 0), u[1]),
        u[2],
        jnp.where(row < 4, roll(load[1], 4, 0), load[0]),
        jnp.where(row < 4, roll(damage, 4, 0), load[2]),
    ]


def low_tile(low, field, k):
    if field < 4:
        return low[field, k]
    return roll(low[3, k], 4, 0) if field == 4 else low[4, k]


def damage_tiles(high, low, k):
    row = tile_row()
    above = jnp.where(row < 2, roll(high[3, k], 2, 0), roll(high[4, k], 4, 0))
    above = jnp.where(row < 4, above, roll(high[5, k], 6, 0))
    below = jnp.where(row < 4, roll(low[0, k], 1, 0), roll(low[4, k], 4, 0))
    return above, below


def past_tile(high, low, k):
    row = tile_row()
    above = jnp.where(row < 1, roll(high[0, k], 1, 0), roll(high[1, k], 2, 0))
    above = jnp.where(row < 2, above, roll(high[2, k], 3, 0))
    return jnp.where(row < 4, above, roll(low[1, k], -2, 0))


def brief(above, below):
    return jnp.where(tile_row() < 4, above, below)


def row_mask(flags):
    row = lax.broadcasted_iota(jnp.int32, (ROWS - LY, LZ), 0)
    return jnp.where(row < 8, flags[3], flags[2])


AHEAD = (7, 7, 7, 6, 6, 6, 6, 3)
BEHIND = (5, 5, 5, 4, 4, 4, 5, 2)
AHEAD_AT = tuple(sum(AHEAD[:k]) for k in range(8))
BEHIND_AT = tuple(sum(BEHIND[:k]) for k in range(8))
FRONT, BACK = sum(AHEAD), sum(BEHIND)


def pack_kernel(
    disp, force, damage, history, crack,
    first, last, front, back,
    top, bottom, top_crack, bottom_crack, front_crack, back_crack, sem,
):
    fields = [disp.at[j] for j in range(3)] + [force.at[j] for j in range(3)]
    fields += [damage, history]
    near, far = [], []
    for rows, into, into_crack in ((0, top, top_crack), (24, bottom, bottom_crack)):
        near += [
            (disp.at[:, :, rows : rows + 8], into.at[0:3]),
            (force.at[:, :, rows : rows + 8], into.at[3:6]),
            (damage.at[:, rows : rows + 8], into.at[6]),
            (history.at[:, rows : rows + 8], into.at[7]),
            (crack.at[:, rows : rows + 8], into_crack),
        ]
    for k, field in enumerate(fields):
        at = AHEAD_AT[k]
        far.append((field.at[0 : AHEAD[k]], front.at[at : at + AHEAD[k]]))
        at = BEHIND_AT[k]
        far.append((field.at[LX - BEHIND[k] : LX], back.at[at : at + BEHIND[k]]))
    far.append((crack.at[0 : AHEAD[7]], front_crack))
    far.append((crack.at[LX - BEHIND[7] : LX], back_crack))
    copies = [
        pltpu.make_async_copy(source, target, sem.at[n])
        for n, (source, target) in enumerate(near + far)
    ]
    for copy in copies:
        copy.start()
    for copy in copies[: len(near)]:
        copy.wait()

    def step(k, carry):
        for into, flag, out, pack in (
            (top, top_crack, first, pack_first),
            (bottom, bottom_crack, last, pack_last),
        ):
            past = jnp.maximum(into[7, k], crack_load * flag[k].astype(f32))
            tiles = pack(
                [into[j, k] for j in range(3)], [into[3 + j, k] for j in range(3)],
                into[6, k], past,
            )
            for at, tile in enumerate(tiles):
                out[at, k] = tile
        return carry

    lax.fori_loop(0, LX, step, 0, unroll=2)
    for copy in copies[len(near) :]:
        copy.wait()
    for out, flag, at in ((front, front_crack, AHEAD_AT[7]), (back, back_crack, BEHIND_AT[7])):
        for c in range(flag.shape[0]):
            out[at + c] = jnp.maximum(out[at + c], crack_load * flag[c].astype(f32))


def corner_kernel(high, low, front, back):
    for counts, starts, out, begin in (
        (AHEAD, AHEAD_AT, front, 0), (BEHIND, BEHIND_AT, back, LX)
    ):
        for k in range(8):
            for c in range(counts[k]):
                at = starts[k] + c
                layer = c if begin == 0 else LX - counts[k] + c
                if k < 6:
                    out[at, 0:8] = high[k, layer]
                    out[at, 8:16] = low_tile(low, k, layer)
                elif k == 6:
                    above, below = damage_tiles(high, low, layer)
                    out[at, 0:8] = above
                    out[at, 8:16] = below
                else:
                    out[at, 0:8] = past_tile(high, low, layer)
                    out[at, 8:16] = jnp.zeros((8, LZ), f32)


def stress(u, n, gain):
    dx = [n[j] - u[j] for j in range(3)]
    dy = [next_row(u[j]) - u[j] for j in range(3)]
    dz = [next_lane(u[j]) - u[j] for j in range(3)]
    twice = gain + gain
    part = 0.75 * (dx[0] + dy[1] + dz[2])
    return (
        twice * (dx[0] + part),
        twice * (dy[1] + part),
        twice * (dz[2] + part),
        gain * (dx[1] + dy[0]),
        gain * (dx[2] + dz[0]),
        gain * (dy[2] + dz[1]),
    )


def divergence(u, s, before, diag):
    s00, s11, s22, s01, s02, s12 = s
    return (
        diag * u[0] + before[0] + last_row(s01) + last_lane(s02) - (s00 + s01 + s02),
        diag * u[1] + before[1] + last_row(s11) + last_lane(s12) - (s01 + s11 + s12),
        diag * u[2] + before[2] + last_row(s12) + last_lane(s22) - (s02 + s12 + s22),
    )


def vector(ref, i):
    return tuple(ref[j, i] for j in range(3))


def sweep(source, gain, begin, end, diag, store, unroll=None):
    u, n = vector(source, begin), vector(source, begin + 1)
    s = stress(u, n, gain[begin])

    def step(i, carry):
        before, u = carry
        n = vector(source, i + 1)
        s = stress(u, n, gain[i])
        store(i, divergence(u, s, before, diag))
        return (s[0], s[3], s[4]), n

    carry = ((s[0], s[3], s[4]), n)
    if unroll is None:
        for i in range(begin + 1, end):
            carry = step(i, carry)
    else:
        lax.fori_loop(begin + 1, end, step, carry, unroll=unroll)


def store_to(ref, mask, flag=None, load=None):
    def store(i, image):
        for j in range(3):
            value = image[j] if load is None else load(j, i) - image[j]
            own, rest = value[0:LY], value[LY:ROWS] * mask
            if flag is not None:
                own, rest = own * flag, rest * flag
            ref[j, i, 0:LY] = own
            ref[j, i, LY:ROWS] = rest

    return store


def fold(x):
    return x[0:8] + x[8:16] + x[16:24] + x[24:32]


def moments_out(out, sums):
    lane = lanes((1, LZ))
    row = jnp.zeros((1, LZ), f32)
    for k, value in enumerate(sums):
        total = jnp.sum(jnp.sum(value, axis=0, keepdims=True), axis=1, keepdims=True)
        row = jnp.where(lane == k, total, row)
    out[...] = jnp.broadcast_to(row, out.shape)


def elastic_moments(v0, v1, v2, gain):
    def add(i, acc):
        u = vector(v2, i)
        up = [next_row(x)[0:LY] for x in u]
        u = [x[0:LY] for x in u]
        dx = [v2[j, i + 1, 0:LY] - u[j] for j in range(3)]
        dy = [up[j] - u[j] for j in range(3)]
        dz = [next_lane(u[j]) - u[j] for j in range(3)]
        trace = dx[0] + dy[1] + dz[2]
        e01, e02, e12 = dx[1] + dy[0], dx[2] + dz[0], dy[2] + dz[1]
        work = 2.0 * (dx[0] * dx[0] + dy[1] * dy[1] + dz[2] * dz[2])
        work = work + 1.5 * (trace * trace) + (e01 * e01 + e02 * e02 + e12 * e12)
        work = gain[i, 0:LY] * work
        a = [v0[j, i, 0:LY] for j in range(3)]
        b = [v1[j, i, 0:LY] for j in range(3)]

        def dot(x, y):
            return x[0] * y[0] + x[1] * y[1] + x[2] * y[2]

        square = dot(u, u)
        new = (
            dot(a, a), dot(a, b), dot(b, b), dot(b, u), square,
            work + (spring_term - SHIFT_U) * square,
        )
        return tuple(x + fold(y) for x, y in zip(acc, new))

    return add


def inner_kernel(
    disp, force, damage, history, crack, high, low, flags,
    wide, load, gain, v0, v1, v2, short_damage, past, partial,
):
    mask = row_mask(flags)

    def assemble(k, carry):
        i = OFF + k
        for j in range(3):
            wide[j, i, 0:LY] = disp[j, k]
            wide[j, i, LY : LY + 8] = high[j, k] * flags[3]
            wide[j, i, LY + 8 : ROWS] = low_tile(low, j, k) * flags[2]
            load[j, k, 0:LY] = force[j, k]
            load[j, k, LY : LY + 8] = high[3 + j, k]
            load[j, k, LY + 8 : ROWS] = low_tile(low, 3 + j, k)
        own = damage[k]
        above, below = damage_tiles(high, low, k)
        short_damage[i, 0:LY] = own
        short_damage[i, LY:SHORT] = brief(above * flags[3], below * flags[2])
        left = 1.0 - own
        gain[i, 0:LY] = left * left + stiff_floor
        left = 1.0 - above
        gain[i, LY : LY + 8] = (left * left + stiff_floor) * mask[0:8]
        left = 1.0 - below
        gain[i, LY + 8 : ROWS] = (left * left + stiff_floor) * mask[8:16]
        past[i, 0:LY] = jnp.maximum(history[k], crack_load * crack[k].astype(f32))
        past[i, LY:SHORT] = past_tile(high, low, k)
        return carry

    lax.fori_loop(0, LX, assemble, 0, unroll=2)
    diag = spring_term - SHIFT_U
    first = store_to(v0, mask, load=lambda j, i: load[j, i - OFF])
    sweep(wide, gain, OFF, OFF + 15, spring_term, first, unroll=UNROLL)
    sweep(v0, gain, OFF + 1, OFF + 14, diag, store_to(v1, mask), unroll=UNROLL)
    sweep(v1, gain, OFF + 2, OFF + 13, diag, store_to(v2, mask), unroll=UNROLL)
    zero = jnp.zeros((8, LZ), f32)
    add = elastic_moments(v0, v1, v2, gain)
    for k, value in enumerate(
        lax.fori_loop(OFF + 3, OFF + 12, add, (zero,) * 6, unroll=3)
    ):
        partial[k] = value


UNROLL = 4


def outer_kernel(
    wide_in, load, gain_in, v0_in, v1_in, v2_in, short_in, past_in, partial,
    ahead, behind, ahead_corner, behind_corner, flags,
    wide, gain, v0, v1, v2, short_damage, past, sums, edge_load,
):
    mask = row_mask(flags)
    for counts, starts, high_side, middle, corner, flag in (
        (AHEAD, AHEAD_AT, True, ahead, ahead_corner, flags[1]),
        (BEHIND, BEHIND_AT, False, behind, behind_corner, flags[0]),
    ):
        for k in range(8):
            for c in range(counts[k]):
                at = starts[k] + c
                i = OFF + LX + c if high_side else OFF - counts[k] + c
                own, high, low = middle[at], corner[at, 0:8], corner[at, 8:16]
                if k == 7:
                    past[i, 0:LY] = own
                    past[i, LY:SHORT] = high
                    continue
                if k < 3:
                    into = wide.at[k, i]
                    own = own * flag
                    high = high * (flag * flags[3])
                    low = low * (flag * flags[2])
                elif k < 6:
                    into = edge_load.at[k - 3, i - OFF - LX + 4 if high_side else i - 1]
                else:
                    into = gain.at[i]
                    short_damage[i, 0:LY] = own * flag
                    short_damage[i, LY:SHORT] = brief(
                        high * (flag * flags[3]), low * (flag * flags[2])
                    )
                    own, high, low = (
                        (1.0 - x) * (1.0 - x) + stiff_floor for x in (own, high, low)
                    )
                    own = own * flag
                    high = high * (mask[0:8] * flag)
                    low = low * (mask[8:16] * flag)
                into[0:LY] = own
                into[LY : LY + 8] = high
                into[LY + 8 : ROWS] = low

    def force_at(j, i):
        if i < OFF:
            return edge_load[j, i - 1]
        if i >= OFF + LX:
            return edge_load[j, i - OFF - LX + 4]
        return load[j, i - OFF]

    def both(source, target, low_end, high_begin, diag, load=None):
        def store(i, image):
            flag = flags[0] if i < OFF else flags[1] if i >= OFF + LX else None
            store_to(target, mask, flag, load)(i, image)

        sweep(source, gain, low_end - 6, low_end, diag, store)
        sweep(source, gain, high_begin, high_begin + 8, diag, store)

    diag = spring_term - SHIFT_U
    both(wide, v0, OFF + 1, OFF + 14, spring_term, force_at)
    both(v0, v1, OFF + 2, OFF + 13, diag)
    both(v1, v2, OFF + 3, OFF + 12, diag)

    add = elastic_moments(v0, v1, v2, gain)
    acc = tuple(partial[k] for k in range(6))
    for i in (*range(OFF, OFF + 3), *range(OFF + 12, OFF + 16)):
        acc = add(i, acc)
    moments_out(sums, acc)


def coefficients(gathered, shift):
    row = jnp.sum(gathered[...], axis=0, keepdims=True)
    lane = lanes((1, LZ))
    mu = [
        jnp.broadcast_to(
            jnp.sum(jnp.where(lane == k, row, 0.0), axis=1, keepdims=True), (1, LZ)
        )
        for k in range(6)
    ]

    def inner(a, b, up=0):
        total = None
        for i, x in enumerate(a):
            for j, y in enumerate(b):
                term = x * y * mu[i + j + up]
                total = term if total is None else total + term
        return total

    one = jnp.ones((1, LZ), f32)
    resid, direction = [one], [one]
    found = []
    norm = mu[0]
    for number in range(3):
        work = inner(direction, direction, 1) + shift * inner(direction, direction)
        alpha = norm / work
        for i, x in enumerate(direction):
            if i < len(found):
                found[i] = found[i] + alpha * x
            else:
                found.append(alpha * x)
        if number < 2:
            image = [shift * x for x in direction] + [jnp.zeros((1, LZ), f32)]
            for i, x in enumerate(direction):
                image[i + 1] = image[i + 1] + x
            resid = [
                (resid[i] if i < len(resid) else 0.0) - alpha * x for i, x in enumerate(image)
            ]
            new = inner(resid, resid)
            ratio = new / norm
            direction = [
                x + ratio * direction[i] if i < len(direction) else x
                for i, x in enumerate(resid)
            ]
            norm = new
    return found


def damage_kernel(
    gathered, wide, v0, v1, v2, short_damage, past, flags,
    moved, found, w0, w1, w2, sums, now, drive,
):
    a0, a1, a2 = coefficients(gathered, SHIFT_U)

    def current(j, i):
        value = wide[j, i] + a0 * v0[j, i] + a1 * v1[j, i] + a2 * v2[j, i]
        now[j, i, 0:LY] = value[0:LY]
        now[j, i, LY:SHORT] = brief(value[LY : LY + 8], value[LY + 8 : ROWS])
        return value

    def middle(i, carry):
        for j in range(3):
            moved[j, i - OFF] = current(j, i)[0:LY]
        return carry

    lax.fori_loop(OFF, OFF + LX, middle, 0, unroll=2)
    for i in (OFF - 2, OFF - 1, *range(OFF + LX, OFF + LX + 4)):
        for j in range(3):
            current(j, i)

    row = lax.broadcasted_iota(jnp.int32, (8, LZ), 0)
    mask = jnp.where(row < 4, flags[3], flags[2])

    def energy(i):
        u, n = vector(now, i), vector(now, i + 1)
        dx = [n[j] - u[j] for j in range(3)]
        dy = [next_row(u[j]) - u[j] for j in range(3)]
        dz = [next_lane(u[j]) - u[j] for j in range(3)]
        trace = dx[0] + dy[1] + dz[2]
        e01, e02, e12 = dx[1] + dy[0], dx[2] + dz[0], dy[2] + dz[1]
        squares = dx[0] * dx[0] + dy[1] * dy[1] + dz[2] * dz[2]
        squares = squares + 0.5 * (e01 * e01 + e02 * e02 + e12 * e12)
        positive = jnp.maximum(trace, 0.0)
        return bulk_half * (positive * positive) + (squares - trace * trace * (1.0 / 3.0))

    def step(i, carry):
        value = jnp.maximum(past[i], energy(i))
        drive[i] = value
        found[i - OFF] = value[0:LY]
        return carry

    lax.fori_loop(OFF, OFF + LX, step, 0, unroll=4)
    for i in (OFF - 2, OFF - 1, *range(OFF + LX, OFF + LX + 3)):
        drive[i] = jnp.maximum(past[i], energy(i))

    def flag_of(i):
        return jnp.where(i < OFF, flags[0], jnp.where(i >= OFF + LX, flags[1], 1.0))

    def apply(source, begin, end, make, target):
        def step(i, carry):
            before, here = carry
            n = source[i + 1]
            beside = before + n + next_row(here) + last_row(here)
            beside = beside + next_lane(here) + last_lane(here)
            value = make(i, here, beside) * flag_of(i)
            target[i, 0:LY] = value[0:LY]
            target[i, LY:SHORT] = value[LY:SHORT] * mask
            return here, n

        lax.fori_loop(begin, end, step, (source[begin - 1], source[begin]), unroll=7)

    full = tough_ratio + 6.0 * length_term

    def start(i, here, beside):
        twice = 2.0 * drive[i]
        return twice - ((full + twice) * here - length_term * beside)

    def image(i, here, beside):
        return ((full - SHIFT_D) + 2.0 * drive[i]) * here - length_term * beside

    apply(short_damage, OFF - 2, OFF + LX + 3, start, w0)
    apply(w0, OFF - 1, OFF + LX + 2, image, w1)
    apply(w1, OFF, OFF + LX + 1, image, w2)

    lane = lanes((LY, LZ))
    row = lax.broadcasted_iota(jnp.int32, (LY, LZ), 0)
    edge = jnp.where(lane == 0, length_term, 0.0)
    edge = edge + jnp.where(row == 0, length_term * (1.0 - flags[2]), 0.0)
    edge = edge + (tough_ratio - SHIFT_D)

    def add(i, acc):
        wide_now = w2[i]
        u = wide_now[0:LY]
        dx = w2[i + 1, 0:LY] - u
        dy = next_row(wide_now)[0:LY] - u
        dz = next_lane(u) - u
        side = jnp.where(i == OFF, length_term * (1.0 - flags[0]), 0.0)
        square = u * u
        work = (edge + side + 2.0 * drive[i, 0:LY]) * square
        work = work + length_term * (dx * dx + dy * dy + dz * dz)
        a, b = w0[i, 0:LY], w1[i, 0:LY]
        new = (a * a, a * b, b * b, b * u, square, work)
        return tuple(x + fold(y) for x, y in zip(acc, new))

    zero = jnp.zeros((8, LZ), f32)
    moments_out(sums, lax.fori_loop(OFF, OFF + LX, add, (zero,) * 6, unroll=4))


def update_kernel(gathered, damage, w0, w1, w2, out):
    b0, b1, b2 = coefficients(gathered, SHIFT_D)

    def step(c, carry):
        i = OFF + c
        image = b0 * w0[i, 0:LY] + b1 * w1[i, 0:LY] + b2 * w2[i, 0:LY]
        out[c] = damage[c] + image
        return carry

    lax.fori_loop(0, LX, step, 0, unroll=2)


def send(values, dx, dy):
    axis, step = ("gx", dx) if dx else ("gy", dy)
    size = lax.axis_size(axis)
    return lax.ppermute(values, axis, [(i, (i + step) % size) for i in range(size)])


def step(displacement, force, damage, history, crack_flags):
    axes = ("gx", "gy")
    count = lax.axis_size(axes)
    ix, iy = lax.axis_index("gx"), lax.axis_index("gy")
    flags = jnp.stack(
        [ix > 0, ix < lax.axis_size("gx") - 1, iy > 0, iy < lax.axis_size("gy") - 1]
    ).astype(f32)

    def gather(sums):
        return lax.all_to_all(sums, axes, 0, 0, tiled=True)

    edge_rows, edge_flags = (8, LX, 8, LZ), pltpu.VMEM((LX, 8, LZ), jnp.int32)
    first, last, front, back = call(
        pack_kernel,
        [(6, LX, 8, LZ), (5, LX, 8, LZ), (FRONT, LY, LZ), (BACK, LY, LZ)],
        [
            edge_rows, edge_rows, edge_flags, edge_flags,
            pltpu.VMEM((AHEAD[7], LY, LZ), jnp.int32),
            pltpu.VMEM((BEHIND[7], LY, LZ), jnp.int32),
            pltpu.SemaphoreType.DMA((28,)),
        ],
        hbm=True,
    )(displacement, force, damage, history, crack_flags)
    high = send(first, 0, -1)
    low = send(last, 0, 1)
    ahead = send(front, -1, 0)
    behind = send(back, 1, 0)
    corners = call(corner_kernel, [(FRONT, 16, LZ), (BACK, 16, LZ)])(high, low)
    ahead_corner = send(corners[0], -1, 0)
    behind_corner = send(corners[1], 1, 0)
    wide, load, gain, v0, v1, v2, short_damage, past, partial = call(
        inner_kernel,
        [VECTOR, (3, LX, ROWS, LZ), SCALAR, VECTOR, VECTOR, VECTOR, BRIEF, BRIEF, (6, 8, LZ)],
    )(displacement, force, damage, history, crack_flags, high, low, flags=flags)
    wide, gain, v0, v1, v2, short_damage, past, sums = call(
        outer_kernel,
        [VECTOR, SCALAR, VECTOR, VECTOR, VECTOR, BRIEF, BRIEF, (count, LZ)],
        scratch=[(3, 10, ROWS, LZ)],
        aliases={0: 0, 2: 1, 3: 2, 4: 3, 5: 4, 6: 5, 7: 6},
    )(
        wide, load, gain, v0, v1, v2, short_damage, past, partial,
        ahead, behind, ahead_corner, behind_corner, flags=flags,
    )
    moved, found, w0, w1, w2, sums = call(
        damage_kernel,
        [whole(3, LX, LY, LZ), whole(LX, LY, LZ), BRIEF, BRIEF, BRIEF, (count, LZ)],
        [(3, DEPTH, SHORT, LZ), BRIEF],
    )(gather(sums), wide, v0, v1, v2, short_damage, past, flags=flags)
    (damage_out,) = call(update_kernel, [whole(LX, LY, LZ)])(
        gather(sums), damage, w0, w1, w2
    )
    return moved, damage_out, found


def solution(mesh):
    return jax.shard_map(
        step,
        mesh=mesh,
        in_specs=(
            P(None, "gx", "gy", None),
            P(None, "gx", "gy", None),
            P("gx", "gy", None),
            P("gx", "gy", None),
            P("gx", "gy", None),
        ),
        out_specs=(P(None, "gx", "gy", None), P("gx", "gy", None), P("gx", "gy", None)),
        check_vma=False,
    )
```

```python
import jax
import jax.numpy as jnp
from jax import lax
from jax.experimental import pallas as pl
from jax.experimental.pallas import tpu as pltpu
from jax.sharding import PartitionSpec as P


INTERPRET = False
f32 = jnp.float32

spring_term = 0.5
stiff_floor = 0.001
crack_load = 4.0
tough_ratio = 0.5
length_term = 2.0
bulk_half = 0.5 * (1.5 + 2.0 / 3.0)

LX, LY, LZ = 16, 32, 128
ROWS, SHORT, DEPTH, OFF = 48, 40, 28, 5

SHIFT_U = 14.0
SHIFT_D = 18.0

VECTOR = (3, DEPTH, ROWS, LZ)
SCALAR = (DEPTH, ROWS, LZ)
BRIEF = (DEPTH, SHORT, LZ)
FIELD = (LX, LY, LZ)


def fast(shape):
    return fast_as(shape, f32)


def fast_as(shape, kind):
    return jax.ShapeDtypeStruct(shape, kind) if INTERPRET else pltpu.VMEM(shape, kind)


def whole(*shape):
    return jax.ShapeDtypeStruct(shape, f32)


def call(kernel, outs, scratch=(), limit=8 << 20, aliases=None, hbm=False):
    vmem = pl.BlockSpec(memory_space=pltpu.VMEM)
    smem = pl.BlockSpec(memory_space=pltpu.SMEM)

    def run(*args, flags=None):
        specs = [pl.BlockSpec(memory_space=pltpu.HBM) if hbm else vmem] * len(args)
        if hbm and not INTERPRET:
            args = [pltpu.with_memory_space_constraint(x, pltpu.HBM) for x in args]
        if flags is not None:
            args, specs = (*args, flags), specs + [smem]
        return pl.pallas_call(
            kernel,
            out_shape=[fast(s) if isinstance(s, tuple) else s for s in outs],
            in_specs=specs,
            out_specs=[vmem] * len(outs),
            scratch_shapes=[pltpu.VMEM(s, f32) if isinstance(s, tuple) else s for s in scratch],
            input_output_aliases=aliases or {},
            compiler_params=pltpu.CompilerParams(vmem_limit_bytes=limit),
            interpret=INTERPRET,
        )(*args)

    return run


def roll(x, shift, axis):
    return pltpu.roll(x, shift % x.shape[axis], axis)


def next_row(x):
    return roll(x, -1, 0)


def last_row(x):
    return roll(x, 1, 0)


def lanes(shape):
    return lax.broadcasted_iota(jnp.int32, shape, 1)


def next_lane(x):
    return jnp.where(lanes(x.shape) == LZ - 1, 0.0, roll(x, -1, 1))


def last_lane(x):
    return jnp.where(lanes(x.shape) == 0, 0.0, roll(x, 1, 1))


def tile_row():
    return lax.broadcasted_iota(jnp.int32, (8, LZ), 0)


def pack_first(u, load, damage, past):
    row = tile_row()
    tiles = [jnp.where(row == 7, roll(past, 7 - j, 0), u[j]) for j in range(3)]
    return tiles + [jnp.where(row < 6, load[j], roll(damage, 6 - 2 * j, 0)) for j in range(3)]


def pack_last(u, load, damage, past):
    row = tile_row()
    return [
        jnp.where(row < 3, roll(damage, -1, 0), u[0]),
        jnp.where(row < 3, roll(past, 2, 0), u[1]),
        u[2],
        jnp.where(row < 4, roll(load[1], 4, 0), load[0]),
        jnp.where(row < 4, roll(damage, 4, 0), load[2]),
    ]


def low_tile(low, field, k):
    if field < 4:
        return low[field, k]
    return roll(low[3, k], 4, 0) if field == 4 else low[4, k]


def damage_tiles(high, low, k):
    row = tile_row()
    above = jnp.where(row < 2, roll(high[3, k], 2, 0), roll(high[4, k], 4, 0))
    above = jnp.where(row < 4, above, roll(high[5, k], 6, 0))
    below = jnp.where(row < 4, roll(low[0, k], 1, 0), roll(low[4, k], 4, 0))
    return above, below


def past_tile(high, low, k):
    row = tile_row()
    above = jnp.where(row < 1, roll(high[0, k], 1, 0), roll(high[1, k], 2, 0))
    above = jnp.where(row < 2, above, roll(high[2, k], 3, 0))
    return jnp.where(row < 4, above, roll(low[1, k], -2, 0))


def brief(above, below):
    return jnp.where(tile_row() < 4, above, below)


def row_mask(flags):
    row = lax.broadcasted_iota(jnp.int32, (ROWS - LY, LZ), 0)
    return jnp.where(row < 8, flags[3], flags[2])


AHEAD = (7, 7, 7, 6, 6, 6, 6, 3)
BEHIND = (5, 5, 5, 4, 4, 4, 5, 2)
AHEAD_AT = tuple(sum(AHEAD[:k]) for k in range(8))
BEHIND_AT = tuple(sum(BEHIND[:k]) for k in range(8))
FRONT, BACK = sum(AHEAD), sum(BEHIND)


def pack_kernel(
    disp_in, force_in, damage_in, history_in, crack_in, flags,
    disp, force, damage, history, crack, first, last, front, back, sem,
):
    copies = [
        pltpu.make_async_copy(source, target, sem.at[n])
        for n, (source, target) in enumerate(
            (
                (crack_in, crack), (history_in, history), (damage_in, damage),
                (disp_in, disp), (force_in, force),
            )
        )
    ]
    for copy in copies:
        copy.start()
    for copy in copies:
        copy.wait()

    def step(k, carry):
        for rows, out, pack in ((0, first, pack_first), (24, last, pack_last)):
            at = slice(rows, rows + 8)
            past = jnp.maximum(history[k, at], crack_load * crack[k, at].astype(f32))
            tiles = pack(
                [disp[j, k, at] for j in range(3)], [force[j, k, at] for j in range(3)],
                damage[k, at], past,
            )
            for n, tile in enumerate(tiles):
                out[n, k] = tile
        return carry

    lax.fori_loop(0, LX, step, 0, unroll=2)
    for counts, starts, out, ahead in ((AHEAD, AHEAD_AT, front, True), (BEHIND, BEHIND_AT, back, False)):
        for k in range(8):
            size, at = counts[k], starts[k]
            begin = 0 if ahead else LX - size
            layers = slice(begin, begin + size)
            if k == 7:
                flag = crack[layers].astype(f32)
                out[at : at + size] = jnp.maximum(history[layers], crack_load * flag)
            else:
                field = disp.at[k] if k < 3 else force.at[k - 3] if k < 6 else damage
                out[at : at + size] = field[layers]


FRONT_TILES = (7, 7, 7, 6, 6, 6, 7, 7, 7, 6, 6)
BACK_TILES = (5,) * 11
FRONT_TILES_AT = tuple(sum(FRONT_TILES[:k]) for k in range(11))
BACK_TILES_AT = tuple(sum(BACK_TILES[:k]) for k in range(11))


def corner_kernel(high, low, front, back):
    for counts, starts, out, ahead in (
        (FRONT_TILES, FRONT_TILES_AT, front, True), (BACK_TILES, BACK_TILES_AT, back, False)
    ):
        for k in range(11):
            size, at = counts[k], starts[k]
            begin = 0 if ahead else LX - size
            source = high.at[k] if k < 6 else low.at[k - 6]
            out[at : at + size] = source[begin : begin + size]


class Corner:
    def __init__(self, ref, starts, offset):
        self.ref, self.starts, self.offset = ref, starts, offset

    def __getitem__(self, key):
        return self.ref[self.starts[key[0] + self.offset] + key[1]]


def stress(u, n, gain):
    dx = [n[j] - u[j] for j in range(3)]
    dy = [next_row(u[j]) - u[j] for j in range(3)]
    dz = [next_lane(u[j]) - u[j] for j in range(3)]
    twice = gain + gain
    part = 0.75 * (dx[0] + dy[1] + dz[2])
    return (
        twice * (dx[0] + part),
        twice * (dy[1] + part),
        twice * (dz[2] + part),
        gain * (dx[1] + dy[0]),
        gain * (dx[2] + dz[0]),
        gain * (dy[2] + dz[1]),
    )


def divergence(u, s, before, diag):
    s00, s11, s22, s01, s02, s12 = s
    return (
        diag * u[0] + before[0] + last_row(s01) + last_lane(s02) - (s00 + s01 + s02),
        diag * u[1] + before[1] + last_row(s11) + last_lane(s12) - (s01 + s11 + s12),
        diag * u[2] + before[2] + last_row(s12) + last_lane(s22) - (s02 + s12 + s22),
    )


def vector(ref, i):
    return tuple(ref[j, i] for j in range(3))


def sweep(source, gain, begin, end, diag, store, unroll=None):
    u, n = vector(source, begin), vector(source, begin + 1)
    s = stress(u, n, gain[begin])

    def step(i, carry):
        before, u = carry
        n = vector(source, i + 1)
        s = stress(u, n, gain[i])
        store(i, divergence(u, s, before, diag))
        return (s[0], s[3], s[4]), n

    carry = ((s[0], s[3], s[4]), n)
    if unroll is None:
        for i in range(begin + 1, end):
            carry = step(i, carry)
    else:
        lax.fori_loop(begin + 1, end, step, carry, unroll=unroll)


def store_to(ref, mask, flag=None, load=None):
    def store(i, image):
        for j in range(3):
            value = image[j] if load is None else load(j, i) - image[j]
            own, rest = value[0:LY], value[LY:ROWS] * mask
            if flag is not None:
                own, rest = own * flag, rest * flag
            ref[j, i, 0:LY] = own
            ref[j, i, LY:ROWS] = rest

    return store


def fold(x):
    return x[0:8] + x[8:16] + x[16:24] + x[24:32]


def moments_out(out, sums):
    lane = lanes((1, LZ))
    row = jnp.zeros((1, LZ), f32)
    for k, value in enumerate(sums):
        total = jnp.sum(jnp.sum(value, axis=0, keepdims=True), axis=1, keepdims=True)
        row = jnp.where(lane == k, total, row)
    out[...] = jnp.broadcast_to(row, out.shape)


def elastic_moments(v0, v1, v2, gain):
    def add(i, acc):
        u = vector(v2, i)
        up = [next_row(x)[0:LY] for x in u]
        u = [x[0:LY] for x in u]
        dx = [v2[j, i + 1, 0:LY] - u[j] for j in range(3)]
        dy = [up[j] - u[j] for j in range(3)]
        dz = [next_lane(u[j]) - u[j] for j in range(3)]
        trace = dx[0] + dy[1] + dz[2]
        e01, e02, e12 = dx[1] + dy[0], dx[2] + dz[0], dy[2] + dz[1]
        work = 2.0 * (dx[0] * dx[0] + dy[1] * dy[1] + dz[2] * dz[2])
        work = work + 1.5 * (trace * trace) + (e01 * e01 + e02 * e02 + e12 * e12)
        work = gain[i, 0:LY] * work
        a = [v0[j, i, 0:LY] for j in range(3)]
        b = [v1[j, i, 0:LY] for j in range(3)]

        def dot(x, y):
            return x[0] * y[0] + x[1] * y[1] + x[2] * y[2]

        square = dot(u, u)
        new = (
            dot(a, a), dot(a, b), dot(b, b), dot(b, u), square,
            work + (spring_term - SHIFT_U) * square,
        )
        return tuple(x + fold(y) for x, y in zip(acc, new))

    return add


def inner_kernel(
    disp, force, damage, history, crack, high, low, flags,
    wide, load, gain, v0, v1, v2, short_damage, past, partial,
):
    mask = row_mask(flags)

    def assemble(k, carry):
        i = OFF + k
        for j in range(3):
            wide[j, i, 0:LY] = disp[j, k]
            wide[j, i, LY : LY + 8] = high[j, k] * flags[3]
            wide[j, i, LY + 8 : ROWS] = low_tile(low, j, k) * flags[2]
            load[j, k, 0:LY] = force[j, k]
            load[j, k, LY : LY + 8] = high[3 + j, k]
            load[j, k, LY + 8 : ROWS] = low_tile(low, 3 + j, k)
        own = damage[k]
        above, below = damage_tiles(high, low, k)
        short_damage[i, 0:LY] = own
        short_damage[i, LY:SHORT] = brief(above * flags[3], below * flags[2])
        left = 1.0 - own
        gain[i, 0:LY] = left * left + stiff_floor
        left = 1.0 - above
        gain[i, LY : LY + 8] = (left * left + stiff_floor) * mask[0:8]
        left = 1.0 - below
        gain[i, LY + 8 : ROWS] = (left * left + stiff_floor) * mask[8:16]
        past[i, 0:LY] = jnp.maximum(history[k], crack_load * crack[k].astype(f32))
        past[i, LY:SHORT] = past_tile(high, low, k)
        return carry

    lax.fori_loop(0, LX, assemble, 0, unroll=2)
    diag = spring_term - SHIFT_U
    first = store_to(v0, mask, load=lambda j, i: load[j, i - OFF])
    sweep(wide, gain, OFF, OFF + 15, spring_term, first, unroll=UNROLL)
    sweep(v0, gain, OFF + 1, OFF + 14, diag, store_to(v1, mask), unroll=UNROLL)
    sweep(v1, gain, OFF + 2, OFF + 13, diag, store_to(v2, mask), unroll=UNROLL)
    zero = jnp.zeros((8, LZ), f32)
    add = elastic_moments(v0, v1, v2, gain)
    for k, value in enumerate(
        lax.fori_loop(OFF + 3, OFF + 12, add, (zero,) * 6, unroll=3)
    ):
        partial[k] = value


UNROLL = 4


def outer_kernel(
    wide_in, load, gain_in, v0_in, v1_in, v2_in, short_in, past_in, partial,
    ahead, behind, ahead_corner, behind_corner, flags,
    wide, gain, v0, v1, v2, short_damage, past, sums, edge_load,
):
    mask = row_mask(flags)
    for counts, starts, high_side, middle, corner, tiles, flag in (
        (AHEAD, AHEAD_AT, True, ahead, ahead_corner, FRONT_TILES_AT, flags[1]),
        (BEHIND, BEHIND_AT, False, behind, behind_corner, BACK_TILES_AT, flags[0]),
    ):
        above, below = Corner(corner, tiles, 0), Corner(corner, tiles, 6)
        for k in range(8):
            for c in range(counts[k]):
                own = middle[starts[k] + c]
                i = OFF + LX + c if high_side else OFF - counts[k] + c
                layer = c if high_side else 5 - counts[k] + c
                if k == 7:
                    past[i, 0:LY] = own
                    past[i, LY:SHORT] = past_tile(above, below, layer)
                    continue
                if k < 6:
                    high, low = above[k, layer], low_tile(below, k, layer)
                else:
                    high, low = damage_tiles(above, below, layer)
                if k < 3:
                    into = wide.at[k, i]
                    own = own * flag
                    high = high * (flag * flags[3])
                    low = low * (flag * flags[2])
                elif k < 6:
                    into = edge_load.at[k - 3, i - OFF - LX + 4 if high_side else i - 1]
                else:
                    into = gain.at[i]
                    short_damage[i, 0:LY] = own * flag
                    short_damage[i, LY:SHORT] = brief(
                        high * (flag * flags[3]), low * (flag * flags[2])
                    )
                    own, high, low = (
                        (1.0 - x) * (1.0 - x) + stiff_floor for x in (own, high, low)
                    )
                    own = own * flag
                    high = high * (mask[0:8] * flag)
                    low = low * (mask[8:16] * flag)
                into[0:LY] = own
                into[LY : LY + 8] = high
                into[LY + 8 : ROWS] = low

    def force_at(j, i):
        if i < OFF:
            return edge_load[j, i - 1]
        if i >= OFF + LX:
            return edge_load[j, i - OFF - LX + 4]
        return load[j, i - OFF]

    def both(source, target, low_end, high_begin, diag, load=None):
        def store(i, image):
            flag = flags[0] if i < OFF else flags[1] if i >= OFF + LX else None
            store_to(target, mask, flag, load)(i, image)

        sweep(source, gain, low_end - 6, low_end, diag, store)
        sweep(source, gain, high_begin, high_begin + 8, diag, store)

    diag = spring_term - SHIFT_U
    both(wide, v0, OFF + 1, OFF + 14, spring_term, force_at)
    both(v0, v1, OFF + 2, OFF + 13, diag)
    both(v1, v2, OFF + 3, OFF + 12, diag)

    add = elastic_moments(v0, v1, v2, gain)
    acc = tuple(partial[k] for k in range(6))
    for i in (*range(OFF, OFF + 3), *range(OFF + 12, OFF + 16)):
        acc = add(i, acc)
    moments_out(sums, acc)


def coefficients(gathered, shift):
    row = jnp.sum(gathered[...], axis=0, keepdims=True)
    lane = lanes((1, LZ))
    mu = [
        jnp.broadcast_to(
            jnp.sum(jnp.where(lane == k, row, 0.0), axis=1, keepdims=True), (1, LZ)
        )
        for k in range(6)
    ]

    def inner(a, b, up=0):
        total = None
        for i, x in enumerate(a):
            for j, y in enumerate(b):
                term = x * y * mu[i + j + up]
                total = term if total is None else total + term
        return total

    one = jnp.ones((1, LZ), f32)
    resid, direction = [one], [one]
    found = []
    norm = mu[0]
    for number in range(3):
        work = inner(direction, direction, 1) + shift * inner(direction, direction)
        alpha = norm / work
        for i, x in enumerate(direction):
            if i < len(found):
                found[i] = found[i] + alpha * x
            else:
                found.append(alpha * x)
        if number < 2:
            image = [shift * x for x in direction] + [jnp.zeros((1, LZ), f32)]
            for i, x in enumerate(direction):
                image[i + 1] = image[i + 1] + x
            resid = [
                (resid[i] if i < len(resid) else 0.0) - alpha * x for i, x in enumerate(image)
            ]
            new = inner(resid, resid)
            ratio = new / norm
            direction = [
                x + ratio * direction[i] if i < len(direction) else x
                for i, x in enumerate(resid)
            ]
            norm = new
    return found


def damage_kernel(
    gathered, wide, v0, v1, v2, short_damage, past, flags,
    moved, found, w0, w1, w2, sums, now, drive,
):
    a0, a1, a2 = coefficients(gathered, SHIFT_U)

    def current(j, i):
        value = wide[j, i] + a0 * v0[j, i] + a1 * v1[j, i] + a2 * v2[j, i]
        now[j, i, 0:LY] = value[0:LY]
        now[j, i, LY:SHORT] = brief(value[LY : LY + 8], value[LY + 8 : ROWS])
        return value

    def middle(i, carry):
        for j in range(3):
            moved[j, i - OFF] = current(j, i)[0:LY]
        return carry

    lax.fori_loop(OFF, OFF + LX, middle, 0, unroll=2)
    for i in (OFF - 2, OFF - 1, *range(OFF + LX, OFF + LX + 4)):
        for j in range(3):
            current(j, i)

    row = lax.broadcasted_iota(jnp.int32, (8, LZ), 0)
    mask = jnp.where(row < 4, flags[3], flags[2])

    def energy(i):
        u, n = vector(now, i), vector(now, i + 1)
        dx = [n[j] - u[j] for j in range(3)]
        dy = [next_row(u[j]) - u[j] for j in range(3)]
        dz = [next_lane(u[j]) - u[j] for j in range(3)]
        trace = dx[0] + dy[1] + dz[2]
        e01, e02, e12 = dx[1] + dy[0], dx[2] + dz[0], dy[2] + dz[1]
        squares = dx[0] * dx[0] + dy[1] * dy[1] + dz[2] * dz[2]
        squares = squares + 0.5 * (e01 * e01 + e02 * e02 + e12 * e12)
        positive = jnp.maximum(trace, 0.0)
        return bulk_half * (positive * positive) + (squares - trace * trace * (1.0 / 3.0))

    def step(i, carry):
        value = jnp.maximum(past[i], energy(i))
        drive[i] = value
        found[i - OFF] = value[0:LY]
        return carry

    lax.fori_loop(OFF, OFF + LX, step, 0, unroll=4)
    for i in (OFF - 2, OFF - 1, *range(OFF + LX, OFF + LX + 3)):
        drive[i] = jnp.maximum(past[i], energy(i))

    def flag_of(i):
        return jnp.where(i < OFF, flags[0], jnp.where(i >= OFF + LX, flags[1], 1.0))

    def apply(source, begin, end, make, target):
        def step(i, carry):
            before, here = carry
            n = source[i + 1]
            beside = before + n + next_row(here) + last_row(here)
            beside = beside + next_lane(here) + last_lane(here)
            value = make(i, here, beside) * flag_of(i)
            target[i, 0:LY] = value[0:LY]
            target[i, LY:SHORT] = value[LY:SHORT] * mask
            return here, n

        lax.fori_loop(begin, end, step, (source[begin - 1], source[begin]), unroll=7)

    full = tough_ratio + 6.0 * length_term

    def start(i, here, beside):
        twice = 2.0 * drive[i]
        return twice - ((full + twice) * here - length_term * beside)

    def image(i, here, beside):
        return ((full - SHIFT_D) + 2.0 * drive[i]) * here - length_term * beside

    apply(short_damage, OFF - 2, OFF + LX + 3, start, w0)
    apply(w0, OFF - 1, OFF + LX + 2, image, w1)
    apply(w1, OFF, OFF + LX + 1, image, w2)

    lane = lanes((LY, LZ))
    row = lax.broadcasted_iota(jnp.int32, (LY, LZ), 0)
    edge = jnp.where(lane == 0, length_term, 0.0)
    edge = edge + jnp.where(row == 0, length_term * (1.0 - flags[2]), 0.0)
    edge = edge + (tough_ratio - SHIFT_D)

    def add(i, acc):
        wide_now = w2[i]
        u = wide_now[0:LY]
        dx = w2[i + 1, 0:LY] - u
        dy = next_row(wide_now)[0:LY] - u
        dz = next_lane(u) - u
        side = jnp.where(i == OFF, length_term * (1.0 - flags[0]), 0.0)
        square = u * u
        work = (edge + side + 2.0 * drive[i, 0:LY]) * square
        work = work + length_term * (dx * dx + dy * dy + dz * dz)
        a, b = w0[i, 0:LY], w1[i, 0:LY]
        new = (a * a, a * b, b * b, b * u, square, work)
        return tuple(x + fold(y) for x, y in zip(acc, new))

    zero = jnp.zeros((8, LZ), f32)
    moments_out(sums, lax.fori_loop(OFF, OFF + LX, add, (zero,) * 6, unroll=4))


def update_kernel(gathered, damage, w0, w1, w2, out):
    b0, b1, b2 = coefficients(gathered, SHIFT_D)

    def step(c, carry):
        i = OFF + c
        image = b0 * w0[i, 0:LY] + b1 * w1[i, 0:LY] + b2 * w2[i, 0:LY]
        out[c] = damage[c] + image
        return carry

    lax.fori_loop(0, LX, step, 0, unroll=2)


def send(values, dx, dy):
    axis, step = ("gx", dx) if dx else ("gy", dy)
    size = lax.axis_size(axis)
    return lax.ppermute(values, axis, [(i, (i + step) % size) for i in range(size)])


def step(displacement, force, damage, history, crack_flags):
    axes = ("gx", "gy")
    count = lax.axis_size(axes)
    ix, iy = lax.axis_index("gx"), lax.axis_index("gy")
    flags = jnp.stack(
        [ix > 0, ix < lax.axis_size("gx") - 1, iy > 0, iy < lax.axis_size("gy") - 1]
    ).astype(f32)

    def gather(sums):
        return lax.all_to_all(sums, axes, 0, 0, tiled=True)

    disp, load, old, history, crack, first, last, front, back = call(
        pack_kernel,
        [(3, *FIELD), (3, *FIELD), FIELD, FIELD, fast_as(FIELD, jnp.int32)]
        + [(6, LX, 8, LZ), (5, LX, 8, LZ), (FRONT, LY, LZ), (BACK, LY, LZ)],
        [pltpu.SemaphoreType.DMA((5,))],
        hbm=True,
    )(displacement, force, damage, history, crack_flags, flags=flags)
    high = send(first, 0, -1)
    low = send(last, 0, 1)
    ahead = send(front, -1, 0)
    behind = send(back, 1, 0)
    corners = call(
        corner_kernel, [(sum(FRONT_TILES), 8, LZ), (sum(BACK_TILES), 8, LZ)]
    )(high, low)
    ahead_corner = send(corners[0], -1, 0)
    behind_corner = send(corners[1], 1, 0)
    wide, load, gain, v0, v1, v2, short_damage, past, partial = call(
        inner_kernel,
        [VECTOR, (3, LX, ROWS, LZ), SCALAR, VECTOR, VECTOR, VECTOR, BRIEF, BRIEF, (6, 8, LZ)],
    )(disp, load, old, history, crack, high, low, flags=flags)
    wide, gain, v0, v1, v2, short_damage, past, sums = call(
        outer_kernel,
        [VECTOR, SCALAR, VECTOR, VECTOR, VECTOR, BRIEF, BRIEF, (count, LZ)],
        scratch=[(3, 10, ROWS, LZ)],
        aliases={0: 0, 2: 1, 3: 2, 4: 3, 5: 4, 6: 5, 7: 6},
    )(
        wide, load, gain, v0, v1, v2, short_damage, past, partial,
        ahead, behind, ahead_corner, behind_corner, flags=flags,
    )
    moved, found, w0, w1, w2, sums = call(
        damage_kernel,
        [whole(3, LX, LY, LZ), whole(LX, LY, LZ), BRIEF, BRIEF, BRIEF, (count, LZ)],
        [(3, DEPTH, SHORT, LZ), BRIEF],
    )(gather(sums), wide, v0, v1, v2, short_damage, past, flags=flags)
    (damage_out,) = call(update_kernel, [whole(LX, LY, LZ)])(
        gather(sums), old, w0, w1, w2
    )
    return moved, damage_out, found


def solution(mesh):
    return jax.shard_map(
        step,
        mesh=mesh,
        in_specs=(
            P(None, "gx", "gy", None),
            P(None, "gx", "gy", None),
            P("gx", "gy", None),
            P("gx", "gy", None),
            P("gx", "gy", None),
        ),
        out_specs=(P(None, "gx", "gy", None), P("gx", "gy", None), P("gx", "gy", None)),
        check_vma=False,
    )
```

```python
import jax
import jax.numpy as jnp
from jax import lax
from jax.experimental import pallas as pl
from jax.experimental.pallas import tpu as pltpu
from jax.sharding import PartitionSpec as P


INTERPRET = False
f32 = jnp.float32

spring_term = 0.5
stiff_floor = 0.001
crack_load = 4.0
tough_ratio = 0.5
length_term = 2.0
bulk_half = 0.5 * (1.5 + 2.0 / 3.0)

LX, LY, LZ = 16, 32, 128
ROWS, SHORT, DEPTH, OFF = 48, 40, 28, 5

SHIFT_U = 14.0
SHIFT_D = 18.0

VECTOR = (3, DEPTH, ROWS, LZ)
SCALAR = (DEPTH, ROWS, LZ)
BRIEF = (DEPTH, SHORT, LZ)
FIELD = (LX, LY, LZ)


def fast(shape):
    return fast_as(shape, f32)


def fast_as(shape, kind):
    return jax.ShapeDtypeStruct(shape, kind) if INTERPRET else pltpu.VMEM(shape, kind)


def whole(*shape):
    return jax.ShapeDtypeStruct(shape, f32)


def call(kernel, outs, scratch=(), limit=8 << 20, aliases=None, hbm=False, far=0):
    vmem = pl.BlockSpec(memory_space=pltpu.VMEM)
    smem = pl.BlockSpec(memory_space=pltpu.SMEM)

    def run(*args, flags=None):
        specs = [pl.BlockSpec(memory_space=pltpu.HBM) if hbm else vmem] * len(args)
        if hbm and not INTERPRET:
            args = [pltpu.with_memory_space_constraint(x, pltpu.HBM) for x in args]
        if flags is not None:
            args, specs = (*args, flags), specs + [smem]
        return pl.pallas_call(
            kernel,
            out_shape=[fast(s) if isinstance(s, tuple) else s for s in outs],
            in_specs=specs,
            out_specs=[pl.BlockSpec(memory_space=pltpu.HBM)] * far + [vmem] * (len(outs) - far),
            scratch_shapes=[pltpu.VMEM(s, f32) if isinstance(s, tuple) else s for s in scratch],
            input_output_aliases=aliases or {},
            compiler_params=pltpu.CompilerParams(vmem_limit_bytes=limit),
            interpret=INTERPRET,
        )(*args)

    return run


def roll(x, shift, axis):
    return pltpu.roll(x, shift % x.shape[axis], axis)


def next_row(x):
    return roll(x, -1, 0)


def last_row(x):
    return roll(x, 1, 0)


def lanes(shape):
    return lax.broadcasted_iota(jnp.int32, shape, 1)


def next_lane(x):
    return jnp.where(lanes(x.shape) == LZ - 1, 0.0, roll(x, -1, 1))


def last_lane(x):
    return jnp.where(lanes(x.shape) == 0, 0.0, roll(x, 1, 1))


def tile_row():
    return lax.broadcasted_iota(jnp.int32, (8, LZ), 0)


def pack_first(u, load, damage, past):
    row = tile_row()
    tiles = [jnp.where(row == 7, roll(past, 7 - j, 0), u[j]) for j in range(3)]
    return tiles + [jnp.where(row < 6, load[j], roll(damage, 6 - 2 * j, 0)) for j in range(3)]


def pack_last(u, load, damage, past):
    row = tile_row()
    return [
        jnp.where(row < 3, roll(damage, -1, 0), u[0]),
        jnp.where(row < 3, roll(past, 2, 0), u[1]),
        u[2],
        jnp.where(row < 4, roll(load[1], 4, 0), load[0]),
        jnp.where(row < 4, roll(damage, 4, 0), load[2]),
    ]


def low_tile(low, field, k):
    if field < 4:
        return low[field, k]
    return roll(low[3, k], 4, 0) if field == 4 else low[4, k]


def damage_tiles(high, low, k):
    row = tile_row()
    above = jnp.where(row < 2, roll(high[3, k], 2, 0), roll(high[4, k], 4, 0))
    above = jnp.where(row < 4, above, roll(high[5, k], 6, 0))
    below = jnp.where(row < 4, roll(low[0, k], 1, 0), roll(low[4, k], 4, 0))
    return above, below


def past_tile(high, low, k):
    row = tile_row()
    above = jnp.where(row < 1, roll(high[0, k], 1, 0), roll(high[1, k], 2, 0))
    above = jnp.where(row < 2, above, roll(high[2, k], 3, 0))
    return jnp.where(row < 4, above, roll(low[1, k], -2, 0))


def brief(above, below):
    return jnp.where(tile_row() < 4, above, below)


def row_mask(flags):
    row = lax.broadcasted_iota(jnp.int32, (ROWS - LY, LZ), 0)
    return jnp.where(row < 8, flags[3], flags[2])


AHEAD = (7, 7, 7, 6, 6, 6, 6, 3)
BEHIND = (5, 5, 5, 4, 4, 4, 5, 2)
AHEAD_AT = tuple(sum(AHEAD[:k]) for k in range(8))
BEHIND_AT = tuple(sum(BEHIND[:k]) for k in range(8))
FRONT, BACK = sum(AHEAD), sum(BEHIND)


def rows_kernel(
    disp, force, damage, history, crack, flags,
    first, last, top, bottom, top_crack, bottom_crack, sem,
):
    copies = []
    for rows, into, into_crack in ((0, top, top_crack), (24, bottom, bottom_crack)):
        for source, target in (
            (crack.at[:, rows : rows + 8], into_crack),
            (history.at[:, rows : rows + 8], into.at[7]),
            (damage.at[:, rows : rows + 8], into.at[6]),
            (disp.at[:, :, rows : rows + 8], into.at[0:3]),
            (force.at[:, :, rows : rows + 8], into.at[3:6]),
        ):
            copies.append(pltpu.make_async_copy(source, target, sem.at[len(copies)]))
    for copy in copies:
        copy.start()
    for copy in copies:
        copy.wait()

    def step(k, carry):
        for into, flag, out, pack in (
            (top, top_crack, first, pack_first), (bottom, bottom_crack, last, pack_last)
        ):
            past = jnp.maximum(into[7, k], crack_load * flag[k].astype(f32))
            tiles = pack(
                [into[j, k] for j in range(3)], [into[3 + j, k] for j in range(3)],
                into[6, k], past,
            )
            for n, tile in enumerate(tiles):
                out[n, k] = tile
        return carry

    lax.fori_loop(0, LX, step, 0, unroll=2)


def bulk_kernel(
    disp_in, force_in, damage_in, history_in, crack_in,
    disp, force, damage, history, crack, front, back, sem,
):
    copies = [
        pltpu.make_async_copy(source, target, sem.at[n])
        for n, (source, target) in enumerate(
            (
                (crack_in, crack), (history_in, history), (damage_in, damage),
                (disp_in, disp), (force_in, force),
            )
        )
    ]
    for copy in copies:
        copy.start()
    for copy in copies:
        copy.wait()
    for counts, starts, out, ahead in (
        (AHEAD, AHEAD_AT, front, True), (BEHIND, BEHIND_AT, back, False)
    ):
        for k in range(8):
            size, at = counts[k], starts[k]
            begin = 0 if ahead else LX - size
            layers = slice(begin, begin + size)
            if k == 7:
                flag = crack[layers].astype(f32)
                out[at : at + size] = jnp.maximum(history[layers], crack_load * flag)
            else:
                field = disp.at[k] if k < 3 else force.at[k - 3] if k < 6 else damage
                out[at : at + size] = field[layers]


FRONT_TILES = (7, 7, 7, 6, 6, 6, 7, 7, 7, 6, 6)
BACK_TILES = (5,) * 11
FRONT_TILES_AT = tuple(sum(FRONT_TILES[:k]) for k in range(11))
BACK_TILES_AT = tuple(sum(BACK_TILES[:k]) for k in range(11))


def corner_kernel(high, low, front, back):
    for counts, starts, out, ahead in (
        (FRONT_TILES, FRONT_TILES_AT, front, True), (BACK_TILES, BACK_TILES_AT, back, False)
    ):
        for k in range(11):
            size, at = counts[k], starts[k]
            begin = 0 if ahead else LX - size
            source = high.at[k] if k < 6 else low.at[k - 6]
            out[at : at + size] = source[begin : begin + size]


class Corner:
    def __init__(self, ref, starts, offset):
        self.ref, self.starts, self.offset = ref, starts, offset

    def __getitem__(self, key):
        return self.ref[self.starts[key[0] + self.offset] + key[1]]


def stress(u, n, gain, ahead):
    dx = [n[j] - u[j] for j in range(3)]
    dy = [next_row(u[j]) - u[j] for j in range(3)]
    dz = [ahead[j] - u[j] for j in range(3)]
    twice = gain + gain
    part = 0.75 * (dx[0] + dy[1] + dz[2])
    return (
        twice * (dx[0] + part),
        twice * (dy[1] + part),
        twice * (dz[2] + part),
        gain * (dx[1] + dy[0]),
        gain * (dx[2] + dz[0]),
        gain * (dy[2] + dz[1]),
    )


def divergence(u, s, before, diag):
    s00, s11, s22, s01, s02, s12 = s
    return (
        diag * u[0] + before[0] + last_row(s01) + last_lane(s02) - (s00 + s01 + s02),
        diag * u[1] + before[1] + last_row(s11) + last_lane(s12) - (s01 + s11 + s12),
        diag * u[2] + before[2] + last_row(s12) + last_lane(s22) - (s02 + s12 + s22),
    )


def vector(ref, i):
    return tuple(ref[j, i] for j in range(3))


def sweep(source, gain, begin, end, diag, store, unroll=None):
    u, n = vector(source, begin), vector(source, begin + 1)
    s = stress(u, n, gain[begin], [next_lane(x) for x in u])

    def step(i, carry):
        before, u, ahead = carry
        n = vector(source, i + 1)
        s = stress(u, n, gain[i], ahead)
        ahead = tuple(next_lane(x) for x in n)
        store(i, divergence(u, s, before, diag))
        return (s[0], s[3], s[4]), n, ahead

    carry = ((s[0], s[3], s[4]), n, tuple(next_lane(x) for x in n))
    if unroll is None:
        for i in range(begin + 1, end):
            carry = step(i, carry)
    else:
        lax.fori_loop(begin + 1, end, step, carry, unroll=unroll)


def store_to(ref, mask, flag=None, load=None):
    def store(i, image):
        for j in range(3):
            value = image[j] if load is None else load(j, i) - image[j]
            own, rest = value[0:LY], value[LY:ROWS] * mask
            if flag is not None:
                own, rest = own * flag, rest * flag
            ref[j, i, 0:LY] = own
            ref[j, i, LY:ROWS] = rest

    return store


def fold(x):
    return x[0:8] + x[8:16] + x[16:24] + x[24:32]


def moments_out(out, sums):
    lane = lanes((1, LZ))
    row = jnp.zeros((1, LZ), f32)
    for k, value in enumerate(sums):
        total = jnp.sum(jnp.sum(value, axis=0, keepdims=True), axis=1, keepdims=True)
        row = jnp.where(lane == k, total, row)
    out[...] = jnp.broadcast_to(row, out.shape)


def elastic_moments(v0, v1, v2, gain):
    def add(i, acc):
        u = vector(v2, i)
        up = [next_row(x)[0:LY] for x in u]
        u = [x[0:LY] for x in u]
        dx = [v2[j, i + 1, 0:LY] - u[j] for j in range(3)]
        dy = [up[j] - u[j] for j in range(3)]
        dz = [next_lane(u[j]) - u[j] for j in range(3)]
        trace = dx[0] + dy[1] + dz[2]
        e01, e02, e12 = dx[1] + dy[0], dx[2] + dz[0], dy[2] + dz[1]
        work = 2.0 * (dx[0] * dx[0] + dy[1] * dy[1] + dz[2] * dz[2])
        work = work + 1.5 * (trace * trace) + (e01 * e01 + e02 * e02 + e12 * e12)
        work = gain[i, 0:LY] * work
        a = [v0[j, i, 0:LY] for j in range(3)]
        b = [v1[j, i, 0:LY] for j in range(3)]

        def dot(x, y):
            return x[0] * y[0] + x[1] * y[1] + x[2] * y[2]

        square = dot(u, u)
        new = (
            dot(a, a), dot(a, b), dot(b, b), dot(b, u), square,
            work + (spring_term - SHIFT_U) * square,
        )
        return tuple(x + fold(y) for x, y in zip(acc, new))

    return add


def inner_kernel(
    disp, force, damage, history, crack, high, low, flags,
    wide, load, gain, v0, v1, v2, short_damage, past, partial,
):
    mask = row_mask(flags)

    def assemble(k, carry):
        i = OFF + k
        for j in range(3):
            wide[j, i, 0:LY] = disp[j, k]
            wide[j, i, LY : LY + 8] = high[j, k] * flags[3]
            wide[j, i, LY + 8 : ROWS] = low_tile(low, j, k) * flags[2]
            load[j, k, 0:LY] = force[j, k]
            load[j, k, LY : LY + 8] = high[3 + j, k]
            load[j, k, LY + 8 : ROWS] = low_tile(low, 3 + j, k)
        own = damage[k]
        above, below = damage_tiles(high, low, k)
        short_damage[i, 0:LY] = own
        short_damage[i, LY:SHORT] = brief(above * flags[3], below * flags[2])
        left = 1.0 - own
        gain[i, 0:LY] = left * left + stiff_floor
        left = 1.0 - above
        gain[i, LY : LY + 8] = (left * left + stiff_floor) * mask[0:8]
        left = 1.0 - below
        gain[i, LY + 8 : ROWS] = (left * left + stiff_floor) * mask[8:16]
        past[i, 0:LY] = jnp.maximum(history[k], crack_load * crack[k].astype(f32))
        past[i, LY:SHORT] = past_tile(high, low, k)
        return carry

    lax.fori_loop(0, LX, assemble, 0, unroll=2)
    diag = spring_term - SHIFT_U
    first = store_to(v0, mask, load=lambda j, i: load[j, i - OFF])
    sweep(wide, gain, OFF, OFF + 15, spring_term, first, unroll=UNROLL)
    sweep(v0, gain, OFF + 1, OFF + 14, diag, store_to(v1, mask), unroll=UNROLL)
    sweep(v1, gain, OFF + 2, OFF + 13, diag, store_to(v2, mask), unroll=UNROLL)
    zero = jnp.zeros((8, LZ), f32)
    add = elastic_moments(v0, v1, v2, gain)
    for k, value in enumerate(
        lax.fori_loop(OFF + 3, OFF + 12, add, (zero,) * 6, unroll=3)
    ):
        partial[k] = value


UNROLL = 4


def outer_kernel(
    wide_in, load, gain_in, v0_in, v1_in, v2_in, short_in, past_in, partial,
    ahead, behind, ahead_corner, behind_corner, flags,
    wide, gain, v0, v1, v2, short_damage, past, sums, edge_load,
):
    mask = row_mask(flags)
    for counts, starts, high_side, middle, corner, tiles, flag in (
        (AHEAD, AHEAD_AT, True, ahead, ahead_corner, FRONT_TILES_AT, flags[1]),
        (BEHIND, BEHIND_AT, False, behind, behind_corner, BACK_TILES_AT, flags[0]),
    ):
        above, below = Corner(corner, tiles, 0), Corner(corner, tiles, 6)
        for k in range(8):
            for c in range(counts[k]):
                own = middle[starts[k] + c]
                i = OFF + LX + c if high_side else OFF - counts[k] + c
                layer = c if high_side else 5 - counts[k] + c
                if k == 7:
                    past[i, 0:LY] = own
                    past[i, LY:SHORT] = past_tile(above, below, layer)
                    continue
                if k < 6:
                    high, low = above[k, layer], low_tile(below, k, layer)
                else:
                    high, low = damage_tiles(above, below, layer)
                if k < 3:
                    into = wide.at[k, i]
                    own = own * flag
                    high = high * (flag * flags[3])
                    low = low * (flag * flags[2])
                elif k < 6:
                    into = edge_load.at[k - 3, i - OFF - LX + 4 if high_side else i - 1]
                else:
                    into = gain.at[i]
                    short_damage[i, 0:LY] = own * flag
                    short_damage[i, LY:SHORT] = brief(
                        high * (flag * flags[3]), low * (flag * flags[2])
                    )
                    own, high, low = (
                        (1.0 - x) * (1.0 - x) + stiff_floor for x in (own, high, low)
                    )
                    own = own * flag
                    high = high * (mask[0:8] * flag)
                    low = low * (mask[8:16] * flag)
                into[0:LY] = own
                into[LY : LY + 8] = high
                into[LY + 8 : ROWS] = low

    def force_at(j, i):
        if i < OFF:
            return edge_load[j, i - 1]
        if i >= OFF + LX:
            return edge_load[j, i - OFF - LX + 4]
        return load[j, i - OFF]

    def both(source, target, low_end, high_begin, diag, load=None):
        def store(i, image):
            flag = flags[0] if i < OFF else flags[1] if i >= OFF + LX else None
            store_to(target, mask, flag, load)(i, image)

        sweep(source, gain, low_end - 6, low_end, diag, store)
        sweep(source, gain, high_begin, high_begin + 8, diag, store)

    diag = spring_term - SHIFT_U
    both(wide, v0, OFF + 1, OFF + 14, spring_term, force_at)
    both(v0, v1, OFF + 2, OFF + 13, diag)
    both(v1, v2, OFF + 3, OFF + 12, diag)

    add = elastic_moments(v0, v1, v2, gain)
    acc = tuple(partial[k] for k in range(6))
    for i in (*range(OFF, OFF + 3), *range(OFF + 12, OFF + 16)):
        acc = add(i, acc)
    moments_out(sums, acc)


def coefficients(gathered, shift):
    row = jnp.sum(gathered[...], axis=0, keepdims=True)
    lane = lanes((1, LZ))
    mu = [
        jnp.broadcast_to(
            jnp.sum(jnp.where(lane == k, row, 0.0), axis=1, keepdims=True), (1, LZ)
        )
        for k in range(6)
    ]

    def inner(a, b, up=0):
        total = None
        for i, x in enumerate(a):
            for j, y in enumerate(b):
                term = x * y * mu[i + j + up]
                total = term if total is None else total + term
        return total

    one = jnp.ones((1, LZ), f32)
    resid, direction = [one], [one]
    found = []
    norm = mu[0]
    for number in range(3):
        work = inner(direction, direction, 1) + shift * inner(direction, direction)
        alpha = norm / work
        for i, x in enumerate(direction):
            if i < len(found):
                found[i] = found[i] + alpha * x
            else:
                found.append(alpha * x)
        if number < 2:
            image = [shift * x for x in direction] + [jnp.zeros((1, LZ), f32)]
            for i, x in enumerate(direction):
                image[i + 1] = image[i + 1] + x
            resid = [
                (resid[i] if i < len(resid) else 0.0) - alpha * x for i, x in enumerate(image)
            ]
            new = inner(resid, resid)
            ratio = new / norm
            direction = [
                x + ratio * direction[i] if i < len(direction) else x
                for i, x in enumerate(resid)
            ]
            norm = new
    return found


def damage_kernel(
    gathered, wide, v0, v1, v2, short_damage, past, flags,
    moved_out, found_out, w0, w1, w2, sums, now, drive, moved, found, sem,
):
    a0, a1, a2 = coefficients(gathered, SHIFT_U)

    def current(j, i):
        value = wide[j, i] + a0 * v0[j, i] + a1 * v1[j, i] + a2 * v2[j, i]
        now[j, i, 0:LY] = value[0:LY]
        now[j, i, LY:SHORT] = brief(value[LY : LY + 8], value[LY + 8 : ROWS])
        return value

    def middle(i, carry):
        for j in range(3):
            moved[j, i - OFF] = current(j, i)[0:LY]
        return carry

    lax.fori_loop(OFF, OFF + LX, middle, 0, unroll=2)
    moved_copy = pltpu.make_async_copy(moved, moved_out, sem.at[0])
    moved_copy.start()
    for i in (OFF - 2, OFF - 1, *range(OFF + LX, OFF + LX + 4)):
        for j in range(3):
            current(j, i)

    row = lax.broadcasted_iota(jnp.int32, (8, LZ), 0)
    mask = jnp.where(row < 4, flags[3], flags[2])

    def energy(i):
        u, n = vector(now, i), vector(now, i + 1)
        dx = [n[j] - u[j] for j in range(3)]
        dy = [next_row(u[j]) - u[j] for j in range(3)]
        dz = [next_lane(u[j]) - u[j] for j in range(3)]
        trace = dx[0] + dy[1] + dz[2]
        e01, e02, e12 = dx[1] + dy[0], dx[2] + dz[0], dy[2] + dz[1]
        squares = dx[0] * dx[0] + dy[1] * dy[1] + dz[2] * dz[2]
        squares = squares + 0.5 * (e01 * e01 + e02 * e02 + e12 * e12)
        positive = jnp.maximum(trace, 0.0)
        return bulk_half * (positive * positive) + (squares - trace * trace * (1.0 / 3.0))

    def step(i, carry):
        value = jnp.maximum(past[i], energy(i))
        drive[i] = value
        found[i - OFF] = value[0:LY]
        return carry

    lax.fori_loop(OFF, OFF + LX, step, 0, unroll=4)
    found_copy = pltpu.make_async_copy(found, found_out, sem.at[1])
    found_copy.start()
    for i in (OFF - 2, OFF - 1, *range(OFF + LX, OFF + LX + 3)):
        drive[i] = jnp.maximum(past[i], energy(i))

    def flag_of(i):
        return jnp.where(i < OFF, flags[0], jnp.where(i >= OFF + LX, flags[1], 1.0))

    def apply(source, begin, end, make, target):
        def step(i, carry):
            before, here = carry
            n = source[i + 1]
            beside = before + n + next_row(here) + last_row(here)
            beside = beside + next_lane(here) + last_lane(here)
            value = make(i, here, beside) * flag_of(i)
            target[i, 0:LY] = value[0:LY]
            target[i, LY:SHORT] = value[LY:SHORT] * mask
            return here, n

        lax.fori_loop(begin, end, step, (source[begin - 1], source[begin]), unroll=7)

    full = tough_ratio + 6.0 * length_term

    def start(i, here, beside):
        twice = 2.0 * drive[i]
        return twice - ((full + twice) * here - length_term * beside)

    def image(i, here, beside):
        return ((full - SHIFT_D) + 2.0 * drive[i]) * here - length_term * beside

    apply(short_damage, OFF - 2, OFF + LX + 3, start, w0)
    apply(w0, OFF - 1, OFF + LX + 2, image, w1)
    apply(w1, OFF, OFF + LX + 1, image, w2)

    lane = lanes((LY, LZ))
    row = lax.broadcasted_iota(jnp.int32, (LY, LZ), 0)
    edge = jnp.where(lane == 0, length_term, 0.0)
    edge = edge + jnp.where(row == 0, length_term * (1.0 - flags[2]), 0.0)
    edge = edge + (tough_ratio - SHIFT_D)

    def add(i, acc):
        wide_now = w2[i]
        u = wide_now[0:LY]
        dx = w2[i + 1, 0:LY] - u
        dy = next_row(wide_now)[0:LY] - u
        dz = next_lane(u) - u
        side = jnp.where(i == OFF, length_term * (1.0 - flags[0]), 0.0)
        square = u * u
        work = (edge + side + 2.0 * drive[i, 0:LY]) * square
        work = work + length_term * (dx * dx + dy * dy + dz * dz)
        a, b = w0[i, 0:LY], w1[i, 0:LY]
        new = (a * a, a * b, b * b, b * u, square, work)
        return tuple(x + fold(y) for x, y in zip(acc, new))

    zero = jnp.zeros((8, LZ), f32)
    moments_out(sums, lax.fori_loop(OFF, OFF + LX, add, (zero,) * 6, unroll=4))
    moved_copy.wait()
    found_copy.wait()


def update_kernel(gathered, damage, w0, w1, w2, out):
    b0, b1, b2 = coefficients(gathered, SHIFT_D)

    def step(c, carry):
        i = OFF + c
        image = b0 * w0[i, 0:LY] + b1 * w1[i, 0:LY] + b2 * w2[i, 0:LY]
        out[c] = damage[c] + image
        return carry

    lax.fori_loop(0, LX, step, 0, unroll=2)


def send(values, dx, dy):
    axis, step = ("gx", dx) if dx else ("gy", dy)
    size = lax.axis_size(axis)
    return lax.ppermute(values, axis, [(i, (i + step) % size) for i in range(size)])


def step(displacement, force, damage, history, crack_flags):
    axes = ("gx", "gy")
    count = lax.axis_size(axes)
    ix, iy = lax.axis_index("gx"), lax.axis_index("gy")
    flags = jnp.stack(
        [ix > 0, ix < lax.axis_size("gx") - 1, iy > 0, iy < lax.axis_size("gy") - 1]
    ).astype(f32)

    def gather(sums):
        return lax.all_to_all(sums, axes, 0, 0, tiled=True)

    given = (displacement, force, damage, history, crack_flags)
    edge_rows, edge_flags = (8, LX, 8, LZ), pltpu.VMEM((LX, 8, LZ), jnp.int32)
    first, last = call(
        rows_kernel,
        [(6, LX, 8, LZ), (5, LX, 8, LZ)],
        [edge_rows, edge_rows, edge_flags, edge_flags, pltpu.SemaphoreType.DMA((10,))],
        hbm=True,
    )(*given, flags=flags)
    disp, load, old, history, crack, front, back = call(
        bulk_kernel,
        [(3, *FIELD), (3, *FIELD), FIELD, FIELD, fast_as(FIELD, jnp.int32)]
        + [(FRONT, LY, LZ), (BACK, LY, LZ)],
        [pltpu.SemaphoreType.DMA((5,))],
        hbm=True,
    )(*given)
    high = send(first, 0, -1)
    low = send(last, 0, 1)
    ahead = send(front, -1, 0)
    behind = send(back, 1, 0)
    corners = call(
        corner_kernel, [(sum(FRONT_TILES), 8, LZ), (sum(BACK_TILES), 8, LZ)]
    )(high, low)
    ahead_corner = send(corners[0], -1, 0)
    behind_corner = send(corners[1], 1, 0)
    wide, load, gain, v0, v1, v2, short_damage, past, partial = call(
        inner_kernel,
        [VECTOR, (3, LX, ROWS, LZ), SCALAR, VECTOR, VECTOR, VECTOR, BRIEF, BRIEF, (6, 8, LZ)],
    )(disp, load, old, history, crack, high, low, flags=flags)
    wide, gain, v0, v1, v2, short_damage, past, sums = call(
        outer_kernel,
        [VECTOR, SCALAR, VECTOR, VECTOR, VECTOR, BRIEF, BRIEF, (count, LZ)],
        scratch=[(3, 10, ROWS, LZ)],
        aliases={0: 0, 2: 1, 3: 2, 4: 3, 5: 4, 6: 5, 7: 6},
    )(
        wide, load, gain, v0, v1, v2, short_damage, past, partial,
        ahead, behind, ahead_corner, behind_corner, flags=flags,
    )
    moved, found, w0, w1, w2, sums = call(
        damage_kernel,
        [whole(3, LX, LY, LZ), whole(LX, LY, LZ), BRIEF, BRIEF, BRIEF, (count, LZ)],
        [(3, DEPTH, SHORT, LZ), BRIEF, (3, *FIELD), FIELD, pltpu.SemaphoreType.DMA((2,))],
        far=2,
    )(gather(sums), wide, v0, v1, v2, short_damage, past, flags=flags)
    (damage_out,) = call(update_kernel, [whole(LX, LY, LZ)])(
        gather(sums), old, w0, w1, w2
    )
    return moved, damage_out, found


def solution(mesh):
    return jax.shard_map(
        step,
        mesh=mesh,
        in_specs=(
            P(None, "gx", "gy", None),
            P(None, "gx", "gy", None),
            P("gx", "gy", None),
            P("gx", "gy", None),
            P("gx", "gy", None),
        ),
        out_specs=(P(None, "gx", "gy", None), P("gx", "gy", None), P("gx", "gy", None)),
        check_vma=False,
    )
```

```python
import jax
import jax.numpy as jnp
from jax import lax
from jax.experimental import pallas as pl
from jax.experimental.pallas import tpu as pltpu
from jax.sharding import PartitionSpec as P


INTERPRET = False
f32 = jnp.float32

spring_term = 0.5
stiff_floor = 0.001
crack_load = 4.0
tough_ratio = 0.5
length_term = 2.0
bulk_half = 0.5 * (1.5 + 2.0 / 3.0)

LX, LY, LZ = 16, 32, 128
ROWS, SHORT, DEPTH, OFF = 48, 40, 28, 5

SHIFT_U = 14.0
SHIFT_D = 18.0

VECTOR = (3, DEPTH, ROWS, LZ)
SCALAR = (DEPTH, ROWS, LZ)
BRIEF = (DEPTH, SHORT, LZ)
FIELD = (LX, LY, LZ)


def fast(shape):
    return fast_as(shape, f32)


def fast_as(shape, kind):
    return jax.ShapeDtypeStruct(shape, kind) if INTERPRET else pltpu.VMEM(shape, kind)


def whole(*shape):
    return jax.ShapeDtypeStruct(shape, f32)


def call(kernel, outs, scratch=(), limit=8 << 20, aliases=None, hbm=False, far=0):
    vmem = pl.BlockSpec(memory_space=pltpu.VMEM)
    smem = pl.BlockSpec(memory_space=pltpu.SMEM)

    def run(*args, flags=None):
        specs = [pl.BlockSpec(memory_space=pltpu.HBM) if hbm else vmem] * len(args)
        if hbm and not INTERPRET:
            args = [pltpu.with_memory_space_constraint(x, pltpu.HBM) for x in args]
        if flags is not None:
            args, specs = (*args, flags), specs + [smem]
        return pl.pallas_call(
            kernel,
            out_shape=[fast(s) if isinstance(s, tuple) else s for s in outs],
            in_specs=specs,
            out_specs=[pl.BlockSpec(memory_space=pltpu.HBM)] * far + [vmem] * (len(outs) - far),
            scratch_shapes=[pltpu.VMEM(s, f32) if isinstance(s, tuple) else s for s in scratch],
            input_output_aliases=aliases or {},
            compiler_params=pltpu.CompilerParams(vmem_limit_bytes=limit),
            interpret=INTERPRET,
        )(*args)

    return run


def roll(x, shift, axis):
    return pltpu.roll(x, shift % x.shape[axis], axis)


def next_row(x):
    return roll(x, -1, 0)


def last_row(x):
    return roll(x, 1, 0)


def lanes(shape):
    return lax.broadcasted_iota(jnp.int32, shape, 1)


def next_lane(x):
    return jnp.where(lanes(x.shape) == LZ - 1, 0.0, roll(x, -1, 1))


def last_lane(x):
    return jnp.where(lanes(x.shape) == 0, 0.0, roll(x, 1, 1))


def tile_row():
    return lax.broadcasted_iota(jnp.int32, (8, LZ), 0)


def pack_first(u, load, damage, past):
    row = tile_row()
    return [
        jnp.where(row < 6, u[0], roll(damage, 6, 0)),
        jnp.where(row < 6, u[1], roll(damage, 4, 0)),
        jnp.where(row < 6, u[2], roll(past, 6, 0)),
        jnp.where(row < 5, load[0], roll(load[2], 5, 0)),
        jnp.where(
            row < 5, load[1], jnp.where(row == 5, roll(damage, 1, 0), roll(load[2], 3, 0))
        ),
    ]


def pack_last(u, load, damage, past):
    row = tile_row()
    return [
        jnp.where(row < 2, roll(damage, -2, 0), u[0]),
        jnp.where(row < 2, roll(damage, -4, 0), u[1]),
        jnp.where(row < 2, roll(damage, -6, 0), u[2]),
        jnp.where(row < 3, roll(load[2], -3, 0), load[0]),
        jnp.where(
            row < 3, jnp.where(row == 2, roll(past, -3, 0), roll(load[2], -6, 0)), load[1]
        ),
    ]


def high_tile(high, field, k):
    if field < 5:
        return high[field, k]
    return jnp.where(tile_row() < 3, roll(high[3, k], 3, 0), roll(high[4, k], 5, 0))


def low_tile(low, field, k):
    if field < 5:
        return low[field, k]
    return jnp.where(tile_row() < 6, roll(low[3, k], 3, 0), roll(low[4, k], 6, 0))


def damage_tiles(high, low, k):
    row = tile_row()
    above = jnp.where(row < 2, roll(high[0, k], 2, 0), roll(high[1, k], 4, 0))
    above = jnp.where(row < 4, above, roll(high[4, k], -1, 0))
    below = jnp.where(row < 4, roll(low[0, k], 2, 0), roll(low[1, k], 4, 0))
    below = jnp.where(row < 6, below, roll(low[2, k], 6, 0))
    return above, below


def past_tile(high, low, k, shared, place):
    row = tile_row()
    below = jnp.where(row < 6, roll(low[4, k], 3, 0), roll(shared, 6 - 2 * place, 0))
    return jnp.where(row < 4, roll(high[2, k], 2, 0), below)


class Tiles:
    def __init__(self, ref, starts):
        self.ref, self.starts = ref, starts

    def __getitem__(self, key):
        return self.ref[self.starts[key[0]] + key[1]]


def brief(above, below):
    return jnp.where(tile_row() < 4, above, below)


def row_mask(flags):
    row = lax.broadcasted_iota(jnp.int32, (ROWS - LY, LZ), 0)
    return jnp.where(row < 8, flags[3], flags[2])


AHEAD = (7, 7, 7, 6, 6, 6, 6, 3)
BEHIND = (5, 5, 5, 4, 4, 4, 5, 2)
AHEAD_AT = tuple(sum(AHEAD[:k]) for k in range(8))
BEHIND_AT = tuple(sum(BEHIND[:k]) for k in range(8))
FRONT, BACK = sum(AHEAD), sum(BEHIND)


def rows_kernel(
    disp, force, damage, history, crack, flags,
    first, last, top, bottom, top_crack, bottom_crack, sem,
):
    copies = []
    for rows, into, into_crack in ((0, top, top_crack), (24, bottom, bottom_crack)):
        for source, target in (
            (crack.at[:, rows : rows + 8], into_crack),
            (history.at[:, rows : rows + 8], into.at[7]),
            (damage.at[:, rows : rows + 8], into.at[6]),
            (disp.at[:, :, rows : rows + 8], into.at[0:3]),
            (force.at[:, :, rows : rows + 8], into.at[3:6]),
        ):
            copies.append(pltpu.make_async_copy(source, target, sem.at[len(copies)]))
    for copy in copies:
        copy.start()
    for copy in copies:
        copy.wait()

    row = tile_row()

    def step(group, carry):
        shared = jnp.zeros((8, LZ), f32)
        for place in range(4):
            k = 4 * group + place
            for into, flag, out, pack in (
                (top, top_crack, first, pack_first), (bottom, bottom_crack, last, pack_last)
            ):
                past = jnp.maximum(into[7, k], crack_load * flag[k].astype(f32))
                tiles = pack(
                    [into[j, k] for j in range(3)], [into[3 + j, k] for j in range(3)],
                    into[6, k], past,
                )
                for n, tile in enumerate(tiles):
                    out[n * LX + k] = tile
                if out is last:
                    here = (row >= 2 * place) & (row < 2 * place + 2)
                    shared = jnp.where(here, roll(past, 2 * place + 2, 0), shared)
        last[5 * LX + group] = shared
        return carry

    lax.fori_loop(0, 4, step, 0)


def bulk_kernel(
    disp_in, force_in, damage_in, history_in, crack_in,
    disp, force, damage, history, crack, front, back, sem,
):
    copies = [
        pltpu.make_async_copy(source, target, sem.at[n])
        for n, (source, target) in enumerate(
            (
                (crack_in, crack), (history_in, history), (damage_in, damage),
                (disp_in, disp), (force_in, force),
            )
        )
    ]
    for copy in copies:
        copy.start()
    for copy in copies:
        copy.wait()
    for counts, starts, out, ahead in (
        (AHEAD, AHEAD_AT, front, True), (BEHIND, BEHIND_AT, back, False)
    ):
        for k in range(8):
            size, at = counts[k], starts[k]
            begin = 0 if ahead else LX - size
            layers = slice(begin, begin + size)
            if k == 7:
                flag = crack[layers].astype(f32)
                out[at : at + size] = jnp.maximum(history[layers], crack_load * flag)
            else:
                field = disp.at[k] if k < 3 else force.at[k - 3] if k < 6 else damage
                out[at : at + size] = field[layers]


FRONT_TILES = (7, 7, 7, 6, 6, 7, 7, 7, 6, 6, 1)
BACK_TILES = (5,) * 10 + (1,)
FRONT_TILES_AT = tuple(sum(FRONT_TILES[:k]) for k in range(11))
BACK_TILES_AT = tuple(sum(BACK_TILES[:k]) for k in range(11))
ROW_TILES_AT = tuple(LX * k for k in range(6))


def corner_kernel(high, low, front, back):
    for counts, starts, out, ahead in (
        (FRONT_TILES, FRONT_TILES_AT, front, True), (BACK_TILES, BACK_TILES_AT, back, False)
    ):
        for k in range(10):
            size, at = counts[k], starts[k]
            begin = LX * (k % 5) + (0 if ahead else LX - size)
            source = high if k < 5 else low
            out[at : at + size] = source[begin : begin + size]
        out[starts[10]] = low[5 * LX + (0 if ahead else 3)]


def stress(u, n, gain, ahead):
    dx = [n[j] - u[j] for j in range(3)]
    dy = [next_row(u[j]) - u[j] for j in range(3)]
    dz = [ahead[j] - u[j] for j in range(3)]
    twice = gain + gain
    part = 0.75 * (dx[0] + dy[1] + dz[2])
    return (
        twice * (dx[0] + part),
        twice * (dy[1] + part),
        twice * (dz[2] + part),
        gain * (dx[1] + dy[0]),
        gain * (dx[2] + dz[0]),
        gain * (dy[2] + dz[1]),
    )


def divergence(u, s, before, diag):
    s00, s11, s22, s01, s02, s12 = s
    return (
        diag * u[0] + before[0] + last_row(s01) + last_lane(s02) - (s00 + s01 + s02),
        diag * u[1] + before[1] + last_row(s11) + last_lane(s12) - (s01 + s11 + s12),
        diag * u[2] + before[2] + last_row(s12) + last_lane(s22) - (s02 + s12 + s22),
    )


def vector(ref, i):
    return tuple(ref[j, i] for j in range(3))


def sweep(source, gain, begin, end, diag, store, unroll=None):
    u, n = vector(source, begin), vector(source, begin + 1)
    s = stress(u, n, gain[begin], [next_lane(x) for x in u])

    def step(i, carry):
        before, u, ahead = carry
        n = vector(source, i + 1)
        s = stress(u, n, gain[i], ahead)
        ahead = tuple(next_lane(x) for x in n)
        store(i, divergence(u, s, before, diag))
        return (s[0], s[3], s[4]), n, ahead

    carry = ((s[0], s[3], s[4]), n, tuple(next_lane(x) for x in n))
    if unroll is None:
        for i in range(begin + 1, end):
            carry = step(i, carry)
    else:
        lax.fori_loop(begin + 1, end, step, carry, unroll=unroll)


def store_to(ref, mask, flag=None, load=None):
    def store(i, image):
        for j in range(3):
            value = image[j] if load is None else load(j, i) - image[j]
            own, rest = value[0:LY], value[LY:ROWS] * mask
            if flag is not None:
                own, rest = own * flag, rest * flag
            ref[j, i, 0:LY] = own
            ref[j, i, LY:ROWS] = rest

    return store


def fold(x):
    return x[0:8] + x[8:16] + x[16:24] + x[24:32]


def moments_out(out, sums):
    lane = lanes((1, LZ))
    row = jnp.zeros((1, LZ), f32)
    for k, value in enumerate(sums):
        total = jnp.sum(jnp.sum(value, axis=0, keepdims=True), axis=1, keepdims=True)
        row = jnp.where(lane == k, total, row)
    out[...] = jnp.broadcast_to(row, out.shape)


def elastic_moments(v0, v1, v2, gain):
    def add(i, acc):
        u = vector(v2, i)
        up = [next_row(x)[0:LY] for x in u]
        u = [x[0:LY] for x in u]
        dx = [v2[j, i + 1, 0:LY] - u[j] for j in range(3)]
        dy = [up[j] - u[j] for j in range(3)]
        dz = [next_lane(u[j]) - u[j] for j in range(3)]
        trace = dx[0] + dy[1] + dz[2]
        e01, e02, e12 = dx[1] + dy[0], dx[2] + dz[0], dy[2] + dz[1]
        work = 2.0 * (dx[0] * dx[0] + dy[1] * dy[1] + dz[2] * dz[2])
        work = work + 1.5 * (trace * trace) + (e01 * e01 + e02 * e02 + e12 * e12)
        work = gain[i, 0:LY] * work
        a = [v0[j, i, 0:LY] for j in range(3)]
        b = [v1[j, i, 0:LY] for j in range(3)]

        def dot(x, y):
            return x[0] * y[0] + x[1] * y[1] + x[2] * y[2]

        square = dot(u, u)
        new = (
            dot(a, a), dot(a, b), dot(b, b), dot(b, u), square,
            work + (spring_term - SHIFT_U) * square,
        )
        return tuple(x + fold(y) for x, y in zip(acc, new))

    return add


def inner_kernel(
    disp, force, damage, history, crack, high, low, flags,
    wide, load, gain, v0, v1, v2, short_damage, past, partial,
):
    mask = row_mask(flags)

    high, low = Tiles(high, ROW_TILES_AT), Tiles(low, ROW_TILES_AT)

    def assemble(group, carry):
        for place in range(4):
            k = 4 * group + place
            i = OFF + k
            for j in range(3):
                wide[j, i, 0:LY] = disp[j, k]
                wide[j, i, LY : LY + 8] = high[j, k] * flags[3]
                wide[j, i, LY + 8 : ROWS] = low[j, k] * flags[2]
                load[j, k, 0:LY] = force[j, k]
                load[j, k, LY : LY + 8] = high_tile(high, 3 + j, k)
                load[j, k, LY + 8 : ROWS] = low_tile(low, 3 + j, k)
            own = damage[k]
            above, below = damage_tiles(high, low, k)
            short_damage[i, 0:LY] = own
            short_damage[i, LY:SHORT] = brief(above * flags[3], below * flags[2])
            left = 1.0 - own
            gain[i, 0:LY] = left * left + stiff_floor
            left = 1.0 - above
            gain[i, LY : LY + 8] = (left * left + stiff_floor) * mask[0:8]
            left = 1.0 - below
            gain[i, LY + 8 : ROWS] = (left * left + stiff_floor) * mask[8:16]
            past[i, 0:LY] = jnp.maximum(history[k], crack_load * crack[k].astype(f32))
            past[i, LY:SHORT] = past_tile(high, low, k, low[5, group], place)
        return carry

    lax.fori_loop(0, 4, assemble, 0)
    diag = spring_term - SHIFT_U
    first = store_to(v0, mask, load=lambda j, i: load[j, i - OFF])
    sweep(wide, gain, OFF, OFF + 15, spring_term, first, unroll=UNROLL)
    sweep(v0, gain, OFF + 1, OFF + 14, diag, store_to(v1, mask), unroll=UNROLL)
    sweep(v1, gain, OFF + 2, OFF + 13, diag, store_to(v2, mask), unroll=UNROLL)
    zero = jnp.zeros((8, LZ), f32)
    add = elastic_moments(v0, v1, v2, gain)
    for k, value in enumerate(
        lax.fori_loop(OFF + 3, OFF + 12, add, (zero,) * 6, unroll=3)
    ):
        partial[k] = value


UNROLL = 4


def outer_kernel(
    wide_in, load, gain_in, v0_in, v1_in, v2_in, short_in, past_in, partial,
    ahead, behind, ahead_corner, behind_corner, flags,
    wide, gain, v0, v1, v2, short_damage, past, sums, edge_load,
):
    mask = row_mask(flags)
    for counts, starts, high_side, middle, corner, tiles, flag in (
        (AHEAD, AHEAD_AT, True, ahead, ahead_corner, FRONT_TILES_AT, flags[1]),
        (BEHIND, BEHIND_AT, False, behind, behind_corner, BACK_TILES_AT, flags[0]),
    ):
        above, below = Tiles(corner, tiles[:5]), Tiles(corner, tiles[5:])
        for k in range(8):
            for c in range(counts[k]):
                own = middle[starts[k] + c]
                i = OFF + LX + c if high_side else OFF - counts[k] + c
                layer = c if high_side else 5 - counts[k] + c
                if k == 7:
                    past[i, 0:LY] = own
                    past[i, LY:SHORT] = past_tile(above, below, layer, below[5, 0], (layer if high_side else layer + 3) % 4)
                    continue
                if k < 6:
                    high, low = high_tile(above, k, layer), low_tile(below, k, layer)
                else:
                    high, low = damage_tiles(above, below, layer)
                if k < 3:
                    into = wide.at[k, i]
                    own = own * flag
                    high = high * (flag * flags[3])
                    low = low * (flag * flags[2])
                elif k < 6:
                    into = edge_load.at[k - 3, i - OFF - LX + 4 if high_side else i - 1]
                else:
                    into = gain.at[i]
                    short_damage[i, 0:LY] = own * flag
                    short_damage[i, LY:SHORT] = brief(
                        high * (flag * flags[3]), low * (flag * flags[2])
                    )
                    own, high, low = (
                        (1.0 - x) * (1.0 - x) + stiff_floor for x in (own, high, low)
                    )
                    own = own * flag
                    high = high * (mask[0:8] * flag)
                    low = low * (mask[8:16] * flag)
                into[0:LY] = own
                into[LY : LY + 8] = high
                into[LY + 8 : ROWS] = low

    def force_at(j, i):
        if i < OFF:
            return edge_load[j, i - 1]
        if i >= OFF + LX:
            return edge_load[j, i - OFF - LX + 4]
        return load[j, i - OFF]

    def both(source, target, low_end, high_begin, diag, load=None):
        def store(i, image):
            flag = flags[0] if i < OFF else flags[1] if i >= OFF + LX else None
            store_to(target, mask, flag, load)(i, image)

        sweep(source, gain, low_end - 6, low_end, diag, store)
        sweep(source, gain, high_begin, high_begin + 8, diag, store)

    diag = spring_term - SHIFT_U
    both(wide, v0, OFF + 1, OFF + 14, spring_term, force_at)
    both(v0, v1, OFF + 2, OFF + 13, diag)
    both(v1, v2, OFF + 3, OFF + 12, diag)

    add = elastic_moments(v0, v1, v2, gain)
    acc = tuple(partial[k] for k in range(6))
    for i in (*range(OFF, OFF + 3), *range(OFF + 12, OFF + 16)):
        acc = add(i, acc)
    moments_out(sums, acc)


def coefficients(gathered, shift):
    row = jnp.sum(gathered[...], axis=0, keepdims=True)
    lane = lanes((1, LZ))
    mu = [
        jnp.broadcast_to(
            jnp.sum(jnp.where(lane == k, row, 0.0), axis=1, keepdims=True), (1, LZ)
        )
        for k in range(6)
    ]

    def inner(a, b, up=0):
        total = None
        for i, x in enumerate(a):
            for j, y in enumerate(b):
                term = x * y * mu[i + j + up]
                total = term if total is None else total + term
        return total

    one = jnp.ones((1, LZ), f32)
    resid, direction = [one], [one]
    found = []
    norm = mu[0]
    for number in range(3):
        work = inner(direction, direction, 1) + shift * inner(direction, direction)
        alpha = norm / work
        for i, x in enumerate(direction):
            if i < len(found):
                found[i] = found[i] + alpha * x
            else:
                found.append(alpha * x)
        if number < 2:
            image = [shift * x for x in direction] + [jnp.zeros((1, LZ), f32)]
            for i, x in enumerate(direction):
                image[i + 1] = image[i + 1] + x
            resid = [
                (resid[i] if i < len(resid) else 0.0) - alpha * x for i, x in enumerate(image)
            ]
            new = inner(resid, resid)
            ratio = new / norm
            direction = [
                x + ratio * direction[i] if i < len(direction) else x
                for i, x in enumerate(resid)
            ]
            norm = new
    return found


def damage_kernel(
    gathered, wide, v0, v1, v2, short_damage, past, flags,
    moved_out, found_out, w0, w1, w2, sums, now, drive, moved, found, sem,
):
    a0, a1, a2 = coefficients(gathered, SHIFT_U)

    def current(j, i):
        value = wide[j, i] + a0 * v0[j, i] + a1 * v1[j, i] + a2 * v2[j, i]
        now[j, i, 0:LY] = value[0:LY]
        now[j, i, LY:SHORT] = brief(value[LY : LY + 8], value[LY + 8 : ROWS])
        return value

    def middle(i, carry):
        for j in range(3):
            moved[j, i - OFF] = current(j, i)[0:LY]
        return carry

    lax.fori_loop(OFF, OFF + LX, middle, 0, unroll=2)
    moved_copy = pltpu.make_async_copy(moved, moved_out, sem.at[0])
    moved_copy.start()
    for i in (OFF - 2, OFF - 1, *range(OFF + LX, OFF + LX + 4)):
        for j in range(3):
            current(j, i)

    row = lax.broadcasted_iota(jnp.int32, (8, LZ), 0)
    mask = jnp.where(row < 4, flags[3], flags[2])

    def energy(i):
        u, n = vector(now, i), vector(now, i + 1)
        dx = [n[j] - u[j] for j in range(3)]
        dy = [next_row(u[j]) - u[j] for j in range(3)]
        dz = [next_lane(u[j]) - u[j] for j in range(3)]
        trace = dx[0] + dy[1] + dz[2]
        e01, e02, e12 = dx[1] + dy[0], dx[2] + dz[0], dy[2] + dz[1]
        squares = dx[0] * dx[0] + dy[1] * dy[1] + dz[2] * dz[2]
        squares = squares + 0.5 * (e01 * e01 + e02 * e02 + e12 * e12)
        positive = jnp.maximum(trace, 0.0)
        return bulk_half * (positive * positive) + (squares - trace * trace * (1.0 / 3.0))

    def step(i, carry):
        value = jnp.maximum(past[i], energy(i))
        drive[i] = value
        found[i - OFF] = value[0:LY]
        return carry

    lax.fori_loop(OFF, OFF + LX, step, 0, unroll=4)
    found_copy = pltpu.make_async_copy(found, found_out, sem.at[1])
    found_copy.start()
    for i in (OFF - 2, OFF - 1, *range(OFF + LX, OFF + LX + 3)):
        drive[i] = jnp.maximum(past[i], energy(i))

    def flag_of(i):
        return jnp.where(i < OFF, flags[0], jnp.where(i >= OFF + LX, flags[1], 1.0))

    def apply(source, begin, end, make, target):
        def step(i, carry):
            before, here = carry
            n = source[i + 1]
            beside = before + n + next_row(here) + last_row(here)
            beside = beside + next_lane(here) + last_lane(here)
            value = make(i, here, beside) * flag_of(i)
            target[i, 0:LY] = value[0:LY]
            target[i, LY:SHORT] = value[LY:SHORT] * mask
            return here, n

        lax.fori_loop(begin, end, step, (source[begin - 1], source[begin]), unroll=7)

    full = tough_ratio + 6.0 * length_term

    def start(i, here, beside):
        twice = 2.0 * drive[i]
        return twice - ((full + twice) * here - length_term * beside)

    def image(i, here, beside):
        return ((full - SHIFT_D) + 2.0 * drive[i]) * here - length_term * beside

    apply(short_damage, OFF - 2, OFF + LX + 3, start, w0)
    apply(w0, OFF - 1, OFF + LX + 2, image, w1)
    apply(w1, OFF, OFF + LX + 1, image, w2)

    lane = lanes((LY, LZ))
    row = lax.broadcasted_iota(jnp.int32, (LY, LZ), 0)
    edge = jnp.where(lane == 0, length_term, 0.0)
    edge = edge + jnp.where(row == LY - 1, length_term * (1.0 - flags[3]), 0.0)
    edge = edge + (tough_ratio - SHIFT_D)

    def add(i, acc):
        wide_now = w2[i]
        u = wide_now[0:LY]
        dx = w2[i + 1, 0:LY] - u
        dy = last_row(wide_now)[0:LY] - u
        dz = next_lane(u) - u
        side = jnp.where(i == OFF, length_term * (1.0 - flags[0]), 0.0)
        square = u * u
        work = (edge + side + 2.0 * drive[i, 0:LY]) * square
        work = work + length_term * (dx * dx + dy * dy + dz * dz)
        a, b = w0[i, 0:LY], w1[i, 0:LY]
        new = (a * a, a * b, b * b, b * u, square, work)
        return tuple(x + fold(y) for x, y in zip(acc, new))

    zero = jnp.zeros((8, LZ), f32)
    moments_out(sums, lax.fori_loop(OFF, OFF + LX, add, (zero,) * 6, unroll=4))
    moved_copy.wait()
    found_copy.wait()


def update_kernel(gathered, damage, w0, w1, w2, out):
    b0, b1, b2 = coefficients(gathered, SHIFT_D)

    def step(c, carry):
        i = OFF + c
        image = b0 * w0[i, 0:LY] + b1 * w1[i, 0:LY] + b2 * w2[i, 0:LY]
        out[c] = damage[c] + image
        return carry

    lax.fori_loop(0, LX, step, 0, unroll=2)


def send(values, dx, dy):
    axis, step = ("gx", dx) if dx else ("gy", dy)
    size = lax.axis_size(axis)
    return lax.ppermute(values, axis, [(i, (i + step) % size) for i in range(size)])


def step(displacement, force, damage, history, crack_flags):
    axes = ("gx", "gy")
    count = lax.axis_size(axes)
    ix, iy = lax.axis_index("gx"), lax.axis_index("gy")
    flags = jnp.stack(
        [ix > 0, ix < lax.axis_size("gx") - 1, iy > 0, iy < lax.axis_size("gy") - 1]
    ).astype(f32)

    def gather(sums):
        return lax.all_to_all(sums, axes, 0, 0, tiled=True)

    given = (displacement, force, damage, history, crack_flags)
    edge_rows, edge_flags = (8, LX, 8, LZ), pltpu.VMEM((LX, 8, LZ), jnp.int32)
    first, last = call(
        rows_kernel,
        [(5 * LX, 8, LZ), (5 * LX + 4, 8, LZ)],
        [edge_rows, edge_rows, edge_flags, edge_flags, pltpu.SemaphoreType.DMA((10,))],
        hbm=True,
    )(*given, flags=flags)
    disp, load, old, history, crack, front, back = call(
        bulk_kernel,
        [(3, *FIELD), (3, *FIELD), FIELD, FIELD, fast_as(FIELD, jnp.int32)]
        + [(FRONT, LY, LZ), (BACK, LY, LZ)],
        [pltpu.SemaphoreType.DMA((5,))],
        hbm=True,
    )(*given)
    high = send(first, 0, -1)
    low = send(last, 0, 1)
    ahead = send(front, -1, 0)
    behind = send(back, 1, 0)
    corners = call(corner_kernel, [(sum(FRONT_TILES), 8, LZ), (sum(BACK_TILES), 8, LZ)])(high, low)
    ahead_corner = send(corners[0], -1, 0)
    behind_corner = send(corners[1], 1, 0)
    wide, load, gain, v0, v1, v2, short_damage, past, partial = call(
        inner_kernel,
        [VECTOR, (3, LX, ROWS, LZ), SCALAR, VECTOR, VECTOR, VECTOR, BRIEF, BRIEF, (6, 8, LZ)],
    )(disp, load, old, history, crack, high, low, flags=flags)
    wide, gain, v0, v1, v2, short_damage, past, sums = call(
        outer_kernel,
        [VECTOR, SCALAR, VECTOR, VECTOR, VECTOR, BRIEF, BRIEF, (count, LZ)],
        scratch=[(3, 10, ROWS, LZ)],
        aliases={0: 0, 2: 1, 3: 2, 4: 3, 5: 4, 6: 5, 7: 6},
    )(
        wide, load, gain, v0, v1, v2, short_damage, past, partial,
        ahead, behind, ahead_corner, behind_corner, flags=flags,
    )
    moved, found, w0, w1, w2, sums = call(
        damage_kernel,
        [whole(3, LX, LY, LZ), whole(LX, LY, LZ), BRIEF, BRIEF, BRIEF, (count, LZ)],
        [(3, DEPTH, SHORT, LZ), BRIEF, (3, *FIELD), FIELD, pltpu.SemaphoreType.DMA((2,))],
        far=2,
    )(gather(sums), wide, v0, v1, v2, short_damage, past, flags=flags)
    (damage_out,) = call(update_kernel, [whole(LX, LY, LZ)])(gather(sums), old, w0, w1, w2)
    return moved, damage_out, found


def solution(mesh):
    return jax.shard_map(
        step,
        mesh=mesh,
        in_specs=(
            P(None, "gx", "gy", None),
            P(None, "gx", "gy", None),
            P("gx", "gy", None),
            P("gx", "gy", None),
            P("gx", "gy", None),
        ),
        out_specs=(P(None, "gx", "gy", None), P("gx", "gy", None), P("gx", "gy", None)),
        check_vma=False,
    )
```

```python
import jax
import jax.numpy as jnp
from jax import lax
from jax.experimental import pallas as pl
from jax.experimental.pallas import tpu as pltpu
from jax.sharding import PartitionSpec as P


INTERPRET = False
f32 = jnp.float32

spring_term = 0.5
stiff_floor = 0.001
crack_load = 4.0
tough_ratio = 0.5
length_term = 2.0
bulk_half = 0.5 * (1.5 + 2.0 / 3.0)

LX, LY, LZ = 16, 32, 128
ROWS, SHORT, DEPTH, OFF = 48, 40, 28, 6

SHIFT_U = 14.0
SHIFT_D = 18.0

VECTOR = (3, DEPTH, ROWS, LZ)
SCALAR = (DEPTH, ROWS, LZ)
BRIEF = (DEPTH, SHORT, LZ)
FIELD = (LX, LY, LZ)


def fast(shape):
    return fast_as(shape, f32)


def fast_as(shape, kind):
    return jax.ShapeDtypeStruct(shape, kind) if INTERPRET else pltpu.VMEM(shape, kind)


def whole(*shape):
    return jax.ShapeDtypeStruct(shape, f32)


def call(kernel, outs, scratch=(), limit=8 << 20, aliases=None, hbm=False, far=0):
    vmem = pl.BlockSpec(memory_space=pltpu.VMEM)
    smem = pl.BlockSpec(memory_space=pltpu.SMEM)

    def run(*args, flags=None):
        specs = [pl.BlockSpec(memory_space=pltpu.HBM) if hbm else vmem] * len(args)
        if hbm and not INTERPRET:
            args = [pltpu.with_memory_space_constraint(x, pltpu.HBM) for x in args]
        if flags is not None:
            args, specs = (*args, flags), specs + [smem]
        return pl.pallas_call(
            kernel,
            out_shape=[fast(s) if isinstance(s, tuple) else s for s in outs],
            in_specs=specs,
            out_specs=[pl.BlockSpec(memory_space=pltpu.HBM)] * far + [vmem] * (len(outs) - far),
            scratch_shapes=[pltpu.VMEM(s, f32) if isinstance(s, tuple) else s for s in scratch],
            input_output_aliases=aliases or {},
            compiler_params=pltpu.CompilerParams(vmem_limit_bytes=limit),
            interpret=INTERPRET,
        )(*args)

    return run


def roll(x, shift, axis):
    return pltpu.roll(x, shift % x.shape[axis], axis)


def next_row(x):
    return roll(x, -1, 0)


def last_row(x):
    return roll(x, 1, 0)


def lanes(shape):
    return lax.broadcasted_iota(jnp.int32, shape, 1)


def next_lane(x):
    return jnp.where(lanes(x.shape) == LZ - 1, 0.0, roll(x, -1, 1))


def last_lane(x):
    return jnp.where(lanes(x.shape) == 0, 0.0, roll(x, 1, 1))


def tile_row():
    return lax.broadcasted_iota(jnp.int32, (8, LZ), 0)


def pack_first(u, load, damage, past):
    row = tile_row()
    return [
        jnp.where(row < 6, u[0], roll(damage, 6, 0)),
        jnp.where(row < 6, u[1], roll(damage, 4, 0)),
        jnp.where(row < 6, u[2], roll(past, 6, 0)),
        jnp.where(row < 5, load[0], roll(load[2], 5, 0)),
        jnp.where(
            row < 5, load[1], jnp.where(row == 5, roll(damage, 1, 0), roll(load[2], 3, 0))
        ),
    ]


def pack_last(u, load, damage, past):
    row = tile_row()
    return [
        jnp.where(row < 2, roll(damage, -2, 0), u[0]),
        jnp.where(row < 2, roll(damage, -4, 0), u[1]),
        jnp.where(row < 2, roll(damage, -6, 0), u[2]),
        jnp.where(row < 3, roll(load[2], -3, 0), load[0]),
        jnp.where(
            row < 3, jnp.where(row == 2, roll(past, -3, 0), roll(load[2], -6, 0)), load[1]
        ),
    ]


def high_tile(high, field, k):
    if field < 5:
        return high[field, k]
    return jnp.where(tile_row() < 3, roll(high[3, k], 3, 0), roll(high[4, k], 5, 0))


def low_tile(low, field, k):
    if field < 5:
        return low[field, k]
    return jnp.where(tile_row() < 6, roll(low[3, k], 3, 0), roll(low[4, k], 6, 0))


def damage_tiles(high, low, k):
    row = tile_row()
    above = jnp.where(row < 2, roll(high[0, k], 2, 0), roll(high[1, k], 4, 0))
    above = jnp.where(row < 4, above, roll(high[4, k], -1, 0))
    below = jnp.where(row < 4, roll(low[0, k], 2, 0), roll(low[1, k], 4, 0))
    below = jnp.where(row < 6, below, roll(low[2, k], 6, 0))
    return above, below


def past_tile(high, low, k, shared, place):
    row = tile_row()
    below = jnp.where(row < 6, roll(low[4, k], 3, 0), roll(shared, 6 - 2 * place, 0))
    return jnp.where(row < 4, roll(high[2, k], 2, 0), below)


class Tiles:
    def __init__(self, ref, starts):
        self.ref, self.starts = ref, starts

    def __getitem__(self, key):
        return self.ref[self.starts[key[0]] + key[1]]


def brief(above, below):
    return jnp.where(tile_row() < 4, above, below)


def row_mask(flags):
    row = lax.broadcasted_iota(jnp.int32, (ROWS - LY, LZ), 0)
    return jnp.where(row < 8, flags[3], flags[2])


AHEAD = (6, 6, 6, 5, 5, 5, 5, 2)
BEHIND = (6, 6, 6, 5, 5, 5, 6, 3)
AHEAD_AT = tuple(sum(AHEAD[:k]) for k in range(8))
BEHIND_AT = tuple(sum(BEHIND[:k]) for k in range(8))
FRONT, BACK = sum(AHEAD), sum(BEHIND)


def rows_kernel(
    disp, force, damage, history, crack, flags,
    first, last, top, bottom, top_crack, bottom_crack, sem,
):
    copies = []
    for rows, into, into_crack in ((0, top, top_crack), (24, bottom, bottom_crack)):
        for source, target in (
            (crack.at[:, rows : rows + 8], into_crack),
            (history.at[:, rows : rows + 8], into.at[7]),
            (damage.at[:, rows : rows + 8], into.at[6]),
            (disp.at[:, :, rows : rows + 8], into.at[0:3]),
            (force.at[:, :, rows : rows + 8], into.at[3:6]),
        ):
            copies.append(pltpu.make_async_copy(source, target, sem.at[len(copies)]))
    for copy in copies:
        copy.start()
    for copy in copies:
        copy.wait()

    row = tile_row()

    def step(group, carry):
        shared = jnp.zeros((8, LZ), f32)
        for place in range(4):
            k = 4 * group + place
            for into, flag, out, pack in (
                (top, top_crack, first, pack_first), (bottom, bottom_crack, last, pack_last)
            ):
                past = jnp.maximum(into[7, k], crack_load * flag[k].astype(f32))
                tiles = pack(
                    [into[j, k] for j in range(3)], [into[3 + j, k] for j in range(3)],
                    into[6, k], past,
                )
                for n, tile in enumerate(tiles):
                    out[n * LX + k] = tile
                if out is last:
                    here = (row >= 2 * place) & (row < 2 * place + 2)
                    shared = jnp.where(here, roll(past, 2 * place + 2, 0), shared)
        last[5 * LX + group] = shared
        return carry

    lax.fori_loop(0, 4, step, 0)


def bulk_kernel(
    disp_in, force_in, damage_in, history_in, crack_in,
    disp, force, damage, history, crack, front, back, sem,
):
    copies = [
        pltpu.make_async_copy(source, target, sem.at[n])
        for n, (source, target) in enumerate(
            (
                (crack_in, crack), (history_in, history), (damage_in, damage),
                (disp_in, disp), (force_in, force),
            )
        )
    ]
    for copy in copies:
        copy.start()
    for copy in copies:
        copy.wait()
    for counts, starts, out, ahead in (
        (AHEAD, AHEAD_AT, front, True), (BEHIND, BEHIND_AT, back, False)
    ):
        for k in range(8):
            size, at = counts[k], starts[k]
            begin = 0 if ahead else LX - size
            layers = slice(begin, begin + size)
            if k == 7:
                flag = crack[layers].astype(f32)
                out[at : at + size] = jnp.maximum(history[layers], crack_load * flag)
            else:
                field = disp.at[k] if k < 3 else force.at[k - 3] if k < 6 else damage
                out[at : at + size] = field[layers]


FRONT_TILES = (6, 6, 6, 5, 5, 6, 6, 6, 5, 5, 1)
BACK_TILES = (6,) * 10 + (1,)
FRONT_TILES_AT = tuple(sum(FRONT_TILES[:k]) for k in range(11))
BACK_TILES_AT = tuple(sum(BACK_TILES[:k]) for k in range(11))
ROW_TILES_AT = tuple(LX * k for k in range(6))


def corner_kernel(high, low, front, back):
    for counts, starts, out, ahead in (
        (FRONT_TILES, FRONT_TILES_AT, front, True), (BACK_TILES, BACK_TILES_AT, back, False)
    ):
        for k in range(10):
            size, at = counts[k], starts[k]
            begin = LX * (k % 5) + (0 if ahead else LX - size)
            source = high if k < 5 else low
            out[at : at + size] = source[begin : begin + size]
        out[starts[10]] = low[5 * LX + (0 if ahead else 3)]


def stress(u, n, gain, ahead):
    dx = [n[j] - u[j] for j in range(3)]
    dy = [next_row(u[j]) - u[j] for j in range(3)]
    dz = [ahead[j] - u[j] for j in range(3)]
    twice = gain + gain
    part = 0.75 * (dx[0] + dy[1] + dz[2])
    return (
        twice * (dx[0] + part),
        twice * (dy[1] + part),
        twice * (dz[2] + part),
        gain * (dx[1] + dy[0]),
        gain * (dx[2] + dz[0]),
        gain * (dy[2] + dz[1]),
    )


def divergence(u, s, before, diag):
    s00, s11, s22, s01, s02, s12 = s
    return (
        diag * u[0] + before[0] + last_row(s01) + last_lane(s02) - (s00 + s01 + s02),
        diag * u[1] + before[1] + last_row(s11) + last_lane(s12) - (s01 + s11 + s12),
        diag * u[2] + before[2] + last_row(s12) + last_lane(s22) - (s02 + s12 + s22),
    )


def vector(ref, i):
    return tuple(ref[j, i] for j in range(3))


def sweep(source, gain, begin, end, diag, store, unroll=None):
    u, n = vector(source, begin), vector(source, begin + 1)
    s = stress(u, n, gain[begin], [next_lane(x) for x in u])

    def step(i, carry):
        before, u, ahead = carry
        n = vector(source, i + 1)
        s = stress(u, n, gain[i], ahead)
        ahead = tuple(next_lane(x) for x in n)
        store(i, divergence(u, s, before, diag))
        return (s[0], s[3], s[4]), n, ahead

    carry = ((s[0], s[3], s[4]), n, tuple(next_lane(x) for x in n))
    if unroll is None:
        for i in range(begin + 1, end):
            carry = step(i, carry)
    else:
        lax.fori_loop(begin + 1, end, step, carry, unroll=unroll)


def store_to(ref, mask, flag=None, load=None):
    def store(i, image):
        for j in range(3):
            value = image[j] if load is None else load(j, i) - image[j]
            own, rest = value[0:LY], value[LY:ROWS] * mask
            if flag is not None:
                own, rest = own * flag, rest * flag
            ref[j, i, 0:LY] = own
            ref[j, i, LY:ROWS] = rest

    return store


def fold(x):
    return x[0:8] + x[8:16] + x[16:24] + x[24:32]


def moments_out(out, sums):
    lane = lanes((1, LZ))
    row = jnp.zeros((1, LZ), f32)
    for k, value in enumerate(sums):
        total = jnp.sum(jnp.sum(value, axis=0, keepdims=True), axis=1, keepdims=True)
        row = jnp.where(lane == k, total, row)
    out[...] = jnp.broadcast_to(row, out.shape)


def elastic_moments(v0, v1, v2, gain):
    def add(i, acc):
        u = vector(v2, i)
        up = [next_row(x)[0:LY] for x in u]
        u = [x[0:LY] for x in u]
        dx = [v2[j, i + 1, 0:LY] - u[j] for j in range(3)]
        dy = [up[j] - u[j] for j in range(3)]
        dz = [next_lane(u[j]) - u[j] for j in range(3)]
        trace = dx[0] + dy[1] + dz[2]
        e01, e02, e12 = dx[1] + dy[0], dx[2] + dz[0], dy[2] + dz[1]
        work = 2.0 * (dx[0] * dx[0] + dy[1] * dy[1] + dz[2] * dz[2])
        work = work + 1.5 * (trace * trace) + (e01 * e01 + e02 * e02 + e12 * e12)
        work = gain[i, 0:LY] * work
        a = [v0[j, i, 0:LY] for j in range(3)]
        b = [v1[j, i, 0:LY] for j in range(3)]

        def dot(x, y):
            return x[0] * y[0] + x[1] * y[1] + x[2] * y[2]

        square = dot(u, u)
        new = (
            dot(a, a), dot(a, b), dot(b, b), dot(b, u), square,
            work + (spring_term - SHIFT_U) * square,
        )
        return tuple(x + fold(y) for x, y in zip(acc, new))

    return add


def inner_kernel(
    disp, force, damage, history, crack, high, low, flags,
    wide, load, gain, v0, v1, v2, short_damage, past, partial,
):
    mask = row_mask(flags)

    high, low = Tiles(high, ROW_TILES_AT), Tiles(low, ROW_TILES_AT)

    def assemble(group, carry):
        for place in range(4):
            k = 4 * group + place
            i = OFF + k
            for j in range(3):
                wide[j, i, 0:LY] = disp[j, k]
                wide[j, i, LY : LY + 8] = high[j, k] * flags[3]
                wide[j, i, LY + 8 : ROWS] = low[j, k] * flags[2]
                load[j, k, 0:LY] = force[j, k]
                load[j, k, LY : LY + 8] = high_tile(high, 3 + j, k)
                load[j, k, LY + 8 : ROWS] = low_tile(low, 3 + j, k)
            own = damage[k]
            above, below = damage_tiles(high, low, k)
            short_damage[i, 0:LY] = own
            short_damage[i, LY:SHORT] = brief(above * flags[3], below * flags[2])
            left = 1.0 - own
            gain[i, 0:LY] = left * left + stiff_floor
            left = 1.0 - above
            gain[i, LY : LY + 8] = (left * left + stiff_floor) * mask[0:8]
            left = 1.0 - below
            gain[i, LY + 8 : ROWS] = (left * left + stiff_floor) * mask[8:16]
            past[i, 0:LY] = jnp.maximum(history[k], crack_load * crack[k].astype(f32))
            past[i, LY:SHORT] = past_tile(high, low, k, low[5, group], place)
        return carry

    lax.fori_loop(0, 4, assemble, 0)
    diag = spring_term - SHIFT_U
    first = store_to(v0, mask, load=lambda j, i: load[j, i - OFF])
    sweep(wide, gain, OFF, OFF + 15, spring_term, first, unroll=UNROLL)
    sweep(v0, gain, OFF + 1, OFF + 14, diag, store_to(v1, mask), unroll=UNROLL)
    sweep(v1, gain, OFF + 2, OFF + 13, diag, store_to(v2, mask), unroll=UNROLL)
    zero = jnp.zeros((8, LZ), f32)
    add = elastic_moments(v0, v1, v2, gain)
    for k, value in enumerate(
        lax.fori_loop(OFF + 3, OFF + 12, add, (zero,) * 6, unroll=3)
    ):
        partial[k] = value


UNROLL = 4


def outer_kernel(
    wide_in, load, gain_in, v0_in, v1_in, v2_in, short_in, past_in, partial,
    ahead, behind, ahead_corner, behind_corner, flags,
    wide, gain, v0, v1, v2, short_damage, past, sums, edge_load,
):
    mask = row_mask(flags)
    for counts, starts, high_side, middle, corner, tiles, flag in (
        (AHEAD, AHEAD_AT, True, ahead, ahead_corner, FRONT_TILES_AT, flags[1]),
        (BEHIND, BEHIND_AT, False, behind, behind_corner, BACK_TILES_AT, flags[0]),
    ):
        above, below = Tiles(corner, tiles[:5]), Tiles(corner, tiles[5:])
        for k in range(8):
            for c in range(counts[k]):
                own = middle[starts[k] + c]
                i = OFF + LX + c if high_side else OFF - counts[k] + c
                layer = c if high_side else 6 - counts[k] + c
                if k == 7:
                    past[i, 0:LY] = own
                    past[i, LY:SHORT] = past_tile(above, below, layer, below[5, 0], (layer if high_side else layer + 2) % 4)
                    continue
                if k < 6:
                    high, low = high_tile(above, k, layer), low_tile(below, k, layer)
                else:
                    high, low = damage_tiles(above, below, layer)
                if k < 3:
                    into = wide.at[k, i]
                    own = own * flag
                    high = high * (flag * flags[3])
                    low = low * (flag * flags[2])
                elif k < 6:
                    into = edge_load.at[k - 3, i - OFF - LX + 5 if high_side else i - 1]
                else:
                    into = gain.at[i]
                    short_damage[i, 0:LY] = own * flag
                    short_damage[i, LY:SHORT] = brief(
                        high * (flag * flags[3]), low * (flag * flags[2])
                    )
                    own, high, low = (
                        (1.0 - x) * (1.0 - x) + stiff_floor for x in (own, high, low)
                    )
                    own = own * flag
                    high = high * (mask[0:8] * flag)
                    low = low * (mask[8:16] * flag)
                into[0:LY] = own
                into[LY : LY + 8] = high
                into[LY + 8 : ROWS] = low

    def force_at(j, i):
        if i < OFF:
            return edge_load[j, i - 1]
        if i >= OFF + LX:
            return edge_load[j, i - OFF - LX + 5]
        return load[j, i - OFF]

    def both(source, target, low_end, high_begin, diag, load=None):
        def store(i, image):
            flag = flags[0] if i < OFF else flags[1] if i >= OFF + LX else None
            store_to(target, mask, flag, load)(i, image)

        sweep(source, gain, low_end - 7, low_end, diag, store)
        sweep(source, gain, high_begin, high_begin + 7, diag, store)

    diag = spring_term - SHIFT_U
    both(wide, v0, OFF + 1, OFF + 14, spring_term, force_at)
    both(v0, v1, OFF + 2, OFF + 13, diag)
    both(v1, v2, OFF + 3, OFF + 12, diag)

    add = elastic_moments(v0, v1, v2, gain)
    acc = tuple(partial[k] for k in range(6))
    for i in (*range(OFF, OFF + 3), *range(OFF + 12, OFF + 16)):
        acc = add(i, acc)
    moments_out(sums, acc)


def coefficients(gathered, shift):
    row = jnp.sum(gathered[...], axis=0, keepdims=True)
    lane = lanes((1, LZ))
    mu = [
        jnp.broadcast_to(
            jnp.sum(jnp.where(lane == k, row, 0.0), axis=1, keepdims=True), (1, LZ)
        )
        for k in range(6)
    ]

    def inner(a, b, up=0):
        total = None
        for i, x in enumerate(a):
            for j, y in enumerate(b):
                term = x * y * mu[i + j + up]
                total = term if total is None else total + term
        return total

    one = jnp.ones((1, LZ), f32)
    resid, direction = [one], [one]
    found = []
    norm = mu[0]
    for number in range(3):
        work = inner(direction, direction, 1) + shift * inner(direction, direction)
        alpha = norm / work
        for i, x in enumerate(direction):
            if i < len(found):
                found[i] = found[i] + alpha * x
            else:
                found.append(alpha * x)
        if number < 2:
            image = [shift * x for x in direction] + [jnp.zeros((1, LZ), f32)]
            for i, x in enumerate(direction):
                image[i + 1] = image[i + 1] + x
            resid = [
                (resid[i] if i < len(resid) else 0.0) - alpha * x for i, x in enumerate(image)
            ]
            new = inner(resid, resid)
            ratio = new / norm
            direction = [
                x + ratio * direction[i] if i < len(direction) else x
                for i, x in enumerate(resid)
            ]
            norm = new
    return found


def damage_kernel(
    gathered, wide, v0, v1, v2, short_damage, past, flags,
    moved_out, found_out, w0, w1, w2, sums, now, drive, moved, found, sem,
):
    a0, a1, a2 = coefficients(gathered, SHIFT_U)

    def current(j, i):
        value = wide[j, i] + a0 * v0[j, i] + a1 * v1[j, i] + a2 * v2[j, i]
        now[j, i, 0:LY] = value[0:LY]
        now[j, i, LY:SHORT] = brief(value[LY : LY + 8], value[LY + 8 : ROWS])
        return value

    def middle(i, carry):
        for j in range(3):
            moved[j, i - OFF] = current(j, i)[0:LY]
        return carry

    lax.fori_loop(OFF, OFF + LX, middle, 0, unroll=2)
    moved_copy = pltpu.make_async_copy(moved, moved_out, sem.at[0])
    moved_copy.start()
    for i in (*range(OFF - 3, OFF), *range(OFF + LX, OFF + LX + 3)):
        for j in range(3):
            current(j, i)

    row = lax.broadcasted_iota(jnp.int32, (8, LZ), 0)
    mask = jnp.where(row < 4, flags[3], flags[2])

    def energy(i):
        u, n = vector(now, i), vector(now, i + 1)
        dx = [n[j] - u[j] for j in range(3)]
        dy = [next_row(u[j]) - u[j] for j in range(3)]
        dz = [next_lane(u[j]) - u[j] for j in range(3)]
        trace = dx[0] + dy[1] + dz[2]
        e01, e02, e12 = dx[1] + dy[0], dx[2] + dz[0], dy[2] + dz[1]
        squares = dx[0] * dx[0] + dy[1] * dy[1] + dz[2] * dz[2]
        squares = squares + 0.5 * (e01 * e01 + e02 * e02 + e12 * e12)
        positive = jnp.maximum(trace, 0.0)
        return bulk_half * (positive * positive) + (squares - trace * trace * (1.0 / 3.0))

    def step(i, carry):
        value = jnp.maximum(past[i], energy(i))
        drive[i] = value
        found[i - OFF] = value[0:LY]
        return carry

    lax.fori_loop(OFF, OFF + LX, step, 0, unroll=4)
    found_copy = pltpu.make_async_copy(found, found_out, sem.at[1])
    found_copy.start()
    for i in (*range(OFF - 3, OFF), *range(OFF + LX, OFF + LX + 2)):
        drive[i] = jnp.maximum(past[i], energy(i))

    def flag_of(i):
        return jnp.where(i < OFF, flags[0], jnp.where(i >= OFF + LX, flags[1], 1.0))

    def apply(source, begin, end, make, target):
        def step(i, carry):
            before, here = carry
            n = source[i + 1]
            beside = before + n + next_row(here) + last_row(here)
            beside = beside + next_lane(here) + last_lane(here)
            value = make(i, here, beside) * flag_of(i)
            target[i, 0:LY] = value[0:LY]
            target[i, LY:SHORT] = value[LY:SHORT] * mask
            return here, n

        lax.fori_loop(begin, end, step, (source[begin - 1], source[begin]), unroll=7)

    full = tough_ratio + 6.0 * length_term

    def start(i, here, beside):
        twice = 2.0 * drive[i]
        return twice - ((full + twice) * here - length_term * beside)

    def image(i, here, beside):
        return ((full - SHIFT_D) + 2.0 * drive[i]) * here - length_term * beside

    apply(short_damage, OFF - 3, OFF + LX + 2, start, w0)
    apply(w0, OFF - 2, OFF + LX + 1, image, w1)
    apply(w1, OFF - 1, OFF + LX, image, w2)

    lane = lanes((LY, LZ))
    row = lax.broadcasted_iota(jnp.int32, (LY, LZ), 0)
    edge = jnp.where(lane == 0, length_term, 0.0)
    edge = edge + jnp.where(row == LY - 1, length_term * (1.0 - flags[3]), 0.0)
    edge = edge + (tough_ratio - SHIFT_D)

    def add(i, acc):
        wide_now = w2[i]
        u = wide_now[0:LY]
        dx = w2[i - 1, 0:LY] - u
        dy = last_row(wide_now)[0:LY] - u
        dz = next_lane(u) - u
        side = jnp.where(i == OFF + LX - 1, length_term * (1.0 - flags[1]), 0.0)
        square = u * u
        work = (edge + side + 2.0 * drive[i, 0:LY]) * square
        work = work + length_term * (dx * dx + dy * dy + dz * dz)
        a, b = w0[i, 0:LY], w1[i, 0:LY]
        new = (a * a, a * b, b * b, b * u, square, work)
        return tuple(x + fold(y) for x, y in zip(acc, new))

    zero = jnp.zeros((8, LZ), f32)
    moments_out(sums, lax.fori_loop(OFF, OFF + LX, add, (zero,) * 6, unroll=4))
    moved_copy.wait()
    found_copy.wait()


def update_kernel(gathered, damage, w0, w1, w2, out):
    b0, b1, b2 = coefficients(gathered, SHIFT_D)

    def step(c, carry):
        i = OFF + c
        image = b0 * w0[i, 0:LY] + b1 * w1[i, 0:LY] + b2 * w2[i, 0:LY]
        out[c] = damage[c] + image
        return carry

    lax.fori_loop(0, LX, step, 0, unroll=2)


def send(values, dx, dy):
    axis, step = ("gx", dx) if dx else ("gy", dy)
    size = lax.axis_size(axis)
    return lax.ppermute(values, axis, [(i, (i + step) % size) for i in range(size)])


def step(displacement, force, damage, history, crack_flags):
    axes = ("gx", "gy")
    count = lax.axis_size(axes)
    ix, iy = lax.axis_index("gx"), lax.axis_index("gy")
    flags = jnp.stack(
        [ix > 0, ix < lax.axis_size("gx") - 1, iy > 0, iy < lax.axis_size("gy") - 1]
    ).astype(f32)

    def gather(sums):
        return lax.all_to_all(sums, axes, 0, 0, tiled=True)

    given = (displacement, force, damage, history, crack_flags)
    edge_rows, edge_flags = (8, LX, 8, LZ), pltpu.VMEM((LX, 8, LZ), jnp.int32)
    first, last = call(
        rows_kernel,
        [(5 * LX, 8, LZ), (5 * LX + 4, 8, LZ)],
        [edge_rows, edge_rows, edge_flags, edge_flags, pltpu.SemaphoreType.DMA((10,))],
        hbm=True,
    )(*given, flags=flags)
    disp, load, old, history, crack, front, back = call(
        bulk_kernel,
        [(3, *FIELD), (3, *FIELD), FIELD, FIELD, fast_as(FIELD, jnp.int32)]
        + [(FRONT, LY, LZ), (BACK, LY, LZ)],
        [pltpu.SemaphoreType.DMA((5,))],
        hbm=True,
    )(*given)
    high = send(first, 0, -1)
    low = send(last, 0, 1)
    ahead = send(front, -1, 0)
    behind = send(back, 1, 0)
    corners = call(corner_kernel, [(sum(FRONT_TILES), 8, LZ), (sum(BACK_TILES), 8, LZ)])(high, low)
    ahead_corner = send(corners[0], -1, 0)
    behind_corner = send(corners[1], 1, 0)
    wide, load, gain, v0, v1, v2, short_damage, past, partial = call(
        inner_kernel,
        [VECTOR, (3, LX, ROWS, LZ), SCALAR, VECTOR, VECTOR, VECTOR, BRIEF, BRIEF, (6, 8, LZ)],
    )(disp, load, old, history, crack, high, low, flags=flags)
    wide, gain, v0, v1, v2, short_damage, past, sums = call(
        outer_kernel,
        [VECTOR, SCALAR, VECTOR, VECTOR, VECTOR, BRIEF, BRIEF, (count, LZ)],
        scratch=[(3, 10, ROWS, LZ)],
        aliases={0: 0, 2: 1, 3: 2, 4: 3, 5: 4, 6: 5, 7: 6},
    )(
        wide, load, gain, v0, v1, v2, short_damage, past, partial,
        ahead, behind, ahead_corner, behind_corner, flags=flags,
    )
    moved, found, w0, w1, w2, sums = call(
        damage_kernel,
        [whole(3, LX, LY, LZ), whole(LX, LY, LZ), BRIEF, BRIEF, BRIEF, (count, LZ)],
        [(3, DEPTH, SHORT, LZ), BRIEF, (3, *FIELD), FIELD, pltpu.SemaphoreType.DMA((2,))],
        far=2,
    )(gather(sums), wide, v0, v1, v2, short_damage, past, flags=flags)
    (damage_out,) = call(update_kernel, [whole(LX, LY, LZ)])(gather(sums), old, w0, w1, w2)
    return moved, damage_out, found


def solution(mesh):
    return jax.shard_map(
        step,
        mesh=mesh,
        in_specs=(
            P(None, "gx", "gy", None),
            P(None, "gx", "gy", None),
            P("gx", "gy", None),
            P("gx", "gy", None),
            P("gx", "gy", None),
        ),
        out_specs=(P(None, "gx", "gy", None), P("gx", "gy", None), P("gx", "gy", None)),
        check_vma=False,
    )
```
